256 devices in a mesh: section: 2 (over x_lo), slab: 128 (over y, x_hi, z, core).
Axes of the slice: x: 4 (x_hi: 2, x_lo: 2; x = x_hi * 2 + x_lo), y: 4, z: 8, core: 2. Of those that a mesh axis runs over, the one named last changes fastest.
Arguments:
- concentration: float32 [4, 2048, 2048], P('section', 'slab'), may hold values from -3.2 to 3.2
Outputs:
- new_concentration: float32 [4, 2048, 2048], P('section', 'slab')
- energy: float32 [], replicated
The draws below stay inside these ranges and needn't reach their ends.
All inputs are finite; a program needn't handle non-finite values.
Results may differ from the reference program's by a relative error of at most 0.000098.
Values sent between devices are 32-bit elements; how exact they have to be, the bound alone decides.
No kernel may reach another device: no remote copies, remote signals or barrier semaphores. Data moves between devices by JAX's collectives and lax.ppermute only.
A program may use at most 64 MiB of HBM per device.

```python
import math
import jax
import jax.numpy as jnp
from jax import lax

NX = 2048
NY = 2048
NZ = 4


def blur_weights(extent, coarse_total, blur_width):
    position = jnp.arange(extent, dtype=jnp.float32)
    spacing = extent / coarse_total
    centers = (jnp.arange(coarse_total, dtype=jnp.float32) + 0.5) * spacing
    offset = position[:, None] - centers[None, :]
    offset = jnp.mod(offset + 0.5 * extent, extent) - 0.5 * extent
    weights = jnp.exp(-offset * offset / (2.0 * blur_width * blur_width))
    return weights / jnp.sqrt(jnp.sum(weights * weights, axis=1, keepdims=True))


def draw_concentration(key, part):
    base_key = jax.random.fold_in(key, 7)
    noise_key = jax.random.fold_in(base_key, 0)
    smooth_key = jax.random.fold_in(base_key, 2)
    coarse_x = max(NX // 16, 4)
    coarse_y = max(NY // 16, 4)
    coarse = jax.random.normal(smooth_key, (NZ, coarse_x, coarse_y), jnp.float32)
    along_x = blur_weights(NX, coarse_x, 16.0)
    along_y = blur_weights(NY, coarse_y, 16.0)
    smooth = jnp.einsum('zij,xi->zxj', coarse, along_x, precision=lax.Precision.HIGHEST)
    smooth = jnp.einsum('zxj,yj->zxy', smooth, along_y, precision=lax.Precision.HIGHEST)
    depth_pos = jnp.arange(NZ, dtype=jnp.float32) / NZ
    row_pos = jnp.arange(NX, dtype=jnp.float32) / NX
    spread = 0.45 * (1.0 + 1.2 * row_pos[None, :, None] + 0.6 * depth_pos[:, None, None])
    jitter = jax.random.truncated_normal(noise_key, -2.5, 2.5, (NZ, NX, NY), jnp.float32)
    values = 0.6 * smooth + jitter * spread
    values = jnp.clip(values, -3.2, 3.2)
    return values.astype(jnp.float32)


def setup_inputs(seed: int = 0) -> dict:
    arg_keys = jax.random.split(jax.random.key(seed), 2)
    return {
        "concentration": draw_concentration(jax.random.fold_in(arg_keys[1], 71), 0),
    }


time_step = 100.0
kappa_grad = 2.0
stabilizer = 8.0


def wave_square(length):
    position = jnp.arange(length, dtype=jnp.int32)
    signed = jnp.where(2 * position >= length, position - length, position)
    phase_angle = signed.astype(jnp.float32) * (2.0 * math.pi / length)
    return phase_angle * phase_angle


def reference(concentration):
    squared = concentration * concentration
    bulk_sum = jnp.sum(0.25 * squared * squared - 0.5 * squared)
    cubic_term = squared * concentration - concentration
    spec_c = jnp.fft.fftn(concentration)
    spec_g = jnp.fft.fftn(cubic_term)
    wave_sq = wave_square(NZ)[:, None, None] + wave_square(NX)[None, :, None] + wave_square(NY)[None, None, :]
    numerator = 1.0 + time_step * stabilizer * wave_sq
    denominator = numerator + time_step * kappa_grad * wave_sq * wave_sq
    updated = (numerator * spec_c - time_step * wave_sq * spec_g) / denominator
    new_field = jnp.real(jnp.fft.ifftn(updated)).astype(jnp.float32)
    cell_count = NX * NY * NZ
    energy = (bulk_sum / cell_count).astype(jnp.float32)
    return (new_field, energy)
```

```python
import math

import jax
import jax.numpy as jnp
import ml_dtypes
import numpy as np
from jax import lax
from jax.experimental import pallas as pl
from jax.experimental.pallas import tpu as pltpu
from jax.sharding import PartitionSpec as P

ALL = ("section", "slab")
NX = 2048
NY = 2048
NZ = 4
CELLS = NX * NY * NZ
time_step = 100.0
kappa_grad = 2.0
stabilizer = 8.0
f32 = jnp.float32
bf16 = jnp.bfloat16


def halves(matrix):
    high = matrix.astype(np.float32).astype(ml_dtypes.bfloat16)
    low = (matrix - high.astype(np.float64)).astype(np.float32).astype(ml_dtypes.bfloat16)
    return np.stack([high, low])


def fourier_table():
    index = np.arange(128)
    angle = 2.0 * np.pi * (np.outer(index, index) % 128) / 128
    return halves(np.block([[np.cos(angle), np.sin(angle)], [-np.sin(angle), np.cos(angle)]]))


def real_table():
    angle = 2.0 * np.pi * (np.outer(np.arange(128), np.arange(256)) % 256) / 256
    lower = -np.sin(angle)
    lower[0] = 1.0 - 2.0 * (np.arange(256) % 2)
    return halves(np.concatenate([np.cos(angle), lower], 0))


def lane_table(parity):
    z_at, x_at = np.arange(2)[:, None, None, None], np.arange(16)[None, :, None, None]
    t_at, q_at = np.arange(2)[None, None, :, None], np.arange(16)[None, None, None, :]
    turn = (4 * parity * z_at + 8 * t_at * z_at + x_at * q_at) % 16
    value = np.exp(-2j * np.pi * turn / 16).reshape(32, 32)
    value = np.kron(np.eye(4), value)
    return halves(np.block([[value.real, value.imag], [-value.imag, value.real]]))


def y_twist_table():
    angle = 2.0 * np.pi * np.outer(np.arange(8), np.arange(128)) / 2048
    return np.concatenate([np.cos(angle), np.sin(angle)], 0).astype(np.float32)


def x_twist_table():
    angle = 2.0 * np.pi * np.outer(np.arange(128), np.arange(128) % 16) / 2048
    return np.stack([np.cos(angle), np.sin(angle)]).astype(np.float32)


FOURIER = fourier_table()
REAL = real_table()
LANES = np.stack([lane_table(0), lane_table(1)])
Y_TWIST = y_twist_table()
X_TWIST = x_twist_table()
COS16 = [math.cos(2.0 * math.pi * m / 16) for m in range(16)]
SIN16 = [math.sin(2.0 * math.pi * m / 16) for m in range(16)]


def split(value):
    high = value.astype(bf16)
    return high, (value - high.astype(f32)).astype(bf16)


NN = (((1,), (0,)), ((), ()))
NT = (((1,), (1,)), ((), ()))


def product(left, right, pattern):
    def one(a, b):
        return lax.dot_general(a, b, pattern, preferred_element_type=f32)

    return one(left[0], right[0]) + (one(left[1], right[0]) + one(left[0], right[1]))


def weighted(terms):
    total = None
    for weight, value in terms:
        if abs(weight) < 1e-12:
            continue
        if abs(weight - 1.0) < 1e-12:
            part = value
        elif abs(weight + 1.0) < 1e-12:
            part = -value
        else:
            part = value * weight
        total = part if total is None else total + part
    return total


def y_slots(field, twist):
    at = [field[:, 128 * a : 128 * a + 128] for a in range(16)]
    add = [at[a] + at[a + 8] for a in range(8)]
    sub = [at[a] - at[a + 8] for a in range(8)]
    slots = [
        jnp.concatenate([(add[0] + add[4]) + (add[2] + add[6]), (add[1] + add[5]) + (add[3] + add[7])], 1)
    ]
    real, imag = {}, {}
    for j in (2, 4, 6):
        real[j] = weighted([(COS16[j * a % 16], add[a]) for a in range(8)])
        imag[j] = weighted([(-SIN16[j * a % 16], add[a]) for a in range(8)])
    minus = [None] + [sub[a] - sub[8 - a] for a in (1, 2, 3)]
    plus = [None] + [sub[a] + sub[8 - a] for a in (1, 2, 3)] + [sub[4]]
    for j in (1, 3, 5, 7):
        real[j] = weighted([(1.0, sub[0])] + [(COS16[j * a % 16], minus[a]) for a in (1, 2, 3)])
        imag[j] = weighted([(-SIN16[j * a % 16], plus[a]) for a in (1, 2, 3, 4)])
    for j in range(1, 8):
        cos, sin = twist[j : j + 1], twist[8 + j : 9 + j]
        slots.append(
            jnp.concatenate([real[j] * cos + imag[j] * sin, imag[j] * cos - real[j] * sin], 1)
        )
    return slots


def forward_y(field, fourier, real_rows, twist, put):
    squared = field * field
    bulk = squared * (0.25 * squared - 0.5)
    cubic = squared * field - field
    for f, value in ((0, field), (1, cubic)):
        slots = y_slots(value, twist)
        first = product(real_rows, split(slots[0]), NT)
        for h in (0, 1):
            rows = jnp.concatenate(slots[4 * h : 4 * h + 4], 0)
            out = product(fourier, split(rows), NT)
            if h == 0:
                lane = lax.broadcasted_iota(jnp.int32, (256, 128), 1)
                wide = jnp.concatenate([first] * 4, 1)
                out = jnp.where(lane < 32, wide, out)
            put(h, 0, f, out[:128])
            put(h, 1, f, out[128:])
    lanes = sum(bulk[:, 128 * a : 128 * a + 128] for a in range(16))
    return lanes


def wave_square(index, length):
    signed = jnp.where(2 * index >= length, index - length, index)
    phase_angle = signed.astype(f32) * (2.0 * math.pi / length)
    return phase_angle * phase_angle


def rates(wave_sq):
    numerator = 1.0 + time_step * stabilizer * wave_sq
    inverse = 1.0 / (numerator + time_step * kappa_grad * wave_sq * wave_sq)
    return numerator * inverse, time_step * wave_sq * inverse


def middle(get, section_at, slab_at, fourier, lanes, twist, put):
    lane = lax.broadcasted_iota(jnp.int32, (128, 128), 1)
    row = lax.broadcasted_iota(jnp.int32, (128, 128), 0)
    packed = (lane < 32) & (section_at == 0) & (slab_at == 0)
    cos, sin = twist[0], twist[1]
    parts = []
    for s in (0, 1):
        c_re, c_im, g_re, g_im = get(s, 0, 0), get(s, 1, 0), get(s, 0, 1), get(s, 1, 1)
        c_im, g_re = jnp.where(packed, g_re, c_im), jnp.where(packed, c_im, g_re)
        parts.append((c_re, c_im, g_re, g_im))
    stacked = []
    for sigma in (0, 1):
        mixed = [a + b if sigma == 0 else a - b for a, b in zip(*parts)]
        stacked.append(
            jnp.concatenate(
                [jnp.concatenate([mixed[0], mixed[2]], 1), jnp.concatenate([mixed[1], mixed[3]], 1)], 0
            )
        )
    slot = 4 * section_at + lane // 32
    y_index = jnp.where(slot == 0, 8 * slab_at, slot + 16 * slab_at)
    x_index = row + 128 * (lane % 16)
    wave_x = wave_square(x_index, NX)
    wave_xy = wave_x + wave_square(y_index, NY)
    half_y = (2.0 * math.pi / NY * (NY // 2)) ** 2
    back = []
    for sigma in (0, 1):
        spread = product(fourier, split(stacked[sigma]), NN)
        rows = []
        for f in (0, 1):
            re, im = spread[:128, 128 * f : 128 * f + 128], spread[128:, 128 * f : 128 * f + 128]
            rows.append(jnp.concatenate([re * cos + im * sin, im * cos - re * sin], 1))
        table = (lanes[sigma, 0], lanes[sigma, 1])
        spec = product(split(jnp.concatenate(rows, 0)), table, NN)
        c_re, c_im, g_re, g_im = spec[:128, :128], spec[:128, 128:], spec[128:, :128], spec[128:, 128:]
        wave_z = wave_square(sigma + 2 * (lane // 16 % 2), NZ)
        keep, mix = rates(wave_z + wave_xy)
        keep_half, mix_half = rates(wave_z + (wave_x + half_y))
        main_re = keep * c_re - mix * jnp.where(packed, c_im, g_re)
        main_im = keep * c_im - mix * jnp.where(packed, -c_re, g_im)
        side_re = keep_half * g_re - mix_half * g_im
        side_im = keep_half * g_im + mix_half * g_re
        rows = jnp.concatenate(
            [jnp.concatenate([main_re, main_im], 1), jnp.concatenate([side_re, side_im], 1)], 0
        )
        back.append(product(split(rows), table, NT))
    for s in (0, 1):
        mixed = back[0] + back[1] if s == 0 else back[0] - back[1]
        both = []
        for f in (0, 1):
            re, im = mixed[128 * f : 128 * f + 128, :128], mixed[128 * f : 128 * f + 128, 128:]
            both.append((re * cos - im * sin, im * cos + re * sin))
        (m_re, m_im), (s_re, s_im) = both
        upper = jnp.concatenate([m_re, jnp.where(packed, s_re, m_im)], 1)
        lower = jnp.concatenate([-m_im, jnp.where(packed, -s_im, m_re)], 1)
        out = product(
            (fourier[0][:128], fourier[1][:128]), split(jnp.concatenate([upper, lower], 0)), NN
        )
        put(s, 0, out[:, :128])
        put(s, 1, out[:, 128:])


def inverse_y(get, fourier, real_rows, twist, put):
    slots = []
    for h in (0, 1):
        re, im = get(h, 0), get(h, 1)
        if h == 0:
            row = lax.broadcasted_iota(jnp.int32, (128, 128), 0)
            lane = lax.broadcasted_iota(jnp.int32, (128, 128), 1)
            single = (row == 0) & (lane < 32)
            re, im = jnp.where(single, 0.5 * re, re), jnp.where(single, 0.5 * im, im)
        rows = split(jnp.concatenate([re.T, im.T], 1))
        if h == 0:
            first = product((rows[0][:32], rows[1][:32]), real_rows, NN)
            rows = (rows[0][32:], rows[1][32:])
        out = product(rows, fourier, NN)
        slots += [out[32 * m : 32 * m + 32] for m in range(out.shape[0] // 32)]
    scale = 2.0 / CELLS
    base = [first[:, :128] * scale, first[:, 128:] * scale]
    real, imag = {}, {}
    for j in range(1, 8):
        re, im = slots[j - 1][:, :128], slots[j - 1][:, 128:]
        cos, sin = twist[j : j + 1] * scale, twist[8 + j : 9 + j] * scale
        real[j], imag[j] = re * cos - im * sin, im * cos + re * sin
    even = [
        weighted(
            [(COS16[j * a % 16], real[j]) for j in (2, 4, 6)]
            + [(-SIN16[j * a % 16], imag[j]) for j in (2, 4, 6)]
        )
        + base[a % 2]
        for a in range(8)
    ]
    cosine = [weighted([(COS16[j * a % 16], real[j]) for j in (1, 3, 5, 7)]) for a in range(4)]
    sine = [None] + [weighted([(SIN16[j * a % 16], imag[j]) for j in (1, 3, 5, 7)]) for a in range(1, 5)]
    odd = [cosine[0]] + [cosine[a] - sine[a] for a in (1, 2, 3)] + [-sine[4]]
    odd += [-cosine[a] - sine[a] for a in (3, 2, 1)]
    for a in range(8):
        put(a, even[a] + odd[a])
        put(a + 8, even[a] - odd[a])


def forward_kernel(c_ref, fourier_ref, real_ref, twist_ref, out_ref, bulk_ref):
    def put(h, part, f, value):
        at = 2 * part + f
        out_ref[128 * h : 128 * h + 128, 128 * at : 128 * at + 128] = value

    field = jnp.concatenate([c_ref[0], c_ref[1]], 0)
    lanes = forward_y(
        field, (fourier_ref[0], fourier_ref[1]), (real_ref[0], real_ref[1]), twist_ref[...], put
    )
    bulk_ref[...] = jnp.broadcast_to(jnp.sum(lanes, 0, keepdims=True), (8, 128))


def middle_kernel(in_ref, bulk_ref, fourier_ref, lanes_ref, twist_ref, out_ref):
    def get(s, part, f):
        at = 2 * part + f
        return in_ref[128 * s : 128 * s + 128, 128 * at : 128 * at + 128]

    def put(s, part, value):
        out_ref[128 * s : 128 * s + 128, 128 * part : 128 * part + 128] = value

    middle(
        get,
        lax.axis_index("section"),
        lax.axis_index("slab"),
        (fourier_ref[0], fourier_ref[1]),
        lanes_ref,
        twist_ref,
        put,
    )
    out_ref[:, 256:384] = jnp.broadcast_to(bulk_ref[0:1, :], (256, 128))


def inverse_kernel(in_ref, fourier_ref, real_ref, twist_ref, out_ref, energy_ref):
    def get(h, part):
        return in_ref[128 * h : 128 * h + 128, 128 * part : 128 * part + 128]

    def put(a, value):
        out_ref[0, :, 128 * a : 128 * a + 128] = value[:16]
        out_ref[1, :, 128 * a : 128 * a + 128] = value[16:]

    inverse_y(
        get, (fourier_ref[0], fourier_ref[1]), (real_ref[0], real_ref[1]), twist_ref[...], put
    )
    energy_ref[...] = jnp.sum(in_ref[:, 256:384], keepdims=True) * (1.0 / CELLS)


def per_device(concentration):
    whole = pl.BlockSpec(memory_space=pltpu.VMEM)
    outgoing, bulk = pl.pallas_call(
        forward_kernel,
        out_shape=(jax.ShapeDtypeStruct((256, 512), f32), jax.ShapeDtypeStruct((8, 128), f32)),
        in_specs=[whole] * 4,
        out_specs=(whole, whole),
    )(concentration, FOURIER, REAL, Y_TWIST)
    columns = lax.all_to_all(outgoing, ALL, split_axis=0, concat_axis=0, tiled=True)
    leaving = pl.pallas_call(
        middle_kernel,
        out_shape=jax.ShapeDtypeStruct((256, 384), f32),
        in_specs=[whole] * 5,
        out_specs=whole,
    )(columns, bulk, FOURIER, LANES, X_TWIST)
    rows_back = lax.all_to_all(leaving, ALL, split_axis=0, concat_axis=0, tiled=True)
    new_field, energy = pl.pallas_call(
        inverse_kernel,
        out_shape=(jax.ShapeDtypeStruct(concentration.shape, f32), jax.ShapeDtypeStruct((1, 1), f32)),
        in_specs=[whole] * 4,
        out_specs=(whole, whole),
    )(rows_back, FOURIER, REAL, Y_TWIST)
    return new_field, energy.reshape(())


def solution(mesh):
    return jax.shard_map(
        per_device,
        mesh=mesh,
        in_specs=(P("section", "slab", None),),
        out_specs=(P("section", "slab", None), P()),
        check_vma=False,
    )
```

```python
import math

import jax
import jax.numpy as jnp
import ml_dtypes
import numpy as np
from jax import lax
from jax.experimental import pallas as pl
from jax.experimental.pallas import tpu as pltpu
from jax.sharding import PartitionSpec as P

ALL = ("section", "slab")
NX = 2048
NY = 2048
NZ = 4
CELLS = NX * NY * NZ
time_step = 100.0
kappa_grad = 2.0
stabilizer = 8.0
f32 = jnp.float32
bf16 = jnp.bfloat16


def halves(matrix):
    high = matrix.astype(np.float32).astype(ml_dtypes.bfloat16)
    low = (matrix - high.astype(np.float64)).astype(np.float32).astype(ml_dtypes.bfloat16)
    return np.stack([high, low])


def fourier_table():
    index = np.arange(128)
    angle = 2.0 * np.pi * (np.outer(index, index) % 128) / 128
    return halves(np.block([[np.cos(angle), np.sin(angle)], [-np.sin(angle), np.cos(angle)]]))


def real_table():
    angle = 2.0 * np.pi * (np.outer(np.arange(128), np.arange(256)) % 256) / 256
    lower = -np.sin(angle)
    lower[0] = 1.0 - 2.0 * (np.arange(256) % 2)
    return halves(np.concatenate([np.cos(angle), lower], 0))


def lane_table(parity):
    z_at, x_at = np.arange(2)[:, None, None, None], np.arange(16)[None, :, None, None]
    t_at, q_at = np.arange(2)[None, None, :, None], np.arange(16)[None, None, None, :]
    turn = (4 * parity * z_at + 8 * t_at * z_at + x_at * q_at) % 16
    value = np.exp(-2j * np.pi * turn / 16).reshape(32, 32)
    value = np.kron(np.eye(4), value)
    return halves(np.block([[value.real, value.imag], [-value.imag, value.real]]))


def y_twist_table():
    angle = 2.0 * np.pi * np.outer(np.arange(8), np.arange(128)) / 2048
    return np.concatenate([np.cos(angle), np.sin(angle)], 0).astype(np.float32)


def x_twist_table():
    angle = 2.0 * np.pi * np.outer(np.arange(128), np.arange(128) % 16) / 2048
    return np.stack([np.cos(angle), np.sin(angle)]).astype(np.float32)


FOURIER = fourier_table()
REAL = real_table()
LANES = np.stack([lane_table(0), lane_table(1)])
Y_TWIST = y_twist_table()
X_TWIST = x_twist_table()
COS16 = [math.cos(2.0 * math.pi * m / 16) for m in range(16)]
SIN16 = [math.sin(2.0 * math.pi * m / 16) for m in range(16)]


def split(value):
    high = value.astype(bf16)
    return high, (value - high.astype(f32)).astype(bf16)


NN = (((1,), (0,)), ((), ()))
NT = (((1,), (1,)), ((), ()))


def product(left, right, pattern):
    def one(a, b):
        return lax.dot_general(a, b, pattern, preferred_element_type=f32)

    return one(left[0], right[0]) + (one(left[1], right[0]) + one(left[0], right[1]))


def weighted(terms):
    total = None
    for weight, value in terms:
        if abs(weight) < 1e-12:
            continue
        if abs(weight - 1.0) < 1e-12:
            part = value
        elif abs(weight + 1.0) < 1e-12:
            part = -value
        else:
            part = value * weight
        total = part if total is None else total + part
    return total


def y_slots(field, twist):
    at = [field[:, 128 * a : 128 * a + 128] for a in range(16)]
    add = [at[a] + at[a + 8] for a in range(8)]
    sub = [at[a] - at[a + 8] for a in range(8)]
    slots = [
        jnp.concatenate([(add[0] + add[4]) + (add[2] + add[6]), (add[1] + add[5]) + (add[3] + add[7])], 1)
    ]
    real, imag = {}, {}
    for j in (2, 4, 6):
        real[j] = weighted([(COS16[j * a % 16], add[a]) for a in range(8)])
        imag[j] = weighted([(-SIN16[j * a % 16], add[a]) for a in range(8)])
    minus = [None] + [sub[a] - sub[8 - a] for a in (1, 2, 3)]
    plus = [None] + [sub[a] + sub[8 - a] for a in (1, 2, 3)] + [sub[4]]
    for j in (1, 3, 5, 7):
        real[j] = weighted([(1.0, sub[0])] + [(COS16[j * a % 16], minus[a]) for a in (1, 2, 3)])
        imag[j] = weighted([(-SIN16[j * a % 16], plus[a]) for a in (1, 2, 3, 4)])
    for j in range(1, 8):
        cos, sin = twist[j : j + 1], twist[8 + j : 9 + j]
        slots.append(
            jnp.concatenate([real[j] * cos + imag[j] * sin, imag[j] * cos - real[j] * sin], 1)
        )
    return slots


def forward_y(field, fourier, real_rows, twist, put):
    squared = field * field
    bulk = squared * (0.25 * squared - 0.5)
    cubic = squared * field - field
    for f, value in ((0, field), (1, cubic)):
        slots = y_slots(value, twist)
        first = product(real_rows, split(slots[0]), NT)
        for h in (0, 1):
            rows = jnp.concatenate(slots[4 * h : 4 * h + 4], 0)
            out = product(fourier, split(rows), NT)
            if h == 0:
                lane = lax.broadcasted_iota(jnp.int32, (256, 128), 1)
                wide = jnp.concatenate([first] * 4, 1)
                out = jnp.where(lane < 32, wide, out)
            put(h, 0, f, out[:128])
            put(h, 1, f, out[128:])
    lanes = sum(bulk[:, 128 * a : 128 * a + 128] for a in range(16))
    return lanes


def wave_square(index, length):
    signed = jnp.where(2 * index >= length, index - length, index)
    phase_angle = signed.astype(f32) * (2.0 * math.pi / length)
    return phase_angle * phase_angle


def rates(wave_sq):
    numerator = 1.0 + time_step * stabilizer * wave_sq
    inverse = 1.0 / (numerator + time_step * kappa_grad * wave_sq * wave_sq)
    return numerator * inverse, time_step * wave_sq * inverse


def middle(get, section_at, slab_at, fourier, lanes, twist, put):
    lane = lax.broadcasted_iota(jnp.int32, (128, 128), 1)
    row = lax.broadcasted_iota(jnp.int32, (128, 128), 0)
    packed = (lane < 32) & (section_at == 0) & (slab_at == 0)
    cos, sin = twist[0], twist[1]
    parts = []
    for s in (0, 1):
        c_re, c_im, g_re, g_im = get(s, 0, 0), get(s, 1, 0), get(s, 0, 1), get(s, 1, 1)
        c_im, g_re = jnp.where(packed, g_re, c_im), jnp.where(packed, c_im, g_re)
        parts.append((c_re, c_im, g_re, g_im))
    stacked = []
    for sigma in (0, 1):
        mixed = [a + b if sigma == 0 else a - b for a, b in zip(*parts)]
        stacked.append(
            jnp.concatenate(
                [jnp.concatenate([mixed[0], mixed[2]], 1), jnp.concatenate([mixed[1], mixed[3]], 1)], 0
            )
        )
    slot = 4 * section_at + lane // 32
    y_index = jnp.where(slot == 0, 8 * slab_at, slot + 16 * slab_at)
    x_index = row + 128 * (lane % 16)
    wave_x = wave_square(x_index, NX)
    wave_xy = wave_x + wave_square(y_index, NY)
    half_y = (2.0 * math.pi / NY * (NY // 2)) ** 2
    back = []
    for sigma in (0, 1):
        spread = product(fourier, split(stacked[sigma]), NN)
        rows = []
        for f in (0, 1):
            re, im = spread[:128, 128 * f : 128 * f + 128], spread[128:, 128 * f : 128 * f + 128]
            rows.append(jnp.concatenate([re * cos + im * sin, im * cos - re * sin], 1))
        table = (lanes[sigma, 0], lanes[sigma, 1])
        spec = product(split(jnp.concatenate(rows, 0)), table, NN)
        c_re, c_im, g_re, g_im = spec[:128, :128], spec[:128, 128:], spec[128:, :128], spec[128:, 128:]
        wave_z = wave_square(sigma + 2 * (lane // 16 % 2), NZ)
        keep, mix = rates(wave_z + wave_xy)
        keep_half, mix_half = rates(wave_z + (wave_x + half_y))
        main_re = keep * c_re - mix * jnp.where(packed, c_im, g_re)
        main_im = keep * c_im - mix * jnp.where(packed, -c_re, g_im)
        side_re = keep_half * g_re - mix_half * g_im
        side_im = keep_half * g_im + mix_half * g_re
        rows = jnp.concatenate(
            [jnp.concatenate([main_re, main_im], 1), jnp.concatenate([side_re, side_im], 1)], 0
        )
        back.append(product(split(rows), table, NT))
    for s in (0, 1):
        mixed = back[0] + back[1] if s == 0 else back[0] - back[1]
        both = []
        for f in (0, 1):
            re, im = mixed[128 * f : 128 * f + 128, :128], mixed[128 * f : 128 * f + 128, 128:]
            both.append((re * cos - im * sin, im * cos + re * sin))
        (m_re, m_im), (s_re, s_im) = both
        upper = jnp.concatenate([m_re, jnp.where(packed, s_re, m_im)], 1)
        lower = jnp.concatenate([-m_im, jnp.where(packed, -s_im, m_re)], 1)
        out = product(
            (fourier[0][:128], fourier[1][:128]), split(jnp.concatenate([upper, lower], 0)), NN
        )
        put(s, 0, out[:, :128])
        put(s, 1, out[:, 128:])


def inverse_y(get, fourier, real_rows, twist, put):
    slots = []
    for h in (0, 1):
        re, im = get(h, 0), get(h, 1)
        if h == 0:
            row = lax.broadcasted_iota(jnp.int32, (128, 128), 0)
            lane = lax.broadcasted_iota(jnp.int32, (128, 128), 1)
            single = (row == 0) & (lane < 32)
            re, im = jnp.where(single, 0.5 * re, re), jnp.where(single, 0.5 * im, im)
        rows = split(jnp.concatenate([re.T, im.T], 1))
        if h == 0:
            first = product((rows[0][:32], rows[1][:32]), real_rows, NN)
            rows = (rows[0][32:], rows[1][32:])
        out = product(rows, fourier, NN)
        slots += [out[32 * m : 32 * m + 32] for m in range(out.shape[0] // 32)]
    scale = 2.0 / CELLS
    base = [first[:, :128] * scale, first[:, 128:] * scale]
    real, imag = {}, {}
    for j in range(1, 8):
        re, im = slots[j - 1][:, :128], slots[j - 1][:, 128:]
        cos, sin = twist[j : j + 1] * scale, twist[8 + j : 9 + j] * scale
        real[j], imag[j] = re * cos - im * sin, im * cos + re * sin
    even = [
        weighted(
            [(COS16[j * a % 16], real[j]) for j in (2, 4, 6)]
            + [(-SIN16[j * a % 16], imag[j]) for j in (2, 4, 6)]
        )
        + base[a % 2]
        for a in range(8)
    ]
    cosine = [weighted([(COS16[j * a % 16], real[j]) for j in (1, 3, 5, 7)]) for a in range(4)]
    sine = [None] + [weighted([(SIN16[j * a % 16], imag[j]) for j in (1, 3, 5, 7)]) for a in range(1, 5)]
    odd = [cosine[0]] + [cosine[a] - sine[a] for a in (1, 2, 3)] + [-sine[4]]
    odd += [-cosine[a] - sine[a] for a in (3, 2, 1)]
    for a in range(8):
        put(a, even[a] + odd[a])
        put(a + 8, even[a] - odd[a])


def forward_kernel(c_ref, fourier_ref, real_ref, twist_ref, out_ref, bulk_ref):
    def put(h, part, f, value):
        out_ref[pl.ds(512 * h + 2 * part + f, 128, stride=4), :] = value

    field = jnp.concatenate([c_ref[0], c_ref[1]], 0)
    lanes = forward_y(
        field, (fourier_ref[0], fourier_ref[1]), (real_ref[0], real_ref[1]), twist_ref[...], put
    )
    bulk_ref[...] = jnp.broadcast_to(jnp.sum(lanes, 0, keepdims=True), (8, 128))


def middle_kernel(in_ref, bulk_ref, fourier_ref, lanes_ref, twist_ref, out_ref):
    def get(s, part, f):
        return in_ref[pl.ds(512 * s + 2 * part + f, 128, stride=4), :]

    def put(s, part, value):
        out_ref[pl.ds(384 * s + part, 128, stride=3), :] = value

    middle(
        get,
        lax.axis_index("section"),
        lax.axis_index("slab"),
        (fourier_ref[0], fourier_ref[1]),
        lanes_ref,
        twist_ref,
        put,
    )
    out_ref[pl.ds(2, 256, stride=3), :] = jnp.broadcast_to(bulk_ref[0:1, :], (256, 128))


def inverse_kernel(in_ref, fourier_ref, real_ref, twist_ref, out_ref, energy_ref):
    def get(h, part):
        return in_ref[pl.ds(384 * h + part, 128, stride=3), :]

    def put(a, value):
        out_ref[0, :, 128 * a : 128 * a + 128] = value[:16]
        out_ref[1, :, 128 * a : 128 * a + 128] = value[16:]

    inverse_y(
        get, (fourier_ref[0], fourier_ref[1]), (real_ref[0], real_ref[1]), twist_ref[...], put
    )
    energy_ref[...] = jnp.sum(in_ref[pl.ds(2, 256, stride=3), :], keepdims=True) * (1.0 / CELLS)


def exchange(rows):
    width = rows.shape[0] // 256
    message = rows.reshape(256, 1, 128 * width)
    return lax.all_to_all(message, ALL, split_axis=0, concat_axis=0, tiled=True).reshape(rows.shape)


def per_device(concentration):
    whole = pl.BlockSpec(memory_space=pltpu.VMEM)
    outgoing, bulk = pl.pallas_call(
        forward_kernel,
        out_shape=(jax.ShapeDtypeStruct((1024, 128), f32), jax.ShapeDtypeStruct((8, 128), f32)),
        in_specs=[whole] * 4,
        out_specs=(whole, whole),
    )(concentration, FOURIER, REAL, Y_TWIST)
    columns = exchange(outgoing)
    leaving = pl.pallas_call(
        middle_kernel,
        out_shape=jax.ShapeDtypeStruct((768, 128), f32),
        in_specs=[whole] * 5,
        out_specs=whole,
    )(columns, bulk, FOURIER, LANES, X_TWIST)
    rows_back = exchange(leaving)
    new_field, energy = pl.pallas_call(
        inverse_kernel,
        out_shape=(jax.ShapeDtypeStruct(concentration.shape, f32), jax.ShapeDtypeStruct((1, 1), f32)),
        in_specs=[whole] * 4,
        out_specs=(whole, whole),
    )(rows_back, FOURIER, REAL, Y_TWIST)
    return new_field, energy.reshape(())


def solution(mesh):
    return jax.shard_map(
        per_device,
        mesh=mesh,
        in_specs=(P("section", "slab", None),),
        out_specs=(P("section", "slab", None), P()),
        check_vma=False,
    )
```

```python
import math

import jax
import jax.numpy as jnp
import ml_dtypes
import numpy as np
from jax import lax
from jax.experimental import pallas as pl
from jax.experimental.pallas import tpu as pltpu
from jax.sharding import PartitionSpec as P

ALL = ("section", "slab")
NX = 2048
NY = 2048
NZ = 4
CELLS = NX * NY * NZ
time_step = 100.0
kappa_grad = 2.0
stabilizer = 8.0
f32 = jnp.float32
bf16 = jnp.bfloat16


def halves(matrix):
    high = matrix.astype(np.float32).astype(ml_dtypes.bfloat16)
    low = (matrix - high.astype(np.float64)).astype(np.float32).astype(ml_dtypes.bfloat16)
    return np.stack([high, low])


def fourier_table():
    index = np.arange(128)
    angle = 2.0 * np.pi * (np.outer(index, index) % 128) / 128
    return halves(np.block([[np.cos(angle), np.sin(angle)], [-np.sin(angle), np.cos(angle)]]))


def real_table():
    angle = 2.0 * np.pi * (np.outer(np.arange(128), np.arange(256)) % 256) / 256
    lower = -np.sin(angle)
    lower[0] = 1.0 - 2.0 * (np.arange(256) % 2)
    return halves(np.concatenate([np.cos(angle), lower], 0))


def lane_table(parity):
    z_at, x_at = np.arange(2)[:, None, None, None], np.arange(16)[None, :, None, None]
    t_at, q_at = np.arange(2)[None, None, :, None], np.arange(16)[None, None, None, :]
    turn = (4 * parity * z_at + 8 * t_at * z_at + x_at * q_at) % 16
    value = np.exp(-2j * np.pi * turn / 16).reshape(32, 32)
    value = np.kron(np.eye(4), value)
    return halves(np.block([[value.real, value.imag], [-value.imag, value.real]]))


def y_twist_table():
    angle = 2.0 * np.pi * np.outer(np.arange(8), np.arange(128)) / 2048
    return np.concatenate([np.cos(angle), np.sin(angle)], 0).astype(np.float32)


def x_twist_table():
    angle = 2.0 * np.pi * np.outer(np.arange(128), np.arange(128) % 16) / 2048
    return np.stack([np.cos(angle), np.sin(angle)]).astype(np.float32)


FOURIER = fourier_table()
REAL = real_table()
LANES = np.stack([lane_table(0), lane_table(1)])
Y_TWIST = y_twist_table()
X_TWIST = x_twist_table()
COS16 = [math.cos(2.0 * math.pi * m / 16) for m in range(16)]
SIN16 = [math.sin(2.0 * math.pi * m / 16) for m in range(16)]


def split(value):
    high = value.astype(bf16)
    return high, (value - high.astype(f32)).astype(bf16)


NN = (((1,), (0,)), ((), ()))
NT = (((1,), (1,)), ((), ()))


def product(left, right, pattern):
    def one(a, b):
        return lax.dot_general(a, b, pattern, preferred_element_type=f32)

    return one(left[0], right[0]) + (one(left[1], right[0]) + one(left[0], right[1]))


def weighted(terms):
    total = None
    for weight, value in terms:
        if abs(weight) < 1e-12:
            continue
        if abs(weight - 1.0) < 1e-12:
            part = value
        elif abs(weight + 1.0) < 1e-12:
            part = -value
        else:
            part = value * weight
        total = part if total is None else total + part
    return total


def y_slots(field):
    at = [field[:, 128 * a : 128 * a + 128] for a in range(16)]
    add = [at[a] + at[a + 8] for a in range(8)]
    sub = [at[a] - at[a + 8] for a in range(8)]
    slots = [
        jnp.concatenate([(add[0] + add[4]) + (add[2] + add[6]), (add[1] + add[5]) + (add[3] + add[7])], 1)
    ]
    real, imag = {}, {}
    for j in (2, 4, 6):
        real[j] = weighted([(COS16[j * a % 16], add[a]) for a in range(8)])
        imag[j] = weighted([(-SIN16[j * a % 16], add[a]) for a in range(8)])
    minus = [None] + [sub[a] - sub[8 - a] for a in (1, 2, 3)]
    plus = [None] + [sub[a] + sub[8 - a] for a in (1, 2, 3)] + [sub[4]]
    for j in (1, 3, 5, 7):
        real[j] = weighted([(1.0, sub[0])] + [(COS16[j * a % 16], minus[a]) for a in (1, 2, 3)])
        imag[j] = weighted([(-SIN16[j * a % 16], plus[a]) for a in (1, 2, 3, 4)])
    return slots + [(real[j], imag[j]) for j in range(1, 8)]


def forward_y(field, read_fourier, read_real, read_twist, put):
    squared = field * field
    bulk = squared * (0.25 * squared - 0.5)
    cubic = squared * field - field
    both = [y_slots(field), y_slots(cubic)]
    twist = read_twist()
    for slots in both:
        for j in range(1, 8):
            real, imag = slots[j]
            cos, sin = twist[j : j + 1], twist[8 + j : 9 + j]
            slots[j] = jnp.concatenate([real * cos + imag * sin, imag * cos - real * sin], 1)
    real_rows = read_real()
    fourier = read_fourier()
    for f, slots in enumerate(both):
        first = product(real_rows, split(slots[0]), NT)
        for h in (0, 1):
            rows = jnp.concatenate(slots[4 * h : 4 * h + 4], 0)
            out = product(fourier, split(rows), NT)
            if h == 0:
                lane = lax.broadcasted_iota(jnp.int32, (256, 128), 1)
                wide = jnp.concatenate([first] * 4, 1)
                out = jnp.where(lane < 32, wide, out)
            put(h, 0, f, out[:128])
            put(h, 1, f, out[128:])
    lanes = sum(bulk[:, 128 * a : 128 * a + 128] for a in range(16))
    return lanes


def wave_square(index, length):
    signed = jnp.where(2 * index >= length, index - length, index)
    phase_angle = signed.astype(f32) * (2.0 * math.pi / length)
    return phase_angle * phase_angle


def rates(wave_sq):
    numerator = 1.0 + time_step * stabilizer * wave_sq
    inverse = 1.0 / (numerator + time_step * kappa_grad * wave_sq * wave_sq)
    return numerator * inverse, time_step * wave_sq * inverse


def middle(get, section_at, slab_at, fourier, lanes, twist, put):
    lane = lax.broadcasted_iota(jnp.int32, (128, 128), 1)
    row = lax.broadcasted_iota(jnp.int32, (128, 128), 0)
    packed = (lane < 32) & (section_at == 0) & (slab_at == 0)
    cos, sin = twist[0], twist[1]
    parts = []
    for s in (0, 1):
        c_re, c_im, g_re, g_im = get(s, 0, 0), get(s, 1, 0), get(s, 0, 1), get(s, 1, 1)
        c_im, g_re = jnp.where(packed, g_re, c_im), jnp.where(packed, c_im, g_re)
        parts.append((c_re, c_im, g_re, g_im))
    stacked = []
    for sigma in (0, 1):
        mixed = [a + b if sigma == 0 else a - b for a, b in zip(*parts)]
        stacked.append(
            jnp.concatenate(
                [jnp.concatenate([mixed[0], mixed[2]], 1), jnp.concatenate([mixed[1], mixed[3]], 1)], 0
            )
        )
    slot = 4 * section_at + lane // 32
    y_index = jnp.where(slot == 0, 8 * slab_at, slot + 16 * slab_at)
    x_index = row + 128 * (lane % 16)
    wave_x = wave_square(x_index, NX)
    wave_xy = wave_x + wave_square(y_index, NY)
    half_y = (2.0 * math.pi / NY * (NY // 2)) ** 2
    back = []
    for sigma in (0, 1):
        spread = product(fourier, split(stacked[sigma]), NN)
        rows = []
        for f in (0, 1):
            re, im = spread[:128, 128 * f : 128 * f + 128], spread[128:, 128 * f : 128 * f + 128]
            rows.append(jnp.concatenate([re * cos + im * sin, im * cos - re * sin], 1))
        table = (lanes[sigma, 0], lanes[sigma, 1])
        spec = product(split(jnp.concatenate(rows, 0)), table, NN)
        c_re, c_im, g_re, g_im = spec[:128, :128], spec[:128, 128:], spec[128:, :128], spec[128:, 128:]
        wave_z = wave_square(sigma + 2 * (lane // 16 % 2), NZ)
        keep, mix = rates(wave_z + wave_xy)
        keep_half, mix_half = rates(wave_z + (wave_x + half_y))
        main_re = keep * c_re - mix * jnp.where(packed, c_im, g_re)
        main_im = keep * c_im - mix * jnp.where(packed, -c_re, g_im)
        side_re = keep_half * g_re - mix_half * g_im
        side_im = keep_half * g_im + mix_half * g_re
        rows = jnp.concatenate(
            [jnp.concatenate([main_re, main_im], 1), jnp.concatenate([side_re, side_im], 1)], 0
        )
        back.append(product(split(rows), table, NT))
    for s in (0, 1):
        mixed = back[0] + back[1] if s == 0 else back[0] - back[1]
        both = []
        for f in (0, 1):
            re, im = mixed[128 * f : 128 * f + 128, :128], mixed[128 * f : 128 * f + 128, 128:]
            both.append((re * cos - im * sin, im * cos + re * sin))
        (m_re, m_im), (s_re, s_im) = both
        upper = jnp.concatenate([m_re, jnp.where(packed, s_re, m_im)], 1)
        lower = jnp.concatenate([-m_im, jnp.where(packed, -s_im, m_re)], 1)
        out = product(
            (fourier[0][:128], fourier[1][:128]), split(jnp.concatenate([upper, lower], 0)), NN
        )
        put(s, 0, out[:, :128])
        put(s, 1, out[:, 128:])


def inverse_y(get, fourier, real_rows, twist, put):
    slots = []
    for h in (0, 1):
        re, im = get(h, 0), get(h, 1)
        if h == 0:
            row = lax.broadcasted_iota(jnp.int32, (128, 128), 0)
            lane = lax.broadcasted_iota(jnp.int32, (128, 128), 1)
            single = (row == 0) & (lane < 32)
            re, im = jnp.where(single, 0.5 * re, re), jnp.where(single, 0.5 * im, im)
        rows = split(jnp.concatenate([re.T, im.T], 1))
        if h == 0:
            first = product((rows[0][:32], rows[1][:32]), real_rows, NN)
            rows = (rows[0][32:], rows[1][32:])
        out = product(rows, fourier, NN)
        slots += [out[32 * m : 32 * m + 32] for m in range(out.shape[0] // 32)]
    scale = 2.0 / CELLS
    base = [first[:, :128] * scale, first[:, 128:] * scale]
    real, imag = {}, {}
    for j in range(1, 8):
        re, im = slots[j - 1][:, :128], slots[j - 1][:, 128:]
        cos, sin = twist[j : j + 1] * scale, twist[8 + j : 9 + j] * scale
        real[j], imag[j] = re * cos - im * sin, im * cos + re * sin
    even = [
        weighted(
            [(COS16[j * a % 16], real[j]) for j in (2, 4, 6)]
            + [(-SIN16[j * a % 16], imag[j]) for j in (2, 4, 6)]
        )
        + base[a % 2]
        for a in range(8)
    ]
    cosine = [weighted([(COS16[j * a % 16], real[j]) for j in (1, 3, 5, 7)]) for a in range(4)]
    sine = [None] + [weighted([(SIN16[j * a % 16], imag[j]) for j in (1, 3, 5, 7)]) for a in range(1, 5)]
    odd = [cosine[0]] + [cosine[a] - sine[a] for a in (1, 2, 3)] + [-sine[4]]
    odd += [-cosine[a] - sine[a] for a in (3, 2, 1)]
    for a in range(8):
        put(a, even[a] + odd[a])
        put(a + 8, even[a] - odd[a])


def forward_kernel(
    c_hbm, fourier_hbm, real_hbm, twist_hbm, out_ref, bulk_ref, c_ref, fourier_ref, real_ref, twist_ref, sems
):
    sources = (c_hbm, twist_hbm, real_hbm, fourier_hbm)
    targets = (c_ref, twist_ref, real_ref, fourier_ref)
    copies = [
        pltpu.make_async_copy(source, target, sems.at[n])
        for n, (source, target) in enumerate(zip(sources, targets))
    ]
    for copy in copies:
        copy.start()

    def put(h, part, f, value):
        out_ref[pl.ds(512 * h + 2 * part + f, 128, stride=4), :] = value

    def late(n, ref):
        def read():
            copies[n].wait()
            return ref[...]

        return read

    copies[0].wait()
    field = jnp.concatenate([c_ref[0], c_ref[1]], 0)
    lanes = forward_y(field, late(3, fourier_ref), late(2, real_ref), late(1, twist_ref), put)
    bulk_ref[...] = jnp.broadcast_to(jnp.sum(lanes, 0, keepdims=True), (8, 128))


def middle_kernel(in_ref, bulk_ref, fourier_ref, lanes_ref, twist_ref, out_ref):
    def get(s, part, f):
        return in_ref[pl.ds(512 * s + 2 * part + f, 128, stride=4), :]

    def put(s, part, value):
        out_ref[pl.ds(384 * s + part, 128, stride=3), :] = value

    middle(
        get,
        lax.axis_index("section"),
        lax.axis_index("slab"),
        (fourier_ref[0], fourier_ref[1]),
        lanes_ref,
        twist_ref,
        put,
    )
    out_ref[pl.ds(2, 256, stride=3), :] = jnp.broadcast_to(bulk_ref[0:1, :], (256, 128))


def inverse_kernel(in_ref, fourier_ref, real_ref, twist_ref, out_ref, energy_ref):
    def get(h, part):
        return in_ref[pl.ds(384 * h + part, 128, stride=3), :]

    def put(a, value):
        out_ref[0, :, 128 * a : 128 * a + 128] = value[:16]
        out_ref[1, :, 128 * a : 128 * a + 128] = value[16:]

    inverse_y(
        get, (fourier_ref[0], fourier_ref[1]), (real_ref[0], real_ref[1]), twist_ref[...], put
    )
    energy_ref[...] = jnp.sum(in_ref[pl.ds(2, 256, stride=3), :], keepdims=True) * (1.0 / CELLS)


def exchange(rows):
    width = rows.shape[0] // 256
    message = rows.reshape(256, 1, 128 * width)
    return lax.all_to_all(message, ALL, split_axis=0, concat_axis=0, tiled=True).reshape(rows.shape)


def per_device(concentration):
    whole = pl.BlockSpec(memory_space=pltpu.VMEM)
    params = pltpu.CompilerParams(vmem_limit_bytes=12 << 20)
    outgoing, bulk = pl.pallas_call(
        forward_kernel,
        out_shape=(jax.ShapeDtypeStruct((1024, 128), f32), jax.ShapeDtypeStruct((8, 128), f32)),
        in_specs=[pl.BlockSpec(memory_space=pltpu.HBM)] * 4,
        out_specs=(whole, whole),
        scratch_shapes=[
            pltpu.VMEM(concentration.shape, f32),
            pltpu.VMEM(FOURIER.shape, bf16),
            pltpu.VMEM(REAL.shape, bf16),
            pltpu.VMEM(Y_TWIST.shape, f32),
            pltpu.SemaphoreType.DMA((4,)),
        ],
        compiler_params=params,
    )(concentration, FOURIER, REAL, Y_TWIST)
    columns = exchange(outgoing)
    leaving = pl.pallas_call(
        middle_kernel,
        out_shape=jax.ShapeDtypeStruct((768, 128), f32),
        in_specs=[whole] * 5,
        out_specs=whole,
        compiler_params=params,
    )(columns, bulk, FOURIER, LANES, X_TWIST)
    rows_back = exchange(leaving)
    new_field, energy = pl.pallas_call(
        inverse_kernel,
        out_shape=(jax.ShapeDtypeStruct(concentration.shape, f32), jax.ShapeDtypeStruct((1, 1), f32)),
        in_specs=[whole] * 4,
        out_specs=(whole, whole),
        compiler_params=params,
    )(rows_back, FOURIER, REAL, Y_TWIST)
    return new_field, energy.reshape(())


def solution(mesh):
    return jax.shard_map(
        per_device,
        mesh=mesh,
        in_specs=(P("section", "slab", None),),
        out_specs=(P("section", "slab", None), P()),
        check_vma=False,
    )
```

```python
import math

import jax
import jax.numpy as jnp
import ml_dtypes
import numpy as np
from jax import lax
from jax.experimental import pallas as pl
from jax.experimental.pallas import tpu as pltpu
from jax.sharding import PartitionSpec as P

ALL = ("section", "slab")
NX = 2048
NY = 2048
NZ = 4
CELLS = NX * NY * NZ
time_step = 100.0
kappa_grad = 2.0
stabilizer = 8.0
f32 = jnp.float32
bf16 = jnp.bfloat16


def halves(matrix):
    high = matrix.astype(np.float32).astype(ml_dtypes.bfloat16)
    low = (matrix - high.astype(np.float64)).astype(np.float32).astype(ml_dtypes.bfloat16)
    return np.stack([high, low])


def fourier_table():
    index = np.arange(128)
    angle = 2.0 * np.pi * (np.outer(index, index) % 128) / 128
    return halves(np.block([[np.cos(angle), np.sin(angle)], [-np.sin(angle), np.cos(angle)]]))


def real_table():
    angle = 2.0 * np.pi * (np.outer(np.arange(128), np.arange(256)) % 256) / 256
    lower = -np.sin(angle)
    lower[0] = 1.0 - 2.0 * (np.arange(256) % 2)
    return halves(np.concatenate([np.cos(angle), lower], 0))


def lane_table(parity):
    z_at, x_at = np.arange(2)[:, None, None, None], np.arange(16)[None, :, None, None]
    t_at, q_at = np.arange(2)[None, None, :, None], np.arange(16)[None, None, None, :]
    turn = (4 * parity * z_at + 8 * t_at * z_at + x_at * q_at) % 16
    value = np.exp(-2j * np.pi * turn / 16).reshape(32, 32)
    value = np.kron(np.eye(4), value)
    return halves(np.block([[value.real, value.imag], [-value.imag, value.real]]))


def y_twist_table():
    angle = 2.0 * np.pi * np.outer(np.arange(8), np.arange(128)) / 2048
    return np.concatenate([np.cos(angle), np.sin(angle)], 0).astype(np.float32)


def x_twist_table():
    angle = 2.0 * np.pi * np.outer(np.arange(128), np.arange(128) % 16) / 2048
    return np.stack([np.cos(angle), np.sin(angle)]).astype(np.float32)


FOURIER = fourier_table()
REAL = real_table()
LANES = np.stack([lane_table(0), lane_table(1)])
Y_TWIST = y_twist_table()
X_TWIST = x_twist_table()
COS16 = [math.cos(2.0 * math.pi * m / 16) for m in range(16)]
SIN16 = [math.sin(2.0 * math.pi * m / 16) for m in range(16)]


def split(value):
    high = value.astype(bf16)
    return high, (value - high.astype(f32)).astype(bf16)


NN = (((1,), (0,)), ((), ()))
NT = (((1,), (1,)), ((), ()))


def product(left, right, pattern):
    def one(a, b):
        return lax.dot_general(a, b, pattern, preferred_element_type=f32)

    return one(left[0], right[0]) + (one(left[1], right[0]) + one(left[0], right[1]))


def weighted(terms):
    total = None
    for weight, value in terms:
        if abs(weight) < 1e-12:
            continue
        if abs(weight - 1.0) < 1e-12:
            part = value
        elif abs(weight + 1.0) < 1e-12:
            part = -value
        else:
            part = value * weight
        total = part if total is None else total + part
    return total


def y_slots(field):
    at = [field[:, 128 * a : 128 * a + 128] for a in range(16)]
    add = [at[a] + at[a + 8] for a in range(8)]
    sub = [at[a] - at[a + 8] for a in range(8)]
    slots = [
        jnp.concatenate([(add[0] + add[4]) + (add[2] + add[6]), (add[1] + add[5]) + (add[3] + add[7])], 1)
    ]
    real, imag = {}, {}
    for j in (2, 4, 6):
        real[j] = weighted([(COS16[j * a % 16], add[a]) for a in range(8)])
        imag[j] = weighted([(-SIN16[j * a % 16], add[a]) for a in range(8)])
    minus = [None] + [sub[a] - sub[8 - a] for a in (1, 2, 3)]
    plus = [None] + [sub[a] + sub[8 - a] for a in (1, 2, 3)] + [sub[4]]
    for j in (1, 3, 5, 7):
        real[j] = weighted([(1.0, sub[0])] + [(COS16[j * a % 16], minus[a]) for a in (1, 2, 3)])
        imag[j] = weighted([(-SIN16[j * a % 16], plus[a]) for a in (1, 2, 3, 4)])
    return slots + [(real[j], imag[j]) for j in range(1, 8)]


def forward_y(field, read_fourier, read_real, read_twist, put):
    squared = field * field
    bulk = squared * (0.25 * squared - 0.5)
    cubic = squared * field - field
    both = [y_slots(field), y_slots(cubic)]
    twist = read_twist()
    for slots in both:
        for j in range(1, 8):
            real, imag = slots[j]
            cos, sin = twist[j : j + 1], twist[8 + j : 9 + j]
            slots[j] = jnp.concatenate([real * cos + imag * sin, imag * cos - real * sin], 1)
    real_rows = read_real()
    fourier = read_fourier()
    for f, slots in enumerate(both):
        first = product(real_rows, split(slots[0]), NT)
        for h in (0, 1):
            rows = jnp.concatenate(slots[4 * h : 4 * h + 4], 0)
            out = product(fourier, split(rows), NT)
            if h == 0:
                lane = lax.broadcasted_iota(jnp.int32, (256, 128), 1)
                wide = jnp.concatenate([first] * 4, 1)
                out = jnp.where(lane < 32, wide, out)
            put(h, 0, f, out[:128])
            put(h, 1, f, out[128:])
    lanes = sum(bulk[:, 128 * a : 128 * a + 128] for a in range(16))
    return lanes


def wave_square(index, length):
    signed = jnp.where(2 * index >= length, index - length, index)
    phase_angle = signed.astype(f32) * (2.0 * math.pi / length)
    return phase_angle * phase_angle


def rates(wave_sq):
    numerator = 1.0 + time_step * stabilizer * wave_sq
    inverse = 1.0 / (numerator + time_step * kappa_grad * wave_sq * wave_sq)
    return numerator * inverse, time_step * wave_sq * inverse


def middle(get, section_at, slab_at, fourier, lanes, twist, put):
    lane = lax.broadcasted_iota(jnp.int32, (128, 128), 1)
    row = lax.broadcasted_iota(jnp.int32, (128, 128), 0)
    packed = (lane < 32) & (section_at == 0) & (slab_at == 0)
    cos, sin = twist[0], twist[1]
    parts = []
    for s in (0, 1):
        c_re, c_im, g_re, g_im = get(s, 0, 0), get(s, 1, 0), get(s, 0, 1), get(s, 1, 1)
        c_im, g_re = jnp.where(packed, g_re, c_im), jnp.where(packed, c_im, g_re)
        parts.append((c_re, c_im, g_re, g_im))
    stacked = []
    for sigma in (0, 1):
        mixed = [a + b if sigma == 0 else a - b for a, b in zip(*parts)]
        stacked.append(
            jnp.concatenate(
                [jnp.concatenate([mixed[0], mixed[2]], 1), jnp.concatenate([mixed[1], mixed[3]], 1)], 0
            )
        )
    slot = 4 * section_at + lane // 32
    y_index = jnp.where(slot == 0, 8 * slab_at, slot + 16 * slab_at)
    x_index = row + 128 * (lane % 16)
    wave_x = wave_square(x_index, NX)
    wave_xy = wave_x + wave_square(y_index, NY)
    half_y = (2.0 * math.pi / NY * (NY // 2)) ** 2
    back = []
    for sigma in (0, 1):
        spread = product(fourier, split(stacked[sigma]), NN)
        rows = []
        for f in (0, 1):
            re, im = spread[:128, 128 * f : 128 * f + 128], spread[128:, 128 * f : 128 * f + 128]
            rows.append(jnp.concatenate([re * cos + im * sin, im * cos - re * sin], 1))
        table = (lanes[sigma, 0], lanes[sigma, 1])
        spec = product(split(jnp.concatenate(rows, 0)), table, NN)
        c_re, c_im, g_re, g_im = spec[:128, :128], spec[:128, 128:], spec[128:, :128], spec[128:, 128:]
        wave_z = wave_square(sigma + 2 * (lane // 16 % 2), NZ)
        keep, mix = rates(wave_z + wave_xy)
        keep_half, mix_half = rates(wave_z + (wave_x + half_y))
        main_re = keep * c_re - mix * jnp.where(packed, c_im, g_re)
        main_im = keep * c_im - mix * jnp.where(packed, -c_re, g_im)
        side_re = keep_half * g_re - mix_half * g_im
        side_im = keep_half * g_im + mix_half * g_re
        rows = jnp.concatenate(
            [jnp.concatenate([main_re, main_im], 1), jnp.concatenate([side_re, side_im], 1)], 0
        )
        back.append(product(split(rows), table, NT))
    for s in (0, 1):
        mixed = back[0] + back[1] if s == 0 else back[0] - back[1]
        both = []
        for f in (0, 1):
            re, im = mixed[128 * f : 128 * f + 128, :128], mixed[128 * f : 128 * f + 128, 128:]
            both.append((re * cos - im * sin, im * cos + re * sin))
        (m_re, m_im), (s_re, s_im) = both
        upper = jnp.concatenate([m_re, jnp.where(packed, s_re, m_im)], 1)
        lower = jnp.concatenate([-m_im, jnp.where(packed, -s_im, m_re)], 1)
        out = product(
            (fourier[0][:128], fourier[1][:128]), split(jnp.concatenate([upper, lower], 0)), NN
        )
        put(s, 0, out[:, :128])
        put(s, 1, out[:, 128:])


def inverse_y(get, fourier, real_rows, twist, put):
    slots = []
    for h in (0, 1):
        re, im = get(h, 0), get(h, 1)
        if h == 0:
            row = lax.broadcasted_iota(jnp.int32, (128, 128), 0)
            lane = lax.broadcasted_iota(jnp.int32, (128, 128), 1)
            single = (row == 0) & (lane < 32)
            re, im = jnp.where(single, 0.5 * re, re), jnp.where(single, 0.5 * im, im)
        rows = split(jnp.concatenate([re.T, im.T], 1))
        if h == 0:
            first = product((rows[0][:32], rows[1][:32]), real_rows, NN)
            rows = (rows[0][32:], rows[1][32:])
        out = product(rows, fourier, NN)
        slots += [out[32 * m : 32 * m + 32] for m in range(out.shape[0] // 32)]
    scale = 2.0 / CELLS
    base = [first[:, :128] * scale, first[:, 128:] * scale]
    real, imag = {}, {}
    for j in range(1, 8):
        re, im = slots[j - 1][:, :128], slots[j - 1][:, 128:]
        cos, sin = twist[j : j + 1] * scale, twist[8 + j : 9 + j] * scale
        real[j], imag[j] = re * cos - im * sin, im * cos + re * sin
    even = [
        weighted(
            [(COS16[j * a % 16], real[j]) for j in (2, 4, 6)]
            + [(-SIN16[j * a % 16], imag[j]) for j in (2, 4, 6)]
        )
        + base[a % 2]
        for a in range(8)
    ]
    cosine = [weighted([(COS16[j * a % 16], real[j]) for j in (1, 3, 5, 7)]) for a in range(4)]
    sine = [None] + [weighted([(SIN16[j * a % 16], imag[j]) for j in (1, 3, 5, 7)]) for a in range(1, 5)]
    odd = [cosine[0]] + [cosine[a] - sine[a] for a in (1, 2, 3)] + [-sine[4]]
    odd += [-cosine[a] - sine[a] for a in (3, 2, 1)]
    for a in range(8):
        put(a, even[a] + odd[a])
        put(a + 8, even[a] - odd[a])


def forward_kernel(
    c_hbm, fourier_hbm, real_hbm, twist_hbm, out_ref, bulk_ref, c_ref, fourier_ref, real_ref, twist_ref, sems
):
    sources = (c_hbm, twist_hbm, real_hbm, fourier_hbm)
    targets = (c_ref, twist_ref, real_ref, fourier_ref)
    copies = [
        pltpu.make_async_copy(source, target, sems.at[n])
        for n, (source, target) in enumerate(zip(sources, targets))
    ]
    for copy in copies:
        copy.start()

    def put(h, part, f, value):
        out_ref[pl.ds(512 * h + 2 * part + f, 128, stride=4), :] = value

    def late(n, ref):
        def read():
            copies[n].wait()
            return ref[...]

        return read

    copies[0].wait()
    field = jnp.concatenate([c_ref[0], c_ref[1]], 0)
    lanes = forward_y(field, late(3, fourier_ref), late(2, real_ref), late(1, twist_ref), put)
    bulk_ref[...] = jnp.broadcast_to(jnp.sum(lanes, 0, keepdims=True), (8, 128))


def middle_kernel(in_ref, bulk_ref, fourier_ref, lanes_ref, twist_ref, out_ref):
    def get(s, part, f):
        return in_ref[pl.ds(512 * s + 2 * part + f, 128, stride=4), :]

    def put(s, part, value):
        out_ref[pl.ds(384 * s + part, 128, stride=3), :] = value

    middle(
        get,
        lax.axis_index("section"),
        lax.axis_index("slab"),
        (fourier_ref[0], fourier_ref[1]),
        lanes_ref,
        twist_ref,
        put,
    )
    out_ref[pl.ds(2, 256, stride=3), :] = jnp.broadcast_to(bulk_ref[0:1, :], (256, 128))


def inverse_kernel(in_ref, fourier_ref, real_ref, twist_ref, out_ref, energy_ref):
    def get(h, part):
        return in_ref[pl.ds(384 * h + part, 128, stride=3), :]

    def put(a, value):
        out_ref[0, :, 128 * a : 128 * a + 128] = value[:16]
        out_ref[1, :, 128 * a : 128 * a + 128] = value[16:]

    inverse_y(
        get, (fourier_ref[0], fourier_ref[1]), (real_ref[0], real_ref[1]), twist_ref[...], put
    )
    energy_ref[...] = jnp.sum(in_ref[pl.ds(2, 256, stride=3), :], keepdims=True) * (1.0 / CELLS)


def exchange(rows):
    width = rows.shape[0] // 256
    message = rows.reshape(256, 1, 128 * width)
    return lax.all_to_all(message, ALL, split_axis=0, concat_axis=0, tiled=True).reshape(rows.shape)


def per_device(concentration):
    whole = pl.BlockSpec(memory_space=pltpu.VMEM)
    params = pltpu.CompilerParams(vmem_limit_bytes=12 << 20)
    outgoing, bulk = pl.pallas_call(
        forward_kernel,
        out_shape=(pltpu.VMEM((1024, 128), f32), pltpu.VMEM((8, 128), f32)),
        in_specs=[pl.BlockSpec(memory_space=pltpu.HBM)] * 4,
        out_specs=(whole, whole),
        scratch_shapes=[
            pltpu.VMEM(concentration.shape, f32),
            pltpu.VMEM(FOURIER.shape, bf16),
            pltpu.VMEM(REAL.shape, bf16),
            pltpu.VMEM(Y_TWIST.shape, f32),
            pltpu.SemaphoreType.DMA((4,)),
        ],
        compiler_params=params,
    )(*[pltpu.with_memory_space_constraint(a, pltpu.HBM) for a in (concentration, FOURIER, REAL, Y_TWIST)])
    columns = exchange(outgoing)
    leaving = pl.pallas_call(
        middle_kernel,
        out_shape=jax.ShapeDtypeStruct((768, 128), f32),
        in_specs=[whole] * 5,
        out_specs=whole,
        compiler_params=params,
    )(columns, bulk, FOURIER, LANES, X_TWIST)
    rows_back = exchange(leaving)
    new_field, energy = pl.pallas_call(
        inverse_kernel,
        out_shape=(jax.ShapeDtypeStruct(concentration.shape, f32), jax.ShapeDtypeStruct((1, 1), f32)),
        in_specs=[whole] * 4,
        out_specs=(whole, whole),
        compiler_params=params,
    )(rows_back, FOURIER, REAL, Y_TWIST)
    return new_field, energy.reshape(())


def solution(mesh):
    return jax.shard_map(
        per_device,
        mesh=mesh,
        in_specs=(P("section", "slab", None),),
        out_specs=(P("section", "slab", None), P()),
        check_vma=False,
    )
```

```python
import math

import jax
import jax.numpy as jnp
import ml_dtypes
import numpy as np
from jax import lax
from jax.experimental import pallas as pl
from jax.experimental.pallas import tpu as pltpu
from jax.sharding import Mesh
from jax.sharding import PartitionSpec as P

SLAB = ("slab_y", "slab_x", "slab_z", "slab_core")
ALL = ("section", "slab_z", "slab_y", "slab_x", "slab_core")
NX = 2048
NY = 2048
NZ = 4
CELLS = NX * NY * NZ
time_step = 100.0
kappa_grad = 2.0
stabilizer = 8.0
f32 = jnp.float32
bf16 = jnp.bfloat16


def halves(matrix):
    high = matrix.astype(np.float32).astype(ml_dtypes.bfloat16)
    low = (matrix - high.astype(np.float64)).astype(np.float32).astype(ml_dtypes.bfloat16)
    return np.stack([high, low])


def fourier_table():
    index = np.arange(128)
    angle = 2.0 * np.pi * (np.outer(index, index) % 128) / 128
    return halves(np.block([[np.cos(angle), np.sin(angle)], [-np.sin(angle), np.cos(angle)]]))


def slab_order():
    return np.arange(128).reshape(4, 2, 8, 2).transpose(2, 0, 1, 3).reshape(128)


def real_table():
    angle = 2.0 * np.pi * (np.outer(np.arange(128), np.arange(256)) % 256) / 256
    lower = -np.sin(angle)
    lower[0] = 1.0 - 2.0 * (np.arange(256) % 2)
    return halves(np.concatenate([np.cos(angle), lower], 0))


def lane_table(parity):
    z_at, x_at = np.arange(2)[:, None, None, None], np.arange(16)[None, :, None, None]
    t_at, q_at = np.arange(2)[None, None, :, None], np.arange(16)[None, None, None, :]
    turn = (4 * parity * z_at + 8 * t_at * z_at + x_at * q_at) % 16
    value = np.exp(-2j * np.pi * turn / 16).reshape(32, 32)
    value = np.kron(np.eye(4), value)
    return halves(np.block([[value.real, value.imag], [-value.imag, value.real]]))


def y_twist_table():
    angle = 2.0 * np.pi * np.outer(np.arange(8), np.arange(128)) / 2048
    return np.concatenate([np.cos(angle), np.sin(angle)], 0).astype(np.float32)


def x_twist_table():
    angle = 2.0 * np.pi * np.outer(np.arange(128), np.arange(128) % 16) / 2048
    return np.stack([np.cos(angle), np.sin(angle)]).astype(np.float32)


FOURIER = fourier_table()
ORDER = slab_order()
GATHER = FOURIER[:, :, np.concatenate([ORDER, 128 + ORDER])]
SPREAD = FOURIER[:, ORDER, :]
REAL = real_table()
LANES = np.stack([lane_table(0), lane_table(1)])
Y_TWIST = y_twist_table()
X_TWIST = x_twist_table()
COS16 = [math.cos(2.0 * math.pi * m / 16) for m in range(16)]
SIN16 = [math.sin(2.0 * math.pi * m / 16) for m in range(16)]


def split(value):
    high = value.astype(bf16)
    return high, (value - high.astype(f32)).astype(bf16)


NN = (((1,), (0,)), ((), ()))
NT = (((1,), (1,)), ((), ()))


def product(left, right, pattern):
    def one(a, b):
        return lax.dot_general(a, b, pattern, preferred_element_type=f32)

    return one(left[0], right[0]) + (one(left[1], right[0]) + one(left[0], right[1]))


def weighted(terms):
    total = None
    for weight, value in terms:
        if abs(weight) < 1e-12:
            continue
        if abs(weight - 1.0) < 1e-12:
            part = value
        elif abs(weight + 1.0) < 1e-12:
            part = -value
        else:
            part = value * weight
        total = part if total is None else total + part
    return total


def y_slots(field):
    at = [field[:, 128 * a : 128 * a + 128] for a in range(16)]
    add = [at[a] + at[a + 8] for a in range(8)]
    sub = [at[a] - at[a + 8] for a in range(8)]
    slots = [
        jnp.concatenate([(add[0] + add[4]) + (add[2] + add[6]), (add[1] + add[5]) + (add[3] + add[7])], 1)
    ]
    real, imag = {}, {}
    for j in (2, 4, 6):
        real[j] = weighted([(COS16[j * a % 16], add[a]) for a in range(8)])
        imag[j] = weighted([(-SIN16[j * a % 16], add[a]) for a in range(8)])
    minus = [None] + [sub[a] - sub[8 - a] for a in (1, 2, 3)]
    plus = [None] + [sub[a] + sub[8 - a] for a in (1, 2, 3)] + [sub[4]]
    for j in (1, 3, 5, 7):
        real[j] = weighted([(1.0, sub[0])] + [(COS16[j * a % 16], minus[a]) for a in (1, 2, 3)])
        imag[j] = weighted([(-SIN16[j * a % 16], plus[a]) for a in (1, 2, 3, 4)])
    return slots + [(real[j], imag[j]) for j in range(1, 8)]


def forward_y(field, read_fourier, read_real, read_twist, put):
    squared = field * field
    bulk = squared * (0.25 * squared - 0.5)
    cubic = squared * field - field
    both = [y_slots(field), y_slots(cubic)]
    twist = read_twist()
    for slots in both:
        for j in range(1, 8):
            real, imag = slots[j]
            cos, sin = twist[j : j + 1], twist[8 + j : 9 + j]
            slots[j] = jnp.concatenate([real * cos + imag * sin, imag * cos - real * sin], 1)
    real_rows = read_real()
    fourier = read_fourier()
    for f, slots in enumerate(both):
        first = product(real_rows, split(slots[0]), NT)
        for h in (0, 1):
            rows = jnp.concatenate(slots[4 * h : 4 * h + 4], 0)
            out = product(fourier, split(rows), NT)
            if h == 0:
                lane = lax.broadcasted_iota(jnp.int32, (256, 128), 1)
                wide = jnp.concatenate([first] * 4, 1)
                out = jnp.where(lane < 32, wide, out)
            put(h, 0, f, out[:128])
            put(h, 1, f, out[128:])
    lanes = sum(bulk[:, 128 * a : 128 * a + 128] for a in range(16))
    return lanes


def wave_square(index, length):
    signed = jnp.where(2 * index >= length, index - length, index)
    phase_angle = signed.astype(f32) * (2.0 * math.pi / length)
    return phase_angle * phase_angle


def rates(wave_sq):
    numerator = 1.0 + time_step * stabilizer * wave_sq
    inverse = 1.0 / (numerator + time_step * kappa_grad * wave_sq * wave_sq)
    return numerator * inverse, time_step * wave_sq * inverse


def middle(get, section_at, lane_at, gather, lanes, spread_table, twist, put):
    lane = lax.broadcasted_iota(jnp.int32, (128, 128), 1)
    row = lax.broadcasted_iota(jnp.int32, (128, 128), 0)
    packed = (lane < 32) & (section_at == 0) & (lane_at == 0)
    cos, sin = twist[0], twist[1]
    parts = []
    for s in (0, 1):
        c_re, c_im, g_re, g_im = get(s, 0, 0), get(s, 1, 0), get(s, 0, 1), get(s, 1, 1)
        c_im, g_re = jnp.where(packed, g_re, c_im), jnp.where(packed, c_im, g_re)
        parts.append((c_re, c_im, g_re, g_im))
    stacked = []
    for sigma in (0, 1):
        mixed = [a + b if sigma == 0 else a - b for a, b in zip(*parts)]
        stacked.append(
            jnp.concatenate(
                [jnp.concatenate([mixed[0], mixed[2]], 1), jnp.concatenate([mixed[1], mixed[3]], 1)], 0
            )
        )
    slot = 4 * section_at + lane // 32
    y_index = jnp.where(slot == 0, 8 * lane_at, slot + 16 * lane_at)
    x_index = row + 128 * (lane % 16)
    wave_x = wave_square(x_index, NX)
    wave_xy = wave_x + wave_square(y_index, NY)
    half_y = (2.0 * math.pi / NY * (NY // 2)) ** 2
    back = []
    for sigma in (0, 1):
        spread = product(gather, split(stacked[sigma]), NN)
        rows = []
        for f in (0, 1):
            re, im = spread[:128, 128 * f : 128 * f + 128], spread[128:, 128 * f : 128 * f + 128]
            rows.append(jnp.concatenate([re * cos + im * sin, im * cos - re * sin], 1))
        table = (lanes[sigma, 0], lanes[sigma, 1])
        spec = product(split(jnp.concatenate(rows, 0)), table, NN)
        c_re, c_im, g_re, g_im = spec[:128, :128], spec[:128, 128:], spec[128:, :128], spec[128:, 128:]
        wave_z = wave_square(sigma + 2 * (lane // 16 % 2), NZ)
        keep, mix = rates(wave_z + wave_xy)
        keep_half, mix_half = rates(wave_z + (wave_x + half_y))
        main_re = keep * c_re - mix * jnp.where(packed, c_im, g_re)
        main_im = keep * c_im - mix * jnp.where(packed, -c_re, g_im)
        side_re = keep_half * g_re - mix_half * g_im
        side_im = keep_half * g_im + mix_half * g_re
        rows = jnp.concatenate(
            [jnp.concatenate([main_re, main_im], 1), jnp.concatenate([side_re, side_im], 1)], 0
        )
        back.append(product(split(rows), table, NT))
    for s in (0, 1):
        mixed = back[0] + back[1] if s == 0 else back[0] - back[1]
        both = []
        for f in (0, 1):
            re, im = mixed[128 * f : 128 * f + 128, :128], mixed[128 * f : 128 * f + 128, 128:]
            both.append((re * cos - im * sin, im * cos + re * sin))
        (m_re, m_im), (s_re, s_im) = both
        upper = jnp.concatenate([m_re, jnp.where(packed, s_re, m_im)], 1)
        lower = jnp.concatenate([-m_im, jnp.where(packed, -s_im, m_re)], 1)
        out = product(spread_table, split(jnp.concatenate([upper, lower], 0)), NN)
        put(s, 0, out[:, :128])
        put(s, 1, out[:, 128:])


def inverse_y(get, fourier, real_rows, twist, put):
    slots = []
    for h in (0, 1):
        re, im = get(h, 0), get(h, 1)
        if h == 0:
            row = lax.broadcasted_iota(jnp.int32, (128, 128), 0)
            lane = lax.broadcasted_iota(jnp.int32, (128, 128), 1)
            single = (row == 0) & (lane < 32)
            re, im = jnp.where(single, 0.5 * re, re), jnp.where(single, 0.5 * im, im)
        rows = split(jnp.concatenate([re.T, im.T], 1))
        if h == 0:
            first = product((rows[0][:32], rows[1][:32]), real_rows, NN)
            rows = (rows[0][32:], rows[1][32:])
        out = product(rows, fourier, NN)
        slots += [out[32 * m : 32 * m + 32] for m in range(out.shape[0] // 32)]
    scale = 2.0 / CELLS
    base = [first[:, :128] * scale, first[:, 128:] * scale]
    real, imag = {}, {}
    for j in range(1, 8):
        re, im = slots[j - 1][:, :128], slots[j - 1][:, 128:]
        cos, sin = twist[j : j + 1] * scale, twist[8 + j : 9 + j] * scale
        real[j], imag[j] = re * cos - im * sin, im * cos + re * sin
    even = [
        weighted(
            [(COS16[j * a % 16], real[j]) for j in (2, 4, 6)]
            + [(-SIN16[j * a % 16], imag[j]) for j in (2, 4, 6)]
        )
        + base[a % 2]
        for a in range(8)
    ]
    cosine = [weighted([(COS16[j * a % 16], real[j]) for j in (1, 3, 5, 7)]) for a in range(4)]
    sine = [None] + [weighted([(SIN16[j * a % 16], imag[j]) for j in (1, 3, 5, 7)]) for a in range(1, 5)]
    odd = [cosine[0]] + [cosine[a] - sine[a] for a in (1, 2, 3)] + [-sine[4]]
    odd += [-cosine[a] - sine[a] for a in (3, 2, 1)]
    for a in range(8):
        put(a, even[a] + odd[a])
        put(a + 8, even[a] - odd[a])


def forward_kernel(
    c_hbm, fourier_hbm, real_hbm, twist_hbm, out_ref, bulk_ref, c_ref, fourier_ref, real_ref, twist_ref, sems
):
    sources = (c_hbm, twist_hbm, real_hbm, fourier_hbm)
    targets = (c_ref, twist_ref, real_ref, fourier_ref)
    copies = [
        pltpu.make_async_copy(source, target, sems.at[n])
        for n, (source, target) in enumerate(zip(sources, targets))
    ]
    for copy in copies:
        copy.start()

    def put(h, part, f, value):
        out_ref[pl.ds(512 * h + 2 * part + f, 128, stride=4), :] = value

    def late(n, ref):
        def read():
            copies[n].wait()
            return ref[...]

        return read

    copies[0].wait()
    field = jnp.concatenate([c_ref[0], c_ref[1]], 0)
    lanes = forward_y(field, late(3, fourier_ref), late(2, real_ref), late(1, twist_ref), put)
    bulk_ref[...] = jnp.broadcast_to(jnp.sum(lanes, 0, keepdims=True), (8, 128))


def middle_kernel(in_ref, bulk_ref, gather_ref, lanes_ref, spread_ref, twist_ref, out_ref):
    def get(s, part, f):
        return in_ref[pl.ds(512 * s + 2 * part + f, 128, stride=4), :]

    def put(s, part, value):
        out_ref[pl.ds(384 * s + part, 128, stride=3), :] = value

    middle(
        get,
        lax.axis_index("section"),
        16 * lax.axis_index("slab_z")
        + 4 * lax.axis_index("slab_y")
        + 2 * lax.axis_index("slab_x")
        + lax.axis_index("slab_core"),
        (gather_ref[0], gather_ref[1]),
        lanes_ref,
        (spread_ref[0], spread_ref[1]),
        twist_ref,
        put,
    )
    out_ref[pl.ds(2, 256, stride=3), :] = jnp.broadcast_to(bulk_ref[0:1, :], (256, 128))


def inverse_kernel(in_ref, fourier_ref, real_ref, twist_ref, out_ref, energy_ref):
    def get(h, part):
        return in_ref[pl.ds(384 * h + part, 128, stride=3), :]

    def put(a, value):
        out_ref[0, :, 128 * a : 128 * a + 128] = value[:16]
        out_ref[1, :, 128 * a : 128 * a + 128] = value[16:]

    inverse_y(
        get, (fourier_ref[0], fourier_ref[1]), (real_ref[0], real_ref[1]), twist_ref[...], put
    )
    energy_ref[...] = jnp.sum(in_ref[pl.ds(2, 256, stride=3), :], keepdims=True) * (1.0 / CELLS)


def exchange(rows):
    width = rows.shape[0] // 256
    message = rows.reshape(256, 1, 128 * width)
    return lax.all_to_all(message, ALL, split_axis=0, concat_axis=0, tiled=True).reshape(rows.shape)


def per_device(concentration):
    whole = pl.BlockSpec(memory_space=pltpu.VMEM)
    params = pltpu.CompilerParams(vmem_limit_bytes=12 << 20)
    outgoing, bulk = pl.pallas_call(
        forward_kernel,
        out_shape=(pltpu.VMEM((1024, 128), f32), pltpu.VMEM((8, 128), f32)),
        in_specs=[pl.BlockSpec(memory_space=pltpu.HBM)] * 4,
        out_specs=(whole, whole),
        scratch_shapes=[
            pltpu.VMEM(concentration.shape, f32),
            pltpu.VMEM(FOURIER.shape, bf16),
            pltpu.VMEM(REAL.shape, bf16),
            pltpu.VMEM(Y_TWIST.shape, f32),
            pltpu.SemaphoreType.DMA((4,)),
        ],
        compiler_params=params,
    )(*[pltpu.with_memory_space_constraint(a, pltpu.HBM) for a in (concentration, FOURIER, REAL, Y_TWIST)])
    columns = exchange(outgoing)
    leaving = pl.pallas_call(
        middle_kernel,
        out_shape=jax.ShapeDtypeStruct((768, 128), f32),
        in_specs=[whole] * 6,
        out_specs=whole,
        compiler_params=params,
    )(columns, bulk, GATHER, LANES, SPREAD, X_TWIST)
    rows_back = exchange(leaving)
    new_field, energy = pl.pallas_call(
        inverse_kernel,
        out_shape=(jax.ShapeDtypeStruct(concentration.shape, f32), jax.ShapeDtypeStruct((1, 1), f32)),
        in_specs=[whole] * 4,
        out_specs=(whole, whole),
        compiler_params=params,
    )(rows_back, FOURIER, REAL, Y_TWIST)
    return new_field, energy.reshape(())


def solution(mesh):
    finer = Mesh(mesh.devices.reshape(2, 4, 2, 8, 2), ("section",) + SLAB)
    return jax.shard_map(
        per_device,
        mesh=finer,
        in_specs=(P("section", SLAB, None),),
        out_specs=(P("section", SLAB, None), P()),
        check_vma=False,
    )
```

```python
import math

import jax
import jax.numpy as jnp
import ml_dtypes
import numpy as np
from jax import lax
from jax.experimental import pallas as pl
from jax.experimental.pallas import tpu as pltpu
from jax.sharding import Mesh
from jax.sharding import PartitionSpec as P

SLAB = ("slab_y", "slab_x", "slab_z", "slab_core")
ALL = ("section", "slab_z", "slab_y", "slab_x", "slab_core")
NX = 2048
NY = 2048
NZ = 4
CELLS = NX * NY * NZ
time_step = 100.0
kappa_grad = 2.0
stabilizer = 8.0
f32 = jnp.float32
bf16 = jnp.bfloat16


def halves(matrix):
    high = matrix.astype(np.float32).astype(ml_dtypes.bfloat16)
    low = (matrix - high.astype(np.float64)).astype(np.float32).astype(ml_dtypes.bfloat16)
    return np.stack([high, low])


def fourier_table():
    index = np.arange(128)
    angle = 2.0 * np.pi * (np.outer(index, index) % 128) / 128
    return halves(np.block([[np.cos(angle), np.sin(angle)], [-np.sin(angle), np.cos(angle)]]))


def slab_order():
    return np.arange(128).reshape(4, 2, 8, 2).transpose(2, 0, 1, 3).reshape(128)


def real_table():
    angle = 2.0 * np.pi * (np.outer(np.arange(128), np.arange(256)) % 256) / 256
    lower = -np.sin(angle)
    lower[0] = 1.0 - 2.0 * (np.arange(256) % 2)
    return halves(np.concatenate([np.cos(angle), lower], 0))


def lane_table(parity):
    z_at, x_at = np.arange(2)[:, None, None, None], np.arange(16)[None, :, None, None]
    t_at, q_at = np.arange(2)[None, None, :, None], np.arange(16)[None, None, None, :]
    turn = (4 * parity * z_at + 8 * t_at * z_at + x_at * q_at) % 16
    value = np.exp(-2j * np.pi * turn / 16).reshape(32, 32)
    value = np.kron(np.eye(4), value)
    return halves(np.block([[value.real, value.imag], [-value.imag, value.real]]))


def y_twist_table():
    angle = 2.0 * np.pi * np.outer(np.arange(8), np.arange(128)) / 2048
    return np.concatenate([np.cos(angle), np.sin(angle)], 0).astype(np.float32)


def x_twist_table():
    angle = 2.0 * np.pi * np.outer(np.arange(128), np.arange(128) % 16) / 2048
    return np.stack([np.cos(angle), np.sin(angle)]).astype(np.float32)


FOURIER = fourier_table()
ORDER = slab_order()
GATHER = FOURIER[:, :, np.concatenate([ORDER, 128 + ORDER])]
SPREAD = FOURIER[:, ORDER, :]
REAL = real_table()
LANES = np.stack([lane_table(0), lane_table(1)])
FOURIER_T = FOURIER.transpose(0, 2, 1)
REAL_T = REAL.transpose(0, 2, 1)
Y_TWIST = y_twist_table()
X_TWIST = x_twist_table()
COS16 = [math.cos(2.0 * math.pi * m / 16) for m in range(16)]
SIN16 = [math.sin(2.0 * math.pi * m / 16) for m in range(16)]


def split(value):
    high = value.astype(bf16)
    return high, (value - high.astype(f32)).astype(bf16)


NN = (((1,), (0,)), ((), ()))
NT = (((1,), (1,)), ((), ()))


def product(left, right, pattern):
    total = left[0].shape[0]
    both = lax.dot_general(
        jnp.concatenate(left, 0), right[0], pattern, preferred_element_type=f32
    )
    rest = lax.dot_general(left[0], right[1], pattern, preferred_element_type=f32)
    return both[:total] + (both[total:] + rest)


def weighted(terms):
    total = None
    for weight, value in terms:
        if abs(weight) < 1e-12:
            continue
        if abs(weight - 1.0) < 1e-12:
            part = value
        elif abs(weight + 1.0) < 1e-12:
            part = -value
        else:
            part = value * weight
        total = part if total is None else total + part
    return total


def y_slots(field):
    at = [field[:, 128 * a : 128 * a + 128] for a in range(16)]
    add = [at[a] + at[a + 8] for a in range(8)]
    sub = [at[a] - at[a + 8] for a in range(8)]
    slots = [
        jnp.concatenate([(add[0] + add[4]) + (add[2] + add[6]), (add[1] + add[5]) + (add[3] + add[7])], 1)
    ]
    real, imag = {}, {}
    for j in (2, 4, 6):
        real[j] = weighted([(COS16[j * a % 16], add[a]) for a in range(8)])
        imag[j] = weighted([(-SIN16[j * a % 16], add[a]) for a in range(8)])
    minus = [None] + [sub[a] - sub[8 - a] for a in (1, 2, 3)]
    plus = [None] + [sub[a] + sub[8 - a] for a in (1, 2, 3)] + [sub[4]]
    for j in (1, 3, 5, 7):
        real[j] = weighted([(1.0, sub[0])] + [(COS16[j * a % 16], minus[a]) for a in (1, 2, 3)])
        imag[j] = weighted([(-SIN16[j * a % 16], plus[a]) for a in (1, 2, 3, 4)])
    return slots + [(real[j], imag[j]) for j in range(1, 8)]


def forward_y(field, read_fourier, read_real, read_twist, put):
    squared = field * field
    bulk = squared * (0.25 * squared - 0.5)
    cubic = squared * field - field
    both = [y_slots(field), y_slots(cubic)]
    twist = read_twist()
    for slots in both:
        for j in range(1, 8):
            real, imag = slots[j]
            cos, sin = twist[j : j + 1], twist[8 + j : 9 + j]
            slots[j] = jnp.concatenate([real * cos + imag * sin, imag * cos - real * sin], 1)
    real_rows = read_real()
    first = product(split(jnp.concatenate([both[0][0], both[1][0]], 0)), real_rows, NN)
    fourier = read_fourier()
    rest = product(split(jnp.concatenate(both[0][1:] + both[1][1:], 0)), fourier, NN)
    for f in (0, 1):
        upper = jnp.concatenate([first[32 * f : 32 * f + 32], rest[224 * f : 224 * f + 96]], 0)
        lower = rest[224 * f + 96 : 224 * f + 224]
        for h, rows in ((0, upper), (1, lower)):
            put(h, 0, f, rows[:, :128].T)
            put(h, 1, f, rows[:, 128:].T)
    lanes = sum(bulk[:, 128 * a : 128 * a + 128] for a in range(16))
    return lanes


def wave_square(index, length):
    signed = jnp.where(2 * index >= length, index - length, index)
    phase_angle = signed.astype(f32) * (2.0 * math.pi / length)
    return phase_angle * phase_angle


def rates(wave_sq):
    numerator = 1.0 + time_step * stabilizer * wave_sq
    inverse = 1.0 / (numerator + time_step * kappa_grad * wave_sq * wave_sq)
    return numerator * inverse, time_step * wave_sq * inverse


def all_rates(section_at, lane_at, put):
    lane = lax.broadcasted_iota(jnp.int32, (128, 128), 1)
    row = lax.broadcasted_iota(jnp.int32, (128, 128), 0)
    slot = 4 * section_at + lane // 32
    y_index = jnp.where(slot == 0, 8 * lane_at, slot + 16 * lane_at)
    x_index = row + 128 * (lane % 16)
    wave_x = wave_square(x_index, NX)
    wave_xy = wave_x + wave_square(y_index, NY)
    half_y = (2.0 * math.pi / NY * (NY // 2)) ** 2
    for sigma in (0, 1):
        wave_z = wave_square(sigma + 2 * (lane // 16 % 2), NZ)
        for side, wave_sq in ((0, wave_z + wave_xy), (1, wave_z + (wave_x + half_y))):
            keep, mix = rates(wave_sq)
            put(sigma, side, 0, keep)
            put(sigma, side, 1, mix)


def middle(get, get_rate, section_at, lane_at, gather, lanes, spread_table, twist, put):
    lane = lax.broadcasted_iota(jnp.int32, (128, 128), 1)
    packed = (lane < 32) & (section_at == 0) & (lane_at == 0)
    cos, sin = twist[0], twist[1]
    parts = []
    for s in (0, 1):
        c_re, c_im, g_re, g_im = get(s, 0, 0), get(s, 1, 0), get(s, 0, 1), get(s, 1, 1)
        c_im, g_re = jnp.where(packed, g_re, c_im), jnp.where(packed, c_im, g_re)
        parts.append((c_re, c_im, g_re, g_im))
    stacked = []
    for sigma in (0, 1):
        mixed = [a + b if sigma == 0 else a - b for a, b in zip(*parts)]
        stacked.append(
            jnp.concatenate(
                [jnp.concatenate([mixed[0], mixed[2]], 1), jnp.concatenate([mixed[1], mixed[3]], 1)], 0
            )
        )
    spreads = [product(gather, split(stacked[sigma]), NN) for sigma in (0, 1)]
    turned = []
    for spread in spreads:
        rows = []
        for f in (0, 1):
            re, im = spread[:128, 128 * f : 128 * f + 128], spread[128:, 128 * f : 128 * f + 128]
            rows.append(jnp.concatenate([re * cos + im * sin, im * cos - re * sin], 1))
        turned.append(split(jnp.concatenate(rows, 0)))
    tables = [(lanes[sigma, 0], lanes[sigma, 1]) for sigma in (0, 1)]
    specs = [product(turned[sigma], tables[sigma], NN) for sigma in (0, 1)]
    filtered = []
    for sigma, spec in enumerate(specs):
        c_re, c_im, g_re, g_im = spec[:128, :128], spec[:128, 128:], spec[128:, :128], spec[128:, 128:]
        keep, mix = get_rate(sigma, 0, 0), get_rate(sigma, 0, 1)
        keep_half, mix_half = get_rate(sigma, 1, 0), get_rate(sigma, 1, 1)
        main_re = keep * c_re - mix * jnp.where(packed, c_im, g_re)
        main_im = keep * c_im - mix * jnp.where(packed, -c_re, g_im)
        side_re = keep_half * g_re - mix_half * g_im
        side_im = keep_half * g_im + mix_half * g_re
        rows = jnp.concatenate(
            [jnp.concatenate([main_re, main_im], 1), jnp.concatenate([side_re, side_im], 1)], 0
        )
        filtered.append(split(rows))
    back = [product(filtered[sigma], tables[sigma], NT) for sigma in (0, 1)]
    for s in (0, 1):
        mixed = back[0] + back[1] if s == 0 else back[0] - back[1]
        both = []
        for f in (0, 1):
            re, im = mixed[128 * f : 128 * f + 128, :128], mixed[128 * f : 128 * f + 128, 128:]
            both.append((re * cos - im * sin, im * cos + re * sin))
        (m_re, m_im), (s_re, s_im) = both
        upper = jnp.concatenate([m_re, jnp.where(packed, s_re, m_im)], 1)
        lower = jnp.concatenate([-m_im, jnp.where(packed, -s_im, m_re)], 1)
        out = product(spread_table, split(jnp.concatenate([upper, lower], 0)), NN)
        put(s, 0, out[:, :128])
        put(s, 1, out[:, 128:])


def inverse_y(get, fourier, real_rows, twist, put):
    slots = []
    for h in (0, 1):
        re, im = get(h, 0), get(h, 1)
        if h == 0:
            row = lax.broadcasted_iota(jnp.int32, (128, 128), 0)
            lane = lax.broadcasted_iota(jnp.int32, (128, 128), 1)
            single = (row == 0) & (lane < 32)
            re, im = jnp.where(single, 0.5 * re, re), jnp.where(single, 0.5 * im, im)
        rows = split(jnp.concatenate([re.T, im.T], 1))
        if h == 0:
            first = product((rows[0][:32], rows[1][:32]), real_rows, NN)
            rows = (rows[0][32:], rows[1][32:])
        out = product(rows, fourier, NN)
        slots += [out[32 * m : 32 * m + 32] for m in range(out.shape[0] // 32)]
    scale = 2.0 / CELLS
    base = [first[:, :128] * scale, first[:, 128:] * scale]
    real, imag = {}, {}
    for j in range(1, 8):
        re, im = slots[j - 1][:, :128], slots[j - 1][:, 128:]
        cos, sin = twist[j : j + 1] * scale, twist[8 + j : 9 + j] * scale
        real[j], imag[j] = re * cos - im * sin, im * cos + re * sin
    even = [
        weighted(
            [(COS16[j * a % 16], real[j]) for j in (2, 4, 6)]
            + [(-SIN16[j * a % 16], imag[j]) for j in (2, 4, 6)]
        )
        + base[a % 2]
        for a in range(8)
    ]
    cosine = [weighted([(COS16[j * a % 16], real[j]) for j in (1, 3, 5, 7)]) for a in range(4)]
    sine = [None] + [weighted([(SIN16[j * a % 16], imag[j]) for j in (1, 3, 5, 7)]) for a in range(1, 5)]
    odd = [cosine[0]] + [cosine[a] - sine[a] for a in (1, 2, 3)] + [-sine[4]]
    odd += [-cosine[a] - sine[a] for a in (3, 2, 1)]
    for a in range(8):
        put(a, even[a] + odd[a])
        put(a + 8, even[a] - odd[a])


def lane_position():
    return (
        16 * lax.axis_index("slab_z")
        + 4 * lax.axis_index("slab_y")
        + 2 * lax.axis_index("slab_x")
        + lax.axis_index("slab_core")
    )


def forward_kernel(
    c_hbm,
    fourier_hbm,
    real_hbm,
    twist_hbm,
    out_ref,
    bulk_ref,
    rate_ref,
    c_ref,
    fourier_ref,
    real_ref,
    twist_ref,
    sems,
):
    sources = (c_hbm, twist_hbm, real_hbm, fourier_hbm)
    targets = (c_ref, twist_ref, real_ref, fourier_ref)
    copies = [
        pltpu.make_async_copy(source, target, sems.at[n])
        for n, (source, target) in enumerate(zip(sources, targets))
    ]
    for copy in copies:
        copy.start()

    def put(h, part, f, value):
        out_ref[pl.ds(512 * h + 2 * part + f, 128, stride=4), :] = value

    def put_rate(sigma, side, kind, value):
        rate_ref[4 * sigma + 2 * side + kind] = value

    def late(n, ref):
        def read():
            copies[n].wait()
            return ref[...]

        return read

    all_rates(lax.axis_index("section"), lane_position(), put_rate)
    copies[0].wait()
    field = jnp.concatenate([c_ref[0], c_ref[1]], 0)
    lanes = forward_y(field, late(3, fourier_ref), late(2, real_ref), late(1, twist_ref), put)
    bulk_ref[...] = jnp.broadcast_to(jnp.sum(lanes, 0, keepdims=True), (8, 128))


def middle_kernel(in_ref, bulk_ref, rate_ref, gather_ref, lanes_ref, spread_ref, twist_ref, out_ref):
    def get(s, part, f):
        return in_ref[pl.ds(512 * s + 2 * part + f, 128, stride=4), :]

    def put(s, part, value):
        out_ref[pl.ds(384 * s + part, 128, stride=3), :] = value

    middle(
        get,
        lambda sigma, side, kind: rate_ref[4 * sigma + 2 * side + kind],
        lax.axis_index("section"),
        lane_position(),
        (gather_ref[0], gather_ref[1]),
        lanes_ref,
        (spread_ref[0], spread_ref[1]),
        twist_ref,
        put,
    )
    out_ref[pl.ds(2, 256, stride=3), :] = jnp.broadcast_to(bulk_ref[0:1, :], (256, 128))


def inverse_kernel(in_ref, fourier_ref, real_ref, twist_ref, out_ref, energy_ref):
    def get(h, part):
        return in_ref[pl.ds(384 * h + part, 128, stride=3), :]

    def put(a, value):
        out_ref[0, :, 128 * a : 128 * a + 128] = value[:16]
        out_ref[1, :, 128 * a : 128 * a + 128] = value[16:]

    inverse_y(
        get, (fourier_ref[0], fourier_ref[1]), (real_ref[0], real_ref[1]), twist_ref[...], put
    )
    energy_ref[...] = jnp.sum(in_ref[pl.ds(2, 256, stride=3), :], keepdims=True) * (1.0 / CELLS)


def exchange(rows):
    width = rows.shape[0] // 256
    message = rows.reshape(256, 1, 128 * width)
    return lax.all_to_all(message, ALL, split_axis=0, concat_axis=0, tiled=True).reshape(rows.shape)


def per_device(concentration):
    whole = pl.BlockSpec(memory_space=pltpu.VMEM)
    params = pltpu.CompilerParams(vmem_limit_bytes=12 << 20)
    outgoing, bulk, rate = pl.pallas_call(
        forward_kernel,
        out_shape=(
            pltpu.VMEM((1024, 128), f32),
            pltpu.VMEM((8, 128), f32),
            pltpu.VMEM((8, 128, 128), f32),
        ),
        in_specs=[pl.BlockSpec(memory_space=pltpu.HBM)] * 4,
        out_specs=(whole, whole, whole),
        scratch_shapes=[
            pltpu.VMEM(concentration.shape, f32),
            pltpu.VMEM(FOURIER.shape, bf16),
            pltpu.VMEM(REAL.shape, bf16),
            pltpu.VMEM(Y_TWIST.shape, f32),
            pltpu.SemaphoreType.DMA((4,)),
        ],
        compiler_params=params,
    )(*[pltpu.with_memory_space_constraint(a, pltpu.HBM) for a in (concentration, FOURIER_T, REAL_T, Y_TWIST)])
    columns = exchange(outgoing)
    leaving = pl.pallas_call(
        middle_kernel,
        out_shape=jax.ShapeDtypeStruct((768, 128), f32),
        in_specs=[whole] * 7,
        out_specs=whole,
        compiler_params=params,
    )(columns, bulk, rate, GATHER, LANES, SPREAD, X_TWIST)
    rows_back = exchange(leaving)
    new_field, energy = pl.pallas_call(
        inverse_kernel,
        out_shape=(jax.ShapeDtypeStruct(concentration.shape, f32), jax.ShapeDtypeStruct((1, 1), f32)),
        in_specs=[whole] * 4,
        out_specs=(whole, whole),
        compiler_params=params,
    )(rows_back, FOURIER, REAL, Y_TWIST)
    return new_field, energy.reshape(())


def solution(mesh):
    finer = Mesh(mesh.devices.reshape(2, 4, 2, 8, 2), ("section",) + SLAB)
    return jax.shard_map(
        per_device,
        mesh=finer,
        in_specs=(P("section", SLAB, None),),
        out_specs=(P("section", SLAB, None), P()),
        check_vma=False,
    )
```

```python
import math

import jax
import jax.numpy as jnp
import ml_dtypes
import numpy as np
from jax import lax
from jax.experimental import pallas as pl
from jax.experimental.pallas import tpu as pltpu
from jax.sharding import Mesh
from jax.sharding import PartitionSpec as P

SLAB = ("slab_y", "slab_x", "slab_z", "slab_core")
ALL = ("section", "slab_z", "slab_y", "slab_x", "slab_core")
NX = 2048
NY = 2048
NZ = 4
CELLS = NX * NY * NZ
time_step = 100.0
kappa_grad = 2.0
stabilizer = 8.0
f32 = jnp.float32
bf16 = jnp.bfloat16


def halves(matrix):
    high = matrix.astype(np.float32).astype(ml_dtypes.bfloat16)
    low = (matrix - high.astype(np.float64)).astype(np.float32).astype(ml_dtypes.bfloat16)
    return np.stack([high, low])


def fourier_table():
    index = np.arange(128)
    angle = 2.0 * np.pi * (np.outer(index, index) % 128) / 128
    return halves(np.block([[np.cos(angle), np.sin(angle)], [-np.sin(angle), np.cos(angle)]]))


def slab_order():
    return np.arange(128).reshape(4, 2, 8, 2).transpose(2, 0, 1, 3).reshape(128)


def real_table():
    angle = 2.0 * np.pi * (np.outer(np.arange(128), np.arange(256)) % 256) / 256
    lower = -np.sin(angle)
    lower[0] = 1.0 - 2.0 * (np.arange(256) % 2)
    return halves(np.concatenate([np.cos(angle), lower], 0))


def lane_table(parity):
    z_at, x_at = np.arange(2)[:, None, None, None], np.arange(16)[None, :, None, None]
    t_at, q_at = np.arange(2)[None, None, :, None], np.arange(16)[None, None, None, :]
    turn = (4 * parity * z_at + 8 * t_at * z_at + x_at * q_at) % 16
    value = np.exp(-2j * np.pi * turn / 16).reshape(32, 32)
    value = np.kron(np.eye(4), value)
    return halves(np.block([[value.real, value.imag], [-value.imag, value.real]]))


def y_twist_table():
    angle = 2.0 * np.pi * np.outer(np.arange(8), np.arange(128)) / 2048
    return np.concatenate([np.cos(angle), np.sin(angle)], 0).astype(np.float32)


def x_twist_table():
    angle = 2.0 * np.pi * np.outer(np.arange(128), np.arange(128) % 16) / 2048
    return np.stack([np.cos(angle), np.sin(angle)]).astype(np.float32)


FOURIER = fourier_table()
ORDER = slab_order()
GATHER = FOURIER[:, :, np.concatenate([ORDER, 128 + ORDER])]
SPREAD = FOURIER[:, ORDER, :]
REAL = real_table()
LANES = np.stack([lane_table(0), lane_table(1)])
FOURIER_T = FOURIER.transpose(0, 2, 1)
REAL_T = REAL.transpose(0, 2, 1)
Y_TWIST = y_twist_table()
X_TWIST = x_twist_table()
COS16 = [math.cos(2.0 * math.pi * m / 16) for m in range(16)]
SIN16 = [math.sin(2.0 * math.pi * m / 16) for m in range(16)]


def split(value):
    high = value.astype(bf16)
    return high, (value - high.astype(f32)).astype(bf16)


NN = (((1,), (0,)), ((), ()))
NT = (((1,), (1,)), ((), ()))


def product(left, right, pattern):
    total = left[0].shape[0]
    both = lax.dot_general(
        jnp.concatenate(left, 0), right[0], pattern, preferred_element_type=f32
    )
    rest = lax.dot_general(left[0], right[1], pattern, preferred_element_type=f32)
    return both[:total] + (both[total:] + rest)


def y_slots(at):
    add = [at[a] + at[a + 8] for a in range(8)]
    sub = [at[a] - at[a + 8] for a in range(8)]
    both = [add[a] + add[a + 4] for a in range(4)]
    diff = [add[a] - add[a + 4] for a in range(4)]
    zero = jnp.concatenate([both[0] + both[2], both[1] + both[3]], 1)
    near, far = (diff[1] - diff[3]) * COS16[2], (diff[1] + diff[3]) * COS16[2]
    minus = [None] + [sub[a] - sub[8 - a] for a in (1, 2, 3)]
    plus = [None] + [sub[a] + sub[8 - a] for a in (1, 2, 3)]
    middle_re = minus[2] * COS16[2]
    re_17, re_35 = sub[0] + middle_re, sub[0] - middle_re
    re_1, re_3 = minus[1] * COS16[1] + minus[3] * COS16[3], minus[1] * COS16[3] - minus[3] * COS16[1]
    im_1, im_3 = plus[1] * SIN16[1] + plus[3] * SIN16[3], plus[1] * SIN16[3] - plus[3] * SIN16[1]
    middle_im = plus[2] * SIN16[2]
    im_17, im_35 = middle_im + sub[4], middle_im - sub[4]
    return [
        zero,
        (re_17 + re_1, im_1 + im_17, -1),
        (diff[0] + near, diff[2] + far, -1),
        (re_35 + re_3, im_3 + im_35, -1),
        (both[0] - both[2], both[3] - both[1], 1),
        (re_35 - re_3, im_35 - im_3, 1),
        (diff[0] - near, diff[2] - far, 1),
        (re_17 - re_1, im_17 - im_1, 1),
    ]


def forward_y(read_rows, read_fourier, read_real, read_twist, put):
    lanes = None
    pieces = {}
    for group in range(4):
        rows = read_rows(group)
        c_at, g_at = [], []
        for a in range(16):
            value = rows[:, 128 * a : 128 * a + 128]
            squared = value * value
            bulk = squared * (0.25 * squared - 0.5)
            lanes = bulk if lanes is None else lanes + bulk
            c_at.append(value)
            g_at.append(squared * value - value)
        if group == 0:
            twist = read_twist()
            turns = [(twist[j : j + 1], twist[8 + j : 9 + j], -twist[j : j + 1]) for j in range(8)]
        for f, at in enumerate((c_at, g_at)):
            slots = y_slots(at)
            pieces[f, 0, group] = slots[0]
            for j in range(1, 8):
                re, n, sign = slots[j]
                cos, sin, negative = turns[j]
                if sign > 0:
                    turned = [re * cos + n * sin, n * cos - re * sin]
                else:
                    turned = [re * cos - n * sin, n * negative - re * sin]
                pieces[f, j, group] = jnp.concatenate(turned, 1)
    real_rows = read_real()
    zeros = jnp.concatenate([pieces[f, 0, group] for f in (0, 1) for group in range(4)], 0)
    first = product(split(zeros), real_rows, NN)
    fourier = read_fourier()
    others = [pieces[f, j, group] for f in (0, 1) for j in range(1, 8) for group in range(4)]
    rest = product(split(jnp.concatenate(others, 0)), fourier, NN)
    for f in (0, 1):
        upper = jnp.concatenate([first[32 * f : 32 * f + 32], rest[224 * f : 224 * f + 96]], 0)
        lower = rest[224 * f + 96 : 224 * f + 224]
        for h, rows in ((0, upper), (1, lower)):
            put(h, 0, f, rows[:, :128].T)
            put(h, 1, f, rows[:, 128:].T)
    return lanes


def wave_square(index, length):
    signed = jnp.where(2 * index >= length, index - length, index)
    phase_angle = signed.astype(f32) * (2.0 * math.pi / length)
    return phase_angle * phase_angle


def rates(wave_sq):
    numerator = 1.0 + time_step * stabilizer * wave_sq
    inverse = 1.0 / (numerator + time_step * kappa_grad * wave_sq * wave_sq)
    return numerator * inverse, time_step * wave_sq * inverse


def all_rates(section_at, lane_at, put):
    lane = lax.broadcasted_iota(jnp.int32, (128, 128), 1)
    row = lax.broadcasted_iota(jnp.int32, (128, 128), 0)
    slot = 4 * section_at + lane // 32
    y_index = jnp.where(slot == 0, 8 * lane_at, slot + 16 * lane_at)
    x_index = row + 128 * (lane % 16)
    wave_x = wave_square(x_index, NX)
    wave_xy = wave_x + wave_square(y_index, NY)
    half_y = (2.0 * math.pi / NY * (NY // 2)) ** 2
    for sigma in (0, 1):
        wave_z = wave_square(sigma + 2 * (lane // 16 % 2), NZ)
        for side, wave_sq in ((0, wave_z + wave_xy), (1, wave_z + (wave_x + half_y))):
            keep, mix = rates(wave_sq)
            put(sigma, side, 0, keep)
            put(sigma, side, 1, mix)


def middle(get, get_rate, section_at, lane_at, gather, lanes, spread_table, twist, put):
    lane = lax.broadcasted_iota(jnp.int32, (128, 128), 1)
    packed = (lane < 32) & (section_at == 0) & (lane_at == 0)
    cos, sin = twist[0], twist[1]
    parts = []
    for s in (0, 1):
        c_re, c_im, g_re, g_im = get(s, 0, 0), get(s, 1, 0), get(s, 0, 1), get(s, 1, 1)
        c_im, g_re = jnp.where(packed, g_re, c_im), jnp.where(packed, c_im, g_re)
        parts.append((c_re, c_im, g_re, g_im))
    stacked = []
    for sigma in (0, 1):
        mixed = [a + b if sigma == 0 else a - b for a, b in zip(*parts)]
        stacked.append(
            jnp.concatenate(
                [jnp.concatenate([mixed[0], mixed[2]], 1), jnp.concatenate([mixed[1], mixed[3]], 1)], 0
            )
        )
    spreads = [product(gather, split(stacked[sigma]), NN) for sigma in (0, 1)]
    turned = []
    for spread in spreads:
        rows = []
        for f in (0, 1):
            re, im = spread[:128, 128 * f : 128 * f + 128], spread[128:, 128 * f : 128 * f + 128]
            rows.append(jnp.concatenate([re * cos + im * sin, im * cos - re * sin], 1))
        turned.append(split(jnp.concatenate(rows, 0)))
    tables = [(lanes[sigma, 0], lanes[sigma, 1]) for sigma in (0, 1)]
    specs = [product(turned[sigma], tables[sigma], NN) for sigma in (0, 1)]
    filtered = []
    for sigma, spec in enumerate(specs):
        c_re, c_im, g_re, g_im = spec[:128, :128], spec[:128, 128:], spec[128:, :128], spec[128:, 128:]
        keep, mix = get_rate(sigma, 0, 0), get_rate(sigma, 0, 1)
        keep_half, mix_half = get_rate(sigma, 1, 0), get_rate(sigma, 1, 1)
        main_re = keep * c_re - mix * jnp.where(packed, c_im, g_re)
        main_im = keep * c_im - mix * jnp.where(packed, -c_re, g_im)
        side_re = keep_half * g_re - mix_half * g_im
        side_im = keep_half * g_im + mix_half * g_re
        rows = jnp.concatenate(
            [jnp.concatenate([main_re, main_im], 1), jnp.concatenate([side_re, side_im], 1)], 0
        )
        filtered.append(split(rows))
    back = [product(filtered[sigma], tables[sigma], NT) for sigma in (0, 1)]
    for s in (0, 1):
        mixed = back[0] + back[1] if s == 0 else back[0] - back[1]
        both = []
        for f in (0, 1):
            re, im = mixed[128 * f : 128 * f + 128, :128], mixed[128 * f : 128 * f + 128, 128:]
            both.append((re * cos - im * sin, im * cos + re * sin))
        (m_re, m_im), (s_re, s_im) = both
        upper = jnp.concatenate([m_re, jnp.where(packed, s_re, m_im)], 1)
        lower = jnp.concatenate([-m_im, jnp.where(packed, -s_im, m_re)], 1)
        out = product(spread_table, split(jnp.concatenate([upper, lower], 0)), NN)
        put(s, 0, out[:, :128])
        put(s, 1, out[:, 128:])


def inverse_y(get, fourier, real_rows, twist, put):
    slots = []
    for h in (0, 1):
        re, im = get(h, 0), get(h, 1)
        if h == 0:
            row = lax.broadcasted_iota(jnp.int32, (128, 128), 0)
            lane = lax.broadcasted_iota(jnp.int32, (128, 128), 1)
            single = (row == 0) & (lane < 32)
            re, im = jnp.where(single, 0.5 * re, re), jnp.where(single, 0.5 * im, im)
        rows = split(jnp.concatenate([re.T, im.T], 1))
        if h == 0:
            first = product((rows[0][:32], rows[1][:32]), real_rows, NN)
            rows = (rows[0][32:], rows[1][32:])
        out = product(rows, fourier, NN)
        slots += [out[32 * m : 32 * m + 32] for m in range(out.shape[0] // 32)]
    scale = 2.0 / CELLS
    base = [first[:, :128] * scale, first[:, 128:] * scale]
    real, imag = {}, {}
    for j in range(1, 8):
        re, im = slots[j - 1][:, :128], slots[j - 1][:, 128:]
        cos, sin = twist[j : j + 1] * scale, twist[8 + j : 9 + j] * scale
        real[j], imag[j] = re * cos - im * sin, im * cos + re * sin
    ends, tips = real[2] + real[6], imag[6] - imag[2]
    near, far = (real[2] - real[6]) * COS16[2], (imag[2] + imag[6]) * COS16[2]
    part = [ends, near - far, tips, -(near + far)]
    four = [base[0] + real[4], base[1] - imag[4], base[0] - real[4], base[1] + imag[4]]
    even = [four[a] + part[a] for a in range(4)] + [four[a] - part[a] for a in range(4)]
    u, v, w, x = real[1] + real[7], real[3] + real[5], real[1] - real[7], real[3] - real[5]
    cosine = [u + v, w * COS16[1] + x * COS16[3], (u - v) * COS16[2], w * COS16[3] - x * COS16[1]]
    u, v, w, x = imag[1] + imag[7], imag[3] + imag[5], imag[1] - imag[7], imag[3] - imag[5]
    sine = [None, u * SIN16[1] + v * SIN16[3], (w + x) * SIN16[2], u * SIN16[3] - v * SIN16[1], w - x]
    put(0, even[0] + cosine[0])
    put(8, even[0] - cosine[0])
    for a in (1, 2, 3):
        odd, mirror = cosine[a] - sine[a], cosine[a] + sine[a]
        put(a, even[a] + odd)
        put(a + 8, even[a] - odd)
        put(8 - a, even[8 - a] - mirror)
        put(16 - a, even[8 - a] + mirror)
    put(4, even[4] - sine[4])
    put(12, even[4] + sine[4])


def lane_position():
    return (
        16 * lax.axis_index("slab_z")
        + 4 * lax.axis_index("slab_y")
        + 2 * lax.axis_index("slab_x")
        + lax.axis_index("slab_core")
    )


def forward_kernel(
    c_hbm,
    fourier_hbm,
    real_hbm,
    twist_hbm,
    out_ref,
    bulk_ref,
    rate_ref,
    c_ref,
    fourier_ref,
    real_ref,
    twist_ref,
    sems,
):
    def group_of(ref, n):
        return ref.at[n // 2, pl.ds(8 * (n % 2), 8), :]

    sources = [group_of(c_hbm, n) for n in range(4)] + [twist_hbm, real_hbm, fourier_hbm]
    targets = [group_of(c_ref, n) for n in range(4)] + [twist_ref, real_ref, fourier_ref]
    copies = [
        pltpu.make_async_copy(source, target, sems.at[n])
        for n, (source, target) in enumerate(zip(sources, targets))
    ]
    for copy in copies:
        copy.start()

    def put(h, part, f, value):
        out_ref[pl.ds(512 * h + 2 * part + f, 128, stride=4), :] = value

    def put_rate(sigma, side, kind, value):
        rate_ref[4 * sigma + 2 * side + kind] = value

    def late(n, ref):
        def read():
            copies[n].wait()
            return ref[...]

        return read

    all_rates(lax.axis_index("section"), lane_position(), put_rate)
    def read_rows(n):
        copies[n].wait()
        return c_ref[n // 2, 8 * (n % 2) : 8 * (n % 2) + 8, :]

    lanes = forward_y(read_rows, late(6, fourier_ref), late(5, real_ref), late(4, twist_ref), put)
    bulk_ref[...] = jnp.broadcast_to(jnp.sum(lanes, 0, keepdims=True), (8, 128))


def middle_kernel(in_ref, bulk_ref, rate_ref, gather_ref, lanes_ref, spread_ref, twist_ref, out_ref):
    def get(s, part, f):
        return in_ref[pl.ds(512 * s + 2 * part + f, 128, stride=4), :]

    def put(s, part, value):
        out_ref[pl.ds(384 * s + part, 128, stride=3), :] = value

    middle(
        get,
        lambda sigma, side, kind: rate_ref[4 * sigma + 2 * side + kind],
        lax.axis_index("section"),
        lane_position(),
        (gather_ref[0], gather_ref[1]),
        lanes_ref,
        (spread_ref[0], spread_ref[1]),
        twist_ref,
        put,
    )
    out_ref[pl.ds(2, 256, stride=3), :] = jnp.broadcast_to(bulk_ref[0:1, :], (256, 128))


def inverse_kernel(in_ref, fourier_ref, real_ref, twist_ref, out_ref, energy_ref):
    def get(h, part):
        return in_ref[pl.ds(384 * h + part, 128, stride=3), :]

    def put(a, value):
        out_ref[0, :, 128 * a : 128 * a + 128] = value[:16]
        out_ref[1, :, 128 * a : 128 * a + 128] = value[16:]

    inverse_y(
        get, (fourier_ref[0], fourier_ref[1]), (real_ref[0], real_ref[1]), twist_ref[...], put
    )
    energy_ref[...] = jnp.sum(in_ref[pl.ds(2, 256, stride=3), :], keepdims=True) * (1.0 / CELLS)


def exchange(rows):
    width = rows.shape[0] // 256
    message = rows.reshape(256, 1, 128 * width)
    return lax.all_to_all(message, ALL, split_axis=0, concat_axis=0, tiled=True).reshape(rows.shape)


def per_device(concentration):
    whole = pl.BlockSpec(memory_space=pltpu.VMEM)
    params = pltpu.CompilerParams(vmem_limit_bytes=12 << 20)
    outgoing, bulk, rate = pl.pallas_call(
        forward_kernel,
        out_shape=(
            pltpu.VMEM((1024, 128), f32),
            pltpu.VMEM((8, 128), f32),
            pltpu.VMEM((8, 128, 128), f32),
        ),
        in_specs=[pl.BlockSpec(memory_space=pltpu.HBM)] * 4,
        out_specs=(whole, whole, whole),
        scratch_shapes=[
            pltpu.VMEM(concentration.shape, f32),
            pltpu.VMEM(FOURIER.shape, bf16),
            pltpu.VMEM(REAL.shape, bf16),
            pltpu.VMEM(Y_TWIST.shape, f32),
            pltpu.SemaphoreType.DMA((7,)),
        ],
        compiler_params=params,
    )(*[pltpu.with_memory_space_constraint(a, pltpu.HBM) for a in (concentration, FOURIER_T, REAL_T, Y_TWIST)])
    columns = exchange(outgoing)
    leaving = pl.pallas_call(
        middle_kernel,
        out_shape=jax.ShapeDtypeStruct((768, 128), f32),
        in_specs=[whole] * 7,
        out_specs=whole,
        compiler_params=params,
    )(columns, bulk, rate, GATHER, LANES, SPREAD, X_TWIST)
    rows_back = exchange(leaving)
    new_field, energy = pl.pallas_call(
        inverse_kernel,
        out_shape=(jax.ShapeDtypeStruct(concentration.shape, f32), jax.ShapeDtypeStruct((1, 1), f32)),
        in_specs=[whole] * 4,
        out_specs=(whole, whole),
        compiler_params=params,
    )(rows_back, FOURIER, REAL, Y_TWIST)
    return new_field, energy.reshape(())


def solution(mesh):
    finer = Mesh(mesh.devices.reshape(2, 4, 2, 8, 2), ("section",) + SLAB)
    return jax.shard_map(
        per_device,
        mesh=finer,
        in_specs=(P("section", SLAB, None),),
        out_specs=(P("section", SLAB, None), P()),
        check_vma=False,
    )
```

```python
import math

import jax
import jax.numpy as jnp
import ml_dtypes
import numpy as np
from jax import lax
from jax.experimental import pallas as pl
from jax.experimental.pallas import tpu as pltpu
from jax.sharding import Mesh
from jax.sharding import PartitionSpec as P

SLAB = ("slab_y", "slab_x", "slab_z", "slab_core")
ALL = ("section", "slab_z", "slab_y", "slab_x", "slab_core")
NX = 2048
NY = 2048
NZ = 4
CELLS = NX * NY * NZ
time_step = 100.0
kappa_grad = 2.0
stabilizer = 8.0
f32 = jnp.float32
bf16 = jnp.bfloat16


def halves(matrix):
    high = matrix.astype(np.float32).astype(ml_dtypes.bfloat16)
    low = (matrix - high.astype(np.float64)).astype(np.float32).astype(ml_dtypes.bfloat16)
    return np.stack([high, low])


def fourier_table():
    index = np.arange(128)
    angle = 2.0 * np.pi * (np.outer(index, index) % 128) / 128
    return halves(np.block([[np.cos(angle), np.sin(angle)], [-np.sin(angle), np.cos(angle)]]))


def slab_order():
    return np.arange(128).reshape(4, 2, 8, 2).transpose(2, 0, 1, 3).reshape(128)


def real_table():
    angle = 2.0 * np.pi * (np.outer(np.arange(128), np.arange(256)) % 256) / 256
    lower = -np.sin(angle)
    lower[0] = 1.0 - 2.0 * (np.arange(256) % 2)
    return halves(np.concatenate([np.cos(angle), lower], 0))


def lane_table(parity):
    z_at, x_at = np.arange(2)[:, None, None, None], np.arange(16)[None, :, None, None]
    t_at, q_at = np.arange(2)[None, None, :, None], np.arange(16)[None, None, None, :]
    turn = (4 * parity * z_at + 8 * t_at * z_at + x_at * q_at) % 16
    value = np.exp(-2j * np.pi * turn / 16).reshape(32, 32)
    value = np.kron(np.eye(4), value)
    return halves(np.block([[value.real, value.imag], [-value.imag, value.real]]))


def y_twist_table():
    angle = 2.0 * np.pi * np.outer(np.arange(8), np.arange(128)) / 2048
    return np.concatenate([np.cos(angle), np.sin(angle)], 0).astype(np.float32)


def x_twist_table():
    angle = 2.0 * np.pi * np.outer(np.arange(128), np.arange(128) % 16) / 2048
    return np.stack([np.cos(angle), np.sin(angle)]).astype(np.float32)


FOURIER = fourier_table()
ORDER = slab_order()
GATHER = FOURIER[:, :, np.concatenate([ORDER, 128 + ORDER])]
SPREAD = FOURIER[:, ORDER, :]
REAL = real_table()
LANES = np.stack([lane_table(0), lane_table(1)])
FOURIER_T = FOURIER.transpose(0, 2, 1)
REAL_T = REAL.transpose(0, 2, 1)
Y_TWIST = y_twist_table()
X_TWIST = x_twist_table()
COS16 = [math.cos(2.0 * math.pi * m / 16) for m in range(16)]
SIN16 = [math.sin(2.0 * math.pi * m / 16) for m in range(16)]


def split(value):
    high = value.astype(bf16)
    return high, (value - high.astype(f32)).astype(bf16)


NN = (((1,), (0,)), ((), ()))
NT = (((1,), (1,)), ((), ()))


def product(left, right, pattern):
    total = left[0].shape[0]
    both = lax.dot_general(
        jnp.concatenate(left, 0), right[0], pattern, preferred_element_type=f32
    )
    rest = lax.dot_general(left[0], right[1], pattern, preferred_element_type=f32)
    return both[:total] + (both[total:] + rest)


def y_slots(at):
    add = [at[a] + at[a + 8] for a in range(8)]
    sub = [at[a] - at[a + 8] for a in range(8)]
    both = [add[a] + add[a + 4] for a in range(4)]
    diff = [add[a] - add[a + 4] for a in range(4)]
    zero = jnp.concatenate([both[0] + both[2], both[1] + both[3]], 1)
    near, far = (diff[1] - diff[3]) * COS16[2], (diff[1] + diff[3]) * COS16[2]
    minus = [None] + [sub[a] - sub[8 - a] for a in (1, 2, 3)]
    plus = [None] + [sub[a] + sub[8 - a] for a in (1, 2, 3)]
    middle_re = minus[2] * COS16[2]
    re_17, re_35 = sub[0] + middle_re, sub[0] - middle_re
    re_1, re_3 = minus[1] * COS16[1] + minus[3] * COS16[3], minus[1] * COS16[3] - minus[3] * COS16[1]
    im_1, im_3 = plus[1] * SIN16[1] + plus[3] * SIN16[3], plus[1] * SIN16[3] - plus[3] * SIN16[1]
    middle_im = plus[2] * SIN16[2]
    im_17, im_35 = middle_im + sub[4], middle_im - sub[4]
    return [
        zero,
        (re_17 + re_1, im_1 + im_17, -1),
        (diff[0] + near, diff[2] + far, -1),
        (re_35 + re_3, im_3 + im_35, -1),
        (both[0] - both[2], both[3] - both[1], 1),
        (re_35 - re_3, im_35 - im_3, 1),
        (diff[0] - near, diff[2] - far, 1),
        (re_17 - re_1, im_17 - im_1, 1),
    ]


def forward_y(read_rows, read_fourier, read_real, read_twist, put):
    lanes = None
    pieces = {}
    for group in range(4):
        rows = read_rows(group)
        c_at, g_at = [], []
        for a in range(16):
            value = rows[:, 128 * a : 128 * a + 128]
            squared = value * value
            bulk = squared * (0.25 * squared - 0.5)
            lanes = bulk if lanes is None else lanes + bulk
            c_at.append(value)
            g_at.append(squared * value - value)
        if group == 0:
            twist = read_twist()
            turns = [(twist[j : j + 1], twist[8 + j : 9 + j], -twist[j : j + 1]) for j in range(8)]
        for f, at in enumerate((c_at, g_at)):
            slots = y_slots(at)
            pieces[f, 0, group] = slots[0]
            for j in range(1, 8):
                re, n, sign = slots[j]
                cos, sin, negative = turns[j]
                if sign > 0:
                    turned = [re * cos + n * sin, n * cos - re * sin]
                else:
                    turned = [re * cos - n * sin, n * negative - re * sin]
                pieces[f, j, group] = jnp.concatenate(turned, 1)
    real_rows = read_real()
    zeros = jnp.concatenate([pieces[f, 0, group] for f in (0, 1) for group in range(4)], 0)
    first = product(split(zeros), real_rows, NN)
    fourier = read_fourier()
    others = [pieces[f, j, group] for f in (0, 1) for j in range(1, 8) for group in range(4)]
    rest = product(split(jnp.concatenate(others, 0)), fourier, NN)
    for f in (0, 1):
        upper = jnp.concatenate([first[32 * f : 32 * f + 32], rest[224 * f : 224 * f + 96]], 0)
        lower = rest[224 * f + 96 : 224 * f + 224]
        for h, rows in ((0, upper), (1, lower)):
            put(h, 0, f, rows[:, :128].T)
            put(h, 1, f, rows[:, 128:].T)
    return lanes


def wave_square(index, length):
    signed = jnp.where(2 * index >= length, index - length, index)
    phase_angle = signed.astype(f32) * (2.0 * math.pi / length)
    return phase_angle * phase_angle


def rates(wave_sq):
    numerator = 1.0 + time_step * stabilizer * wave_sq
    inverse = 1.0 / (numerator + time_step * kappa_grad * wave_sq * wave_sq)
    return numerator * inverse, time_step * wave_sq * inverse


def all_rates(section_at, lane_at, put):
    lane = lax.broadcasted_iota(jnp.int32, (128, 128), 1)
    row = lax.broadcasted_iota(jnp.int32, (128, 128), 0)
    slot = 4 * section_at + lane // 32
    y_index = jnp.where(slot == 0, 8 * lane_at, slot + 16 * lane_at)
    x_index = row + 128 * (lane % 16)
    wave_x = wave_square(x_index, NX)
    wave_xy = wave_x + wave_square(y_index, NY)
    half_y = (2.0 * math.pi / NY * (NY // 2)) ** 2
    for sigma in (0, 1):
        wave_z = wave_square(sigma + 2 * (lane // 16 % 2), NZ)
        for side, wave_sq in ((0, wave_z + wave_xy), (1, wave_z + (wave_x + half_y))):
            keep, mix = rates(wave_sq)
            put(sigma, side, 0, keep)
            put(sigma, side, 1, mix)


def middle(get, get_rate, section_at, lane_at, gather, lanes, spread_table, twist, put):
    lane = lax.broadcasted_iota(jnp.int32, (128, 128), 1)
    packed = (lane < 32) & (section_at == 0) & (lane_at == 0)
    cos, sin = twist[0], twist[1]
    parts = []
    for s in (0, 1):
        c_re, c_im, g_re, g_im = get(s, 0, 0), get(s, 1, 0), get(s, 0, 1), get(s, 1, 1)
        c_im, g_re = jnp.where(packed, g_re, c_im), jnp.where(packed, c_im, g_re)
        parts.append((c_re, c_im, g_re, g_im))
    stacked = []
    for sigma in (0, 1):
        mixed = [a + b if sigma == 0 else a - b for a, b in zip(*parts)]
        stacked.append(
            jnp.concatenate(
                [jnp.concatenate([mixed[0], mixed[2]], 1), jnp.concatenate([mixed[1], mixed[3]], 1)], 0
            )
        )
    spreads = [product(gather, split(stacked[sigma]), NN) for sigma in (0, 1)]
    turned = []
    for spread in spreads:
        rows = []
        for f in (0, 1):
            re, im = spread[:128, 128 * f : 128 * f + 128], spread[128:, 128 * f : 128 * f + 128]
            rows.append(jnp.concatenate([re * cos + im * sin, im * cos - re * sin], 1))
        turned.append(split(jnp.concatenate(rows, 0)))
    tables = [(lanes[sigma, 0], lanes[sigma, 1]) for sigma in (0, 1)]
    specs = [product(turned[sigma], tables[sigma], NN) for sigma in (0, 1)]
    filtered = []
    for sigma, spec in enumerate(specs):
        c_re, c_im, g_re, g_im = spec[:128, :128], spec[:128, 128:], spec[128:, :128], spec[128:, 128:]
        keep, mix = get_rate(sigma, 0, 0), get_rate(sigma, 0, 1)
        keep_half, mix_half = get_rate(sigma, 1, 0), get_rate(sigma, 1, 1)
        main_re = keep * c_re - mix * jnp.where(packed, c_im, g_re)
        main_im = keep * c_im - mix * jnp.where(packed, -c_re, g_im)
        side_re = keep_half * g_re - mix_half * g_im
        side_im = keep_half * g_im + mix_half * g_re
        rows = jnp.concatenate(
            [jnp.concatenate([main_re, main_im], 1), jnp.concatenate([side_re, side_im], 1)], 0
        )
        filtered.append(split(rows))
    back = [product(filtered[sigma], tables[sigma], NT) for sigma in (0, 1)]
    for s in (0, 1):
        mixed = back[0] + back[1] if s == 0 else back[0] - back[1]
        both = []
        for f in (0, 1):
            re, im = mixed[128 * f : 128 * f + 128, :128], mixed[128 * f : 128 * f + 128, 128:]
            both.append((re * cos - im * sin, im * cos + re * sin))
        (m_re, m_im), (s_re, s_im) = both
        upper = jnp.concatenate([m_re, jnp.where(packed, s_re, m_im)], 1)
        lower = jnp.concatenate([-m_im, jnp.where(packed, -s_im, m_re)], 1)
        out = product(spread_table, split(jnp.concatenate([upper, lower], 0)), NN)
        put(s, 0, out[:, :128])
        put(s, 1, out[:, 128:])


def inverse_y(get, fourier, real_rows, twist, put):
    slots = []
    for h in (0, 1):
        re, im = get(h, 0), get(h, 1)
        if h == 0:
            row = lax.broadcasted_iota(jnp.int32, (128, 128), 0)
            lane = lax.broadcasted_iota(jnp.int32, (128, 128), 1)
            single = (row == 0) & (lane < 32)
            re, im = jnp.where(single, 0.5 * re, re), jnp.where(single, 0.5 * im, im)
        rows = split(jnp.concatenate([re.T, im.T], 1))
        if h == 0:
            first = product((rows[0][:32], rows[1][:32]), real_rows, NN)
            rows = (rows[0][32:], rows[1][32:])
        out = product(rows, fourier, NN)
        slots += [out[32 * m : 32 * m + 32] for m in range(out.shape[0] // 32)]
    scale = 2.0 / CELLS
    base = [first[:, :128] * scale, first[:, 128:] * scale]
    real, imag = {}, {}
    for j in range(1, 8):
        re, im = slots[j - 1][:, :128], slots[j - 1][:, 128:]
        cos, sin = twist[j : j + 1] * scale, twist[8 + j : 9 + j] * scale
        real[j], imag[j] = re * cos - im * sin, im * cos + re * sin
    ends, tips = real[2] + real[6], imag[6] - imag[2]
    near, far = (real[2] - real[6]) * COS16[2], (imag[2] + imag[6]) * COS16[2]
    part = [ends, near - far, tips, -(near + far)]
    four = [base[0] + real[4], base[1] - imag[4], base[0] - real[4], base[1] + imag[4]]
    even = [four[a] + part[a] for a in range(4)] + [four[a] - part[a] for a in range(4)]
    u, v, w, x = real[1] + real[7], real[3] + real[5], real[1] - real[7], real[3] - real[5]
    cosine = [u + v, w * COS16[1] + x * COS16[3], (u - v) * COS16[2], w * COS16[3] - x * COS16[1]]
    u, v, w, x = imag[1] + imag[7], imag[3] + imag[5], imag[1] - imag[7], imag[3] - imag[5]
    sine = [None, u * SIN16[1] + v * SIN16[3], (w + x) * SIN16[2], u * SIN16[3] - v * SIN16[1], w - x]
    put(0, even[0] + cosine[0])
    put(8, even[0] - cosine[0])
    for a in (1, 2, 3):
        odd, mirror = cosine[a] - sine[a], cosine[a] + sine[a]
        put(a, even[a] + odd)
        put(a + 8, even[a] - odd)
        put(8 - a, even[8 - a] - mirror)
        put(16 - a, even[8 - a] + mirror)
    put(4, even[4] - sine[4])
    put(12, even[4] + sine[4])


def lane_position():
    return (
        16 * lax.axis_index("slab_z")
        + 4 * lax.axis_index("slab_y")
        + 2 * lax.axis_index("slab_x")
        + lax.axis_index("slab_core")
    )


def forward_kernel(
    c_hbm,
    fourier_hbm,
    real_hbm,
    twist_hbm,
    out_ref,
    rate_ref,
    c_ref,
    fourier_ref,
    real_ref,
    twist_ref,
    sems,
):
    def group_of(ref, n):
        return ref.at[n // 2, pl.ds(8 * (n % 2), 8), :]

    sources = [group_of(c_hbm, n) for n in range(4)] + [twist_hbm, real_hbm, fourier_hbm]
    targets = [group_of(c_ref, n) for n in range(4)] + [twist_ref, real_ref, fourier_ref]
    copies = [
        pltpu.make_async_copy(source, target, sems.at[n])
        for n, (source, target) in enumerate(zip(sources, targets))
    ]
    for copy in copies:
        copy.start()

    def put(h, part, f, value):
        out_ref[pl.ds(640 * h + 2 * part + f, 128, stride=5), :] = value

    def put_rate(sigma, side, kind, value):
        rate_ref[4 * sigma + 2 * side + kind] = value

    def late(n, ref):
        def read():
            copies[n].wait()
            return ref[...]

        return read

    all_rates(lax.axis_index("section"), lane_position(), put_rate)
    def read_rows(n):
        copies[n].wait()
        return c_ref[n // 2, 8 * (n % 2) : 8 * (n % 2) + 8, :]

    lanes = forward_y(read_rows, late(6, fourier_ref), late(5, real_ref), late(4, twist_ref), put)
    out_ref[pl.ds(4, 256, stride=5), :] = jnp.broadcast_to(jnp.sum(lanes, 0, keepdims=True), (256, 128))


def middle_kernel(
    in_ref, rate_ref, gather_ref, lanes_ref, spread_ref, twist_ref, out_ref, bulk_ref
):
    def get(s, part, f):
        return in_ref[pl.ds(640 * s + 2 * part + f, 128, stride=5), :]

    def put(s, part, value):
        out_ref[pl.ds(256 * s + part, 128, stride=2), :] = value

    middle(
        get,
        lambda sigma, side, kind: rate_ref[4 * sigma + 2 * side + kind],
        lax.axis_index("section"),
        lane_position(),
        (gather_ref[0], gather_ref[1]),
        lanes_ref,
        (spread_ref[0], spread_ref[1]),
        twist_ref,
        put,
    )
    bulk = jnp.sum(in_ref[pl.ds(4, 256, stride=5), :], 0, keepdims=True)
    bulk_ref[...] = jnp.broadcast_to(bulk, (8, 128))


def inverse_kernel(in_ref, bulk_ref, fourier_ref, real_ref, twist_ref, out_ref, energy_ref):
    def get(h, part):
        return in_ref[pl.ds(256 * h + part, 128, stride=2), :]

    def put(a, value):
        out_ref[0, :, 128 * a : 128 * a + 128] = value[:16]
        out_ref[1, :, 128 * a : 128 * a + 128] = value[16:]

    energy_ref[...] = jnp.sum(bulk_ref[0:1, :], keepdims=True) * (1.0 / CELLS)
    inverse_y(
        get, (fourier_ref[0], fourier_ref[1]), (real_ref[0], real_ref[1]), twist_ref[...], put
    )


def exchange(rows):
    width = rows.shape[0] // 256
    message = rows.reshape(256, 1, 128 * width)
    return lax.all_to_all(message, ALL, split_axis=0, concat_axis=0, tiled=True).reshape(rows.shape)


def per_device(concentration):
    whole = pl.BlockSpec(memory_space=pltpu.VMEM)
    params = pltpu.CompilerParams(vmem_limit_bytes=12 << 20)
    outgoing, rate = pl.pallas_call(
        forward_kernel,
        out_shape=(
            pltpu.VMEM((1280, 128), f32),
            pltpu.VMEM((8, 128, 128), f32),
        ),
        in_specs=[pl.BlockSpec(memory_space=pltpu.HBM)] * 4,
        out_specs=(whole, whole),
        scratch_shapes=[
            pltpu.VMEM(concentration.shape, f32),
            pltpu.VMEM(FOURIER.shape, bf16),
            pltpu.VMEM(REAL.shape, bf16),
            pltpu.VMEM(Y_TWIST.shape, f32),
            pltpu.SemaphoreType.DMA((7,)),
        ],
        compiler_params=params,
    )(*[pltpu.with_memory_space_constraint(a, pltpu.HBM) for a in (concentration, FOURIER_T, REAL_T, Y_TWIST)])
    columns = exchange(outgoing)
    leaving, bulk = pl.pallas_call(
        middle_kernel,
        out_shape=(pltpu.VMEM((512, 128), f32), pltpu.VMEM((8, 128), f32)),
        in_specs=[whole] * 6,
        out_specs=(whole, whole),
        compiler_params=params,
    )(columns, rate, GATHER, LANES, SPREAD, X_TWIST)
    rows_back = exchange(leaving)
    new_field, energy = pl.pallas_call(
        inverse_kernel,
        out_shape=(jax.ShapeDtypeStruct(concentration.shape, f32), jax.ShapeDtypeStruct((1, 1), f32)),
        in_specs=[whole] * 5,
        out_specs=(whole, whole),
        compiler_params=params,
    )(rows_back, bulk, FOURIER, REAL, Y_TWIST)
    return new_field, energy.reshape(())


def solution(mesh):
    finer = Mesh(mesh.devices.reshape(2, 4, 2, 8, 2), ("section",) + SLAB)
    return jax.shard_map(
        per_device,
        mesh=finer,
        in_specs=(P("section", SLAB, None),),
        out_specs=(P("section", SLAB, None), P()),
        check_vma=False,
    )
```

```python
import math

import jax
import jax.numpy as jnp
import ml_dtypes
import numpy as np
from jax import lax
from jax.experimental import pallas as pl
from jax.experimental.pallas import tpu as pltpu
from jax.sharding import Mesh
from jax.sharding import PartitionSpec as P

SLAB = ("slab_y", "slab_x", "slab_z", "slab_core")
ALL = ("section", "slab_z", "slab_y", "slab_x", "slab_core")
NX = 2048
NY = 2048
NZ = 4
CELLS = NX * NY * NZ
time_step = 100.0
kappa_grad = 2.0
stabilizer = 8.0
f32 = jnp.float32
bf16 = jnp.bfloat16


def halves(matrix):
    high = matrix.astype(np.float32).astype(ml_dtypes.bfloat16)
    low = (matrix - high.astype(np.float64)).astype(np.float32).astype(ml_dtypes.bfloat16)
    return np.stack([high, low])


def fourier_table():
    index = np.arange(128)
    angle = 2.0 * np.pi * (np.outer(index, index) % 128) / 128
    return halves(np.block([[np.cos(angle), np.sin(angle)], [-np.sin(angle), np.cos(angle)]]))


def slab_order():
    return np.arange(128).reshape(4, 2, 8, 2).transpose(2, 0, 1, 3).reshape(128)


def real_table():
    angle = 2.0 * np.pi * (np.outer(np.arange(128), np.arange(256)) % 256) / 256
    lower = -np.sin(angle)
    lower[0] = 1.0 - 2.0 * (np.arange(256) % 2)
    return halves(np.concatenate([np.cos(angle), lower], 0))


def lane_table(parity):
    z_at, x_at = np.arange(2)[:, None, None, None], np.arange(16)[None, :, None, None]
    t_at, q_at = np.arange(2)[None, None, :, None], np.arange(16)[None, None, None, :]
    turn = (4 * parity * z_at + 8 * t_at * z_at + x_at * q_at) % 16
    value = np.exp(-2j * np.pi * turn / 16).reshape(32, 32)
    value = np.kron(np.eye(4), value)
    return halves(np.block([[value.real, value.imag], [-value.imag, value.real]]))


def y_twist_table():
    angle = 2.0 * np.pi * np.outer(np.arange(8), np.arange(128)) / 2048
    return np.concatenate([np.cos(angle), np.sin(angle)], 0).astype(np.float32)


def x_twist_table():
    angle = 2.0 * np.pi * np.outer(np.arange(128), np.arange(128) % 16) / 2048
    return np.stack([np.cos(angle), np.sin(angle)]).astype(np.float32)


FOURIER = fourier_table()
ORDER = slab_order()
GATHER = FOURIER[:, :, np.concatenate([ORDER, 128 + ORDER])]
SPREAD = FOURIER[:, ORDER, :]
REAL = real_table()
LANES = np.stack([lane_table(0), lane_table(1)])
FOURIER_T = FOURIER.transpose(0, 2, 1)
REAL_T = REAL.transpose(0, 2, 1)
Y_TWIST = y_twist_table()
X_TWIST = x_twist_table()
COS16 = [math.cos(2.0 * math.pi * m / 16) for m in range(16)]
SIN16 = [math.sin(2.0 * math.pi * m / 16) for m in range(16)]


def split(value):
    high = value.astype(bf16)
    return high, (value - high.astype(f32)).astype(bf16)


NN = (((1,), (0,)), ((), ()))
NT = (((1,), (1,)), ((), ()))


def product(left, right, pattern):
    total = left[0].shape[0]
    both = lax.dot_general(
        jnp.concatenate(left, 0), right[0], pattern, preferred_element_type=f32
    )
    rest = lax.dot_general(left[0], right[1], pattern, preferred_element_type=f32)
    return both[:total] + (both[total:] + rest)


def y_slots(at):
    add = [at[a] + at[a + 8] for a in range(8)]
    sub = [at[a] - at[a + 8] for a in range(8)]
    both = [add[a] + add[a + 4] for a in range(4)]
    diff = [add[a] - add[a + 4] for a in range(4)]
    zero = jnp.concatenate([both[0] + both[2], both[1] + both[3]], 1)
    near, far = (diff[1] - diff[3]) * COS16[2], (diff[1] + diff[3]) * COS16[2]
    minus = [None] + [sub[a] - sub[8 - a] for a in (1, 2, 3)]
    plus = [None] + [sub[a] + sub[8 - a] for a in (1, 2, 3)]
    middle_re = minus[2] * COS16[2]
    re_17, re_35 = sub[0] + middle_re, sub[0] - middle_re
    re_1, re_3 = minus[1] * COS16[1] + minus[3] * COS16[3], minus[1] * COS16[3] - minus[3] * COS16[1]
    im_1, im_3 = plus[1] * SIN16[1] + plus[3] * SIN16[3], plus[1] * SIN16[3] - plus[3] * SIN16[1]
    middle_im = plus[2] * SIN16[2]
    im_17, im_35 = middle_im + sub[4], middle_im - sub[4]
    return [
        zero,
        (re_17 + re_1, im_1 + im_17, -1),
        (diff[0] + near, diff[2] + far, -1),
        (re_35 + re_3, im_3 + im_35, -1),
        (both[0] - both[2], both[3] - both[1], 1),
        (re_35 - re_3, im_35 - im_3, 1),
        (diff[0] - near, diff[2] - far, 1),
        (re_17 - re_1, im_17 - im_1, 1),
    ]


def forward_y(read_rows, read_fourier, read_real, read_twist, put):
    lanes = None
    pieces = {}
    for group in range(4):
        rows = read_rows(group)
        c_at, g_at = [], []
        for a in range(16):
            value = rows[:, 128 * a : 128 * a + 128]
            squared = value * value
            bulk = squared * (0.25 * squared - 0.5)
            lanes = bulk if lanes is None else lanes + bulk
            c_at.append(value)
            g_at.append(squared * value - value)
        if group == 0:
            twist = read_twist()
            turns = [(twist[j : j + 1], twist[8 + j : 9 + j], -twist[j : j + 1]) for j in range(8)]
        for f, at in enumerate((c_at, g_at)):
            slots = y_slots(at)
            pieces[f, 0, group] = slots[0]
            for j in range(1, 8):
                re, n, sign = slots[j]
                cos, sin, negative = turns[j]
                if sign > 0:
                    turned = [re * cos + n * sin, n * cos - re * sin]
                else:
                    turned = [re * cos - n * sin, n * negative - re * sin]
                pieces[f, j, group] = jnp.concatenate(turned, 1)
    real_rows = read_real()
    zeros = jnp.concatenate([pieces[f, 0, group] for f in (0, 1) for group in range(4)], 0)
    first = product(split(zeros), real_rows, NN)
    fourier = read_fourier()
    others = [pieces[f, j, group] for f in (0, 1) for j in range(1, 8) for group in range(4)]
    rest = product(split(jnp.concatenate(others, 0)), fourier, NN)
    for f in (0, 1):
        upper = jnp.concatenate([first[32 * f : 32 * f + 32], rest[224 * f : 224 * f + 96]], 0)
        lower = rest[224 * f + 96 : 224 * f + 224]
        for h, rows in ((0, upper), (1, lower)):
            put(h, 0, f, rows[:, :128].T)
            put(h, 1, f, rows[:, 128:].T)
    return lanes


def wave_square(index, length):
    signed = jnp.where(2 * index >= length, index - length, index)
    phase_angle = signed.astype(f32) * (2.0 * math.pi / length)
    return phase_angle * phase_angle


def rates(wave_sq):
    numerator = 1.0 + time_step * stabilizer * wave_sq
    inverse = 1.0 / (numerator + time_step * kappa_grad * wave_sq * wave_sq)
    return numerator * inverse, time_step * wave_sq * inverse


def all_rates(section_at, lane_at, put):
    lane = lax.broadcasted_iota(jnp.int32, (128, 128), 1)
    row = lax.broadcasted_iota(jnp.int32, (128, 128), 0)
    slot = 4 * section_at + lane // 32
    y_index = jnp.where(slot == 0, 8 * lane_at, slot + 16 * lane_at)
    x_index = row + 128 * (lane % 16)
    wave_x = wave_square(x_index, NX)
    wave_xy = wave_x + wave_square(y_index, NY)
    half_y = (2.0 * math.pi / NY * (NY // 2)) ** 2
    for sigma in (0, 1):
        wave_z = wave_square(sigma + 2 * (lane // 16 % 2), NZ)
        for side, wave_sq in ((0, wave_z + wave_xy), (1, wave_z + (wave_x + half_y))):
            keep, mix = rates(wave_sq)
            put(sigma, side, 0, keep)
            put(sigma, side, 1, mix)


def middle(get, get_rate, section_at, lane_at, gather, lanes, spread_table, twist, put):
    lane = lax.broadcasted_iota(jnp.int32, (128, 128), 1)
    packed = (lane < 32) & (section_at == 0) & (lane_at == 0)
    cos, sin = twist[0], twist[1]
    parts = []
    for s in (0, 1):
        c_re, c_im, g_re, g_im = get(s, 0, 0), get(s, 1, 0), get(s, 0, 1), get(s, 1, 1)
        c_im, g_re = jnp.where(packed, g_re, c_im), jnp.where(packed, c_im, g_re)
        parts.append((c_re, c_im, g_re, g_im))
    stacked = []
    for sigma in (0, 1):
        mixed = [a + b if sigma == 0 else a - b for a, b in zip(*parts)]
        stacked.append(
            jnp.concatenate(
                [jnp.concatenate([mixed[0], mixed[2]], 1), jnp.concatenate([mixed[1], mixed[3]], 1)], 0
            )
        )
    tables = [(lanes[sigma, 0], lanes[sigma, 1]) for sigma in (0, 1)]

    def turn(spread):
        rows = []
        for f in (0, 1):
            re, im = spread[:128, 128 * f : 128 * f + 128], spread[128:, 128 * f : 128 * f + 128]
            rows.append(jnp.concatenate([re * cos + im * sin, im * cos - re * sin], 1))
        return split(jnp.concatenate(rows, 0))

    def filtered(sigma, spec):
        c_re, c_im, g_re, g_im = spec[:128, :128], spec[:128, 128:], spec[128:, :128], spec[128:, 128:]
        keep, mix = get_rate(sigma, 0, 0), get_rate(sigma, 0, 1)
        keep_half, mix_half = get_rate(sigma, 1, 0), get_rate(sigma, 1, 1)
        main_re = keep * c_re - mix * jnp.where(packed, c_im, g_re)
        main_im = keep * c_im - mix * jnp.where(packed, -c_re, g_im)
        side_re = keep_half * g_re - mix_half * g_im
        side_im = keep_half * g_im + mix_half * g_re
        rows = jnp.concatenate(
            [jnp.concatenate([main_re, main_im], 1), jnp.concatenate([side_re, side_im], 1)], 0
        )
        return split(rows)

    first = product(gather, split(stacked[0]), NN)
    second = product(gather, split(stacked[1]), NN)
    first = product(turn(first), tables[0], NN)
    second = product(turn(second), tables[1], NN)
    first = product(filtered(0, first), tables[0], NT)
    second = product(filtered(1, second), tables[1], NT)
    back = [first, second]
    for s in (0, 1):
        mixed = back[0] + back[1] if s == 0 else back[0] - back[1]
        both = []
        for f in (0, 1):
            re, im = mixed[128 * f : 128 * f + 128, :128], mixed[128 * f : 128 * f + 128, 128:]
            both.append((re * cos - im * sin, im * cos + re * sin))
        (m_re, m_im), (s_re, s_im) = both
        upper = jnp.concatenate([m_re, jnp.where(packed, s_re, m_im)], 1)
        lower = jnp.concatenate([-m_im, jnp.where(packed, -s_im, m_re)], 1)
        out = product(spread_table, split(jnp.concatenate([upper, lower], 0)), NN)
        put(s, 0, out[:, :128])
        put(s, 1, out[:, 128:])


def inverse_y(get, fourier, real_rows, twist, put):
    slots = []
    for h in (0, 1):
        re, im = get(h, 0), get(h, 1)
        if h == 0:
            row = lax.broadcasted_iota(jnp.int32, (128, 128), 0)
            lane = lax.broadcasted_iota(jnp.int32, (128, 128), 1)
            single = (row == 0) & (lane < 32)
            re, im = jnp.where(single, 0.5 * re, re), jnp.where(single, 0.5 * im, im)
        rows = split(jnp.concatenate([re.T, im.T], 1))
        if h == 0:
            first = product((rows[0][:32], rows[1][:32]), real_rows, NN)
            rows = (rows[0][32:], rows[1][32:])
        out = product(rows, fourier, NN)
        slots += [out[32 * m : 32 * m + 32] for m in range(out.shape[0] // 32)]
    scale = 2.0 / CELLS
    base = [first[:, :128] * scale, first[:, 128:] * scale]
    real, imag = {}, {}
    for j in range(1, 8):
        re, im = slots[j - 1][:, :128], slots[j - 1][:, 128:]
        cos, sin = twist[j : j + 1] * scale, twist[8 + j : 9 + j] * scale
        real[j], imag[j] = re * cos - im * sin, im * cos + re * sin
    ends, tips = real[2] + real[6], imag[6] - imag[2]
    near, far = (real[2] - real[6]) * COS16[2], (imag[2] + imag[6]) * COS16[2]
    part = [ends, near - far, tips, -(near + far)]
    four = [base[0] + real[4], base[1] - imag[4], base[0] - real[4], base[1] + imag[4]]
    even = [four[a] + part[a] for a in range(4)] + [four[a] - part[a] for a in range(4)]
    u, v, w, x = real[1] + real[7], real[3] + real[5], real[1] - real[7], real[3] - real[5]
    cosine = [u + v, w * COS16[1] + x * COS16[3], (u - v) * COS16[2], w * COS16[3] - x * COS16[1]]
    u, v, w, x = imag[1] + imag[7], imag[3] + imag[5], imag[1] - imag[7], imag[3] - imag[5]
    sine = [None, u * SIN16[1] + v * SIN16[3], (w + x) * SIN16[2], u * SIN16[3] - v * SIN16[1], w - x]
    put(0, even[0] + cosine[0])
    put(8, even[0] - cosine[0])
    for a in (1, 2, 3):
        odd, mirror = cosine[a] - sine[a], cosine[a] + sine[a]
        put(a, even[a] + odd)
        put(a + 8, even[a] - odd)
        put(8 - a, even[8 - a] - mirror)
        put(16 - a, even[8 - a] + mirror)
    put(4, even[4] - sine[4])
    put(12, even[4] + sine[4])


def lane_position():
    return (
        16 * lax.axis_index("slab_z")
        + 4 * lax.axis_index("slab_y")
        + 2 * lax.axis_index("slab_x")
        + lax.axis_index("slab_core")
    )


def forward_kernel(
    c_hbm,
    fourier_hbm,
    real_hbm,
    twist_hbm,
    out_ref,
    rate_ref,
    c_ref,
    fourier_ref,
    real_ref,
    twist_ref,
    sems,
):
    def group_of(ref, n):
        return ref.at[n // 2, pl.ds(8 * (n % 2), 8), :]

    sources = [group_of(c_hbm, n) for n in range(4)] + [twist_hbm, real_hbm, fourier_hbm]
    targets = [group_of(c_ref, n) for n in range(4)] + [twist_ref, real_ref, fourier_ref]
    copies = [
        pltpu.make_async_copy(source, target, sems.at[n])
        for n, (source, target) in enumerate(zip(sources, targets))
    ]
    for copy in copies:
        copy.start()

    def put(h, part, f, value):
        out_ref[pl.ds(640 * h + 2 * part + f, 128, stride=5), :] = value

    def put_rate(sigma, side, kind, value):
        rate_ref[4 * sigma + 2 * side + kind] = value

    def late(n, ref):
        def read():
            copies[n].wait()
            return ref[...]

        return read

    all_rates(lax.axis_index("section"), lane_position(), put_rate)
    def read_rows(n):
        copies[n].wait()
        return c_ref[n // 2, 8 * (n % 2) : 8 * (n % 2) + 8, :]

    lanes = forward_y(read_rows, late(6, fourier_ref), late(5, real_ref), late(4, twist_ref), put)
    out_ref[pl.ds(4, 256, stride=5), :] = jnp.broadcast_to(jnp.sum(lanes, 0, keepdims=True), (256, 128))


def middle_kernel(
    in_ref, rate_ref, gather_ref, lanes_ref, spread_ref, twist_ref, out_ref, bulk_ref
):
    def get(s, part, f):
        return in_ref[pl.ds(640 * s + 2 * part + f, 128, stride=5), :]

    def put(s, part, value):
        out_ref[pl.ds(256 * s + part, 128, stride=2), :] = value

    middle(
        get,
        lambda sigma, side, kind: rate_ref[4 * sigma + 2 * side + kind],
        lax.axis_index("section"),
        lane_position(),
        (gather_ref[0], gather_ref[1]),
        lanes_ref,
        (spread_ref[0], spread_ref[1]),
        twist_ref,
        put,
    )
    bulk = jnp.sum(in_ref[pl.ds(4, 256, stride=5), :], 0, keepdims=True)
    bulk_ref[...] = jnp.broadcast_to(bulk, (8, 128))


def inverse_kernel(in_ref, bulk_ref, fourier_ref, real_ref, twist_ref, out_ref, energy_ref):
    def get(h, part):
        return in_ref[pl.ds(256 * h + part, 128, stride=2), :]

    def put(a, value):
        out_ref[0, :, 128 * a : 128 * a + 128] = value[:16]
        out_ref[1, :, 128 * a : 128 * a + 128] = value[16:]

    energy_ref[...] = jnp.sum(bulk_ref[0:1, :], keepdims=True) * (1.0 / CELLS)
    inverse_y(
        get, (fourier_ref[0], fourier_ref[1]), (real_ref[0], real_ref[1]), twist_ref[...], put
    )


def exchange(rows):
    width = rows.shape[0] // 256
    message = rows.reshape(256, 1, 128 * width)
    return lax.all_to_all(message, ALL, split_axis=0, concat_axis=0, tiled=True).reshape(rows.shape)


def per_device(concentration):
    whole = pl.BlockSpec(memory_space=pltpu.VMEM)
    params = pltpu.CompilerParams(vmem_limit_bytes=12 << 20)
    outgoing, rate = pl.pallas_call(
        forward_kernel,
        out_shape=(
            pltpu.VMEM((1280, 128), f32),
            pltpu.VMEM((8, 128, 128), f32),
        ),
        in_specs=[pl.BlockSpec(memory_space=pltpu.HBM)] * 4,
        out_specs=(whole, whole),
        scratch_shapes=[
            pltpu.VMEM(concentration.shape, f32),
            pltpu.VMEM(FOURIER.shape, bf16),
            pltpu.VMEM(REAL.shape, bf16),
            pltpu.VMEM(Y_TWIST.shape, f32),
            pltpu.SemaphoreType.DMA((7,)),
        ],
        compiler_params=params,
    )(*[pltpu.with_memory_space_constraint(a, pltpu.HBM) for a in (concentration, FOURIER_T, REAL_T, Y_TWIST)])
    columns = exchange(outgoing)
    leaving, bulk = pl.pallas_call(
        middle_kernel,
        out_shape=(pltpu.VMEM((512, 128), f32), pltpu.VMEM((8, 128), f32)),
        in_specs=[whole] * 6,
        out_specs=(whole, whole),
        compiler_params=pltpu.CompilerParams(vmem_limit_bytes=12 << 20),
    )(columns, rate, GATHER, LANES, SPREAD, X_TWIST)
    rows_back = exchange(leaving)
    new_field, energy = pl.pallas_call(
        inverse_kernel,
        out_shape=(jax.ShapeDtypeStruct(concentration.shape, f32), jax.ShapeDtypeStruct((1, 1), f32)),
        in_specs=[whole] * 5,
        out_specs=(whole, whole),
        compiler_params=params,
    )(rows_back, bulk, FOURIER, REAL, Y_TWIST)
    return new_field, energy.reshape(())


def solution(mesh):
    finer = Mesh(mesh.devices.reshape(2, 4, 2, 8, 2), ("section",) + SLAB)
    return jax.shard_map(
        per_device,
        mesh=finer,
        in_specs=(P("section", SLAB, None),),
        out_specs=(P("section", SLAB, None), P()),
        check_vma=False,
    )
```

```python
import math

import jax
import jax.numpy as jnp
import ml_dtypes
import numpy as np
from jax import lax
from jax.experimental import pallas as pl
from jax.experimental.pallas import tpu as pltpu
from jax.sharding import Mesh
from jax.sharding import PartitionSpec as P

SLAB = ("slab_y", "slab_x", "slab_z", "slab_core")
ALL = ("section", "slab_z", "slab_y", "slab_x", "slab_core")
NX = 2048
NY = 2048
NZ = 4
CELLS = NX * NY * NZ
time_step = 100.0
kappa_grad = 2.0
stabilizer = 8.0
f32 = jnp.float32
bf16 = jnp.bfloat16


def halves(matrix):
    high = matrix.astype(np.float32).astype(ml_dtypes.bfloat16)
    low = (matrix - high.astype(np.float64)).astype(np.float32).astype(ml_dtypes.bfloat16)
    return np.stack([high, low])


def fourier_table():
    index = np.arange(128)
    angle = 2.0 * np.pi * (np.outer(index, index) % 128) / 128
    return halves(np.block([[np.cos(angle), np.sin(angle)], [-np.sin(angle), np.cos(angle)]]))


def slab_order():
    return np.arange(128).reshape(4, 2, 8, 2).transpose(2, 0, 1, 3).reshape(128)


def real_table():
    angle = 2.0 * np.pi * (np.outer(np.arange(128), np.arange(256)) % 256) / 256
    lower = -np.sin(angle)
    lower[0] = 1.0 - 2.0 * (np.arange(256) % 2)
    return halves(np.concatenate([np.cos(angle), lower], 0))


def lane_table(parity):
    z_at, x_at = np.arange(2)[:, None, None, None], np.arange(16)[None, :, None, None]
    t_at, q_at = np.arange(2)[None, None, :, None], np.arange(16)[None, None, None, :]
    turn = (4 * parity * z_at + 8 * t_at * z_at + x_at * q_at) % 16
    value = np.exp(-2j * np.pi * turn / 16).reshape(32, 32)
    value = np.kron(np.eye(4), value)
    return halves(np.block([[value.real, value.imag], [-value.imag, value.real]]))


def y_twist_table():
    angle = 2.0 * np.pi * np.outer(np.arange(8), np.arange(128)) / 2048
    return np.concatenate([np.cos(angle), np.sin(angle)], 0).astype(np.float32)


def x_twist_table():
    angle = 2.0 * np.pi * np.outer(np.arange(128), np.arange(128) % 16) / 2048
    return np.stack([np.cos(angle), np.sin(angle)]).astype(np.float32)


FOURIER = fourier_table()
ORDER = slab_order()
GATHER = FOURIER[:, :, np.concatenate([ORDER, 128 + ORDER])]
SPREAD = FOURIER[:, ORDER, :]
REAL = real_table()
LANES = np.stack([lane_table(0), lane_table(1)])
FOURIER_T = FOURIER.transpose(0, 2, 1)
REAL_T = REAL.transpose(0, 2, 1)
Y_TWIST = y_twist_table()
X_TWIST = x_twist_table()
COS16 = [math.cos(2.0 * math.pi * m / 16) for m in range(16)]
SIN16 = [math.sin(2.0 * math.pi * m / 16) for m in range(16)]


def split(value):
    high = value.astype(bf16)
    return high, (value - high.astype(f32)).astype(bf16)


NN = (((1,), (0,)), ((), ()))
NT = (((1,), (1,)), ((), ()))


def product(left, right, pattern):
    total = left[0].shape[0]
    both = lax.dot_general(
        jnp.concatenate(left, 0), right[0], pattern, preferred_element_type=f32
    )
    rest = lax.dot_general(left[0], right[1], pattern, preferred_element_type=f32)
    return both[:total] + (both[total:] + rest)


def y_slots(at):
    add = [at[a] + at[a + 8] for a in range(8)]
    sub = [at[a] - at[a + 8] for a in range(8)]
    both = [add[a] + add[a + 4] for a in range(4)]
    diff = [add[a] - add[a + 4] for a in range(4)]
    zero = jnp.concatenate([both[0] + both[2], both[1] + both[3]], 1)
    near, far = (diff[1] - diff[3]) * COS16[2], (diff[1] + diff[3]) * COS16[2]
    minus = [None] + [sub[a] - sub[8 - a] for a in (1, 2, 3)]
    plus = [None] + [sub[a] + sub[8 - a] for a in (1, 2, 3)]
    middle_re = minus[2] * COS16[2]
    re_17, re_35 = sub[0] + middle_re, sub[0] - middle_re
    re_1, re_3 = minus[1] * COS16[1] + minus[3] * COS16[3], minus[1] * COS16[3] - minus[3] * COS16[1]
    im_1, im_3 = plus[1] * SIN16[1] + plus[3] * SIN16[3], plus[1] * SIN16[3] - plus[3] * SIN16[1]
    middle_im = plus[2] * SIN16[2]
    im_17, im_35 = middle_im + sub[4], middle_im - sub[4]
    return [
        zero,
        (re_17 + re_1, im_1 + im_17, -1),
        (diff[0] + near, diff[2] + far, -1),
        (re_35 + re_3, im_3 + im_35, -1),
        (both[0] - both[2], both[3] - both[1], 1),
        (re_35 - re_3, im_35 - im_3, 1),
        (diff[0] - near, diff[2] - far, 1),
        (re_17 - re_1, im_17 - im_1, 1),
    ]


def turned_slots(at, turns):
    slots = y_slots(at)
    for j in range(1, 8):
        re, n, sign = slots[j]
        cos, sin, negative = turns[j]
        if sign > 0:
            turned = [re * cos + n * sin, n * cos - re * sin]
        else:
            turned = [re * cos - n * sin, n * negative - re * sin]
        slots[j] = jnp.concatenate(turned, 1)
    return slots


def forward_y(read_rows, read_fourier, read_real, read_twist, put):
    twist = read_twist()
    turns = [(twist[j : j + 1], twist[8 + j : 9 + j], -twist[j : j + 1]) for j in range(8)]
    blocks, slots = [], []
    for group in range(4):
        rows = read_rows(group)
        blocks.append([rows[:, 128 * a : 128 * a + 128] for a in range(16)])
        slots.append(turned_slots(blocks[group], turns))
    real_rows = read_real()
    fourier = read_fourier()
    lanes = None
    for f in (0, 1):
        if f == 1:
            slots = []
            for block in blocks:
                cubic = []
                for value in block:
                    squared = value * value
                    bulk = squared * (0.25 * squared - 0.5)
                    lanes = bulk if lanes is None else lanes + bulk
                    cubic.append(squared * value - value)
                slots.append(turned_slots(cubic, turns))
        first = product(split(jnp.concatenate([slot[0] for slot in slots], 0)), real_rows, NN)
        others = [slot[j] for j in range(1, 8) for slot in slots]
        rest = product(split(jnp.concatenate(others, 0)), fourier, NN)
        for h, rows in ((0, jnp.concatenate([first, rest[:96]], 0)), (1, rest[96:])):
            put(h, 0, f, rows[:, :128].T)
            put(h, 1, f, rows[:, 128:].T)
    return lanes


def wave_square(index, length):
    signed = jnp.where(2 * index >= length, index - length, index)
    phase_angle = signed.astype(f32) * (2.0 * math.pi / length)
    return phase_angle * phase_angle


def rates(wave_sq):
    numerator = 1.0 + time_step * stabilizer * wave_sq
    inverse = 1.0 / (numerator + time_step * kappa_grad * wave_sq * wave_sq)
    return numerator * inverse, time_step * wave_sq * inverse


def all_rates(section_at, lane_at, put):
    lane = lax.broadcasted_iota(jnp.int32, (128, 128), 1)
    row = lax.broadcasted_iota(jnp.int32, (128, 128), 0)
    slot = 4 * section_at + lane // 32
    y_index = jnp.where(slot == 0, 8 * lane_at, slot + 16 * lane_at)
    x_index = row + 128 * (lane % 16)
    wave_x = wave_square(x_index, NX)
    wave_xy = wave_x + wave_square(y_index, NY)
    half_y = (2.0 * math.pi / NY * (NY // 2)) ** 2
    for sigma in (0, 1):
        wave_z = wave_square(sigma + 2 * (lane // 16 % 2), NZ)
        for side, wave_sq in ((0, wave_z + wave_xy), (1, wave_z + (wave_x + half_y))):
            keep, mix = rates(wave_sq)
            put(sigma, side, 0, keep)
            put(sigma, side, 1, mix)


def middle(get, get_rate, section_at, lane_at, gather, lanes, spread_table, twist, put):
    lane = lax.broadcasted_iota(jnp.int32, (128, 128), 1)
    packed = (lane < 32) & (section_at == 0) & (lane_at == 0)
    cos, sin = twist[0], twist[1]
    parts = []
    for s in (0, 1):
        c_re, c_im, g_re, g_im = get(s, 0, 0), get(s, 1, 0), get(s, 0, 1), get(s, 1, 1)
        c_im, g_re = jnp.where(packed, g_re, c_im), jnp.where(packed, c_im, g_re)
        parts.append((c_re, c_im, g_re, g_im))
    stacked = []
    for sigma in (0, 1):
        mixed = [a + b if sigma == 0 else a - b for a, b in zip(*parts)]
        stacked.append(
            jnp.concatenate(
                [jnp.concatenate([mixed[0], mixed[2]], 1), jnp.concatenate([mixed[1], mixed[3]], 1)], 0
            )
        )
    spreads = [product(gather, split(stacked[sigma]), NN) for sigma in (0, 1)]
    turned = []
    for spread in spreads:
        rows = []
        for f in (0, 1):
            re, im = spread[:128, 128 * f : 128 * f + 128], spread[128:, 128 * f : 128 * f + 128]
            rows.append(jnp.concatenate([re * cos + im * sin, im * cos - re * sin], 1))
        turned.append(split(jnp.concatenate(rows, 0)))
    tables = [(lanes[sigma, 0], lanes[sigma, 1]) for sigma in (0, 1)]
    specs = [product(turned[sigma], tables[sigma], NN) for sigma in (0, 1)]
    filtered = []
    for sigma, spec in enumerate(specs):
        c_re, c_im, g_re, g_im = spec[:128, :128], spec[:128, 128:], spec[128:, :128], spec[128:, 128:]
        keep, mix = get_rate(sigma, 0, 0), get_rate(sigma, 0, 1)
        keep_half, mix_half = get_rate(sigma, 1, 0), get_rate(sigma, 1, 1)
        main_re = keep * c_re - mix * jnp.where(packed, c_im, g_re)
        main_im = keep * c_im - mix * jnp.where(packed, -c_re, g_im)
        side_re = keep_half * g_re - mix_half * g_im
        side_im = keep_half * g_im + mix_half * g_re
        rows = jnp.concatenate(
            [jnp.concatenate([main_re, main_im], 1), jnp.concatenate([side_re, side_im], 1)], 0
        )
        filtered.append(split(rows))
    back = [product(filtered[sigma], tables[sigma], NT) for sigma in (0, 1)]
    for s in (0, 1):
        mixed = back[0] + back[1] if s == 0 else back[0] - back[1]
        both = []
        for f in (0, 1):
            re, im = mixed[128 * f : 128 * f + 128, :128], mixed[128 * f : 128 * f + 128, 128:]
            both.append((re * cos - im * sin, im * cos + re * sin))
        (m_re, m_im), (s_re, s_im) = both
        upper = jnp.concatenate([m_re, jnp.where(packed, s_re, m_im)], 1)
        lower = jnp.concatenate([-m_im, jnp.where(packed, -s_im, m_re)], 1)
        out = product(spread_table, split(jnp.concatenate([upper, lower], 0)), NN)
        put(s, 0, out[:, :128])
        put(s, 1, out[:, 128:])


def inverse_y(get, fourier, real_rows, twist, put):
    slots = []
    for h in (0, 1):
        re, im = get(h, 0), get(h, 1)
        if h == 0:
            row = lax.broadcasted_iota(jnp.int32, (128, 128), 0)
            lane = lax.broadcasted_iota(jnp.int32, (128, 128), 1)
            single = (row == 0) & (lane < 32)
            re, im = jnp.where(single, 0.5 * re, re), jnp.where(single, 0.5 * im, im)
        rows = split(jnp.concatenate([re.T, im.T], 1))
        if h == 0:
            first = product((rows[0][:32], rows[1][:32]), real_rows, NN)
            rows = (rows[0][32:], rows[1][32:])
        out = product(rows, fourier, NN)
        slots += [out[32 * m : 32 * m + 32] for m in range(out.shape[0] // 32)]
    scale = 2.0 / CELLS
    base = [first[:, :128] * scale, first[:, 128:] * scale]
    real, imag = {}, {}
    for j in range(1, 8):
        re, im = slots[j - 1][:, :128], slots[j - 1][:, 128:]
        cos, sin = twist[j : j + 1] * scale, twist[8 + j : 9 + j] * scale
        real[j], imag[j] = re * cos - im * sin, im * cos + re * sin
    ends, tips = real[2] + real[6], imag[6] - imag[2]
    near, far = (real[2] - real[6]) * COS16[2], (imag[2] + imag[6]) * COS16[2]
    part = [ends, near - far, tips, -(near + far)]
    four = [base[0] + real[4], base[1] - imag[4], base[0] - real[4], base[1] + imag[4]]
    even = [four[a] + part[a] for a in range(4)] + [four[a] - part[a] for a in range(4)]
    u, v, w, x = real[1] + real[7], real[3] + real[5], real[1] - real[7], real[3] - real[5]
    cosine = [u + v, w * COS16[1] + x * COS16[3], (u - v) * COS16[2], w * COS16[3] - x * COS16[1]]
    u, v, w, x = imag[1] + imag[7], imag[3] + imag[5], imag[1] - imag[7], imag[3] - imag[5]
    sine = [None, u * SIN16[1] + v * SIN16[3], (w + x) * SIN16[2], u * SIN16[3] - v * SIN16[1], w - x]
    put(0, even[0] + cosine[0])
    put(8, even[0] - cosine[0])
    for a in (1, 2, 3):
        odd, mirror = cosine[a] - sine[a], cosine[a] + sine[a]
        put(a, even[a] + odd)
        put(a + 8, even[a] - odd)
        put(8 - a, even[8 - a] - mirror)
        put(16 - a, even[8 - a] + mirror)
    put(4, even[4] - sine[4])
    put(12, even[4] + sine[4])


def lane_position():
    return (
        16 * lax.axis_index("slab_z")
        + 4 * lax.axis_index("slab_y")
        + 2 * lax.axis_index("slab_x")
        + lax.axis_index("slab_core")
    )


def forward_kernel(
    c_hbm,
    fourier_hbm,
    real_hbm,
    twist_hbm,
    out_ref,
    rate_ref,
    c_ref,
    fourier_ref,
    real_ref,
    twist_ref,
    sems,
):
    def group_of(ref, n):
        return ref.at[n // 2, pl.ds(8 * (n % 2), 8), :]

    sources = [twist_hbm] + [group_of(c_hbm, n) for n in range(4)] + [real_hbm, fourier_hbm]
    targets = [twist_ref] + [group_of(c_ref, n) for n in range(4)] + [real_ref, fourier_ref]
    copies = [
        pltpu.make_async_copy(source, target, sems.at[n])
        for n, (source, target) in enumerate(zip(sources, targets))
    ]
    for copy in copies:
        copy.start()

    def put(h, part, f, value):
        out_ref[pl.ds(640 * h + 2 * part + f, 128, stride=5), :] = value

    def put_rate(sigma, side, kind, value):
        rate_ref[4 * sigma + 2 * side + kind] = value

    def late(n, ref):
        def read():
            copies[n].wait()
            return ref[...]

        return read

    all_rates(lax.axis_index("section"), lane_position(), put_rate)
    def read_rows(n):
        copies[n + 1].wait()
        return c_ref[n // 2, 8 * (n % 2) : 8 * (n % 2) + 8, :]

    lanes = forward_y(read_rows, late(6, fourier_ref), late(5, real_ref), late(0, twist_ref), put)
    out_ref[pl.ds(4, 256, stride=5), :] = jnp.broadcast_to(jnp.sum(lanes, 0, keepdims=True), (256, 128))


def middle_kernel(
    in_ref, rate_ref, gather_ref, lanes_ref, spread_ref, twist_ref, out_ref, bulk_ref
):
    def get(s, part, f):
        return in_ref[pl.ds(640 * s + 2 * part + f, 128, stride=5), :]

    def put(s, part, value):
        out_ref[pl.ds(256 * s + part, 128, stride=2), :] = value

    middle(
        get,
        lambda sigma, side, kind: rate_ref[4 * sigma + 2 * side + kind],
        lax.axis_index("section"),
        lane_position(),
        (gather_ref[0], gather_ref[1]),
        lanes_ref,
        (spread_ref[0], spread_ref[1]),
        twist_ref,
        put,
    )
    bulk = jnp.sum(in_ref[pl.ds(4, 256, stride=5), :], 0, keepdims=True)
    bulk_ref[...] = jnp.broadcast_to(bulk, (8, 128))


def inverse_kernel(in_ref, bulk_ref, fourier_ref, real_ref, twist_ref, out_ref, energy_ref):
    def get(h, part):
        return in_ref[pl.ds(256 * h + part, 128, stride=2), :]

    def put(a, value):
        out_ref[0, :, 128 * a : 128 * a + 128] = value[:16]
        out_ref[1, :, 128 * a : 128 * a + 128] = value[16:]

    energy_ref[...] = jnp.sum(bulk_ref[0:1, :], keepdims=True) * (1.0 / CELLS)
    inverse_y(
        get, (fourier_ref[0], fourier_ref[1]), (real_ref[0], real_ref[1]), twist_ref[...], put
    )


def exchange(rows):
    width = rows.shape[0] // 256
    message = rows.reshape(256, 1, 128 * width)
    return lax.all_to_all(message, ALL, split_axis=0, concat_axis=0, tiled=True).reshape(rows.shape)


def per_device(concentration):
    whole = pl.BlockSpec(memory_space=pltpu.VMEM)
    params = pltpu.CompilerParams(vmem_limit_bytes=12 << 20)
    outgoing, rate = pl.pallas_call(
        forward_kernel,
        out_shape=(
            pltpu.VMEM((1280, 128), f32),
            pltpu.VMEM((8, 128, 128), f32),
        ),
        in_specs=[pl.BlockSpec(memory_space=pltpu.HBM)] * 4,
        out_specs=(whole, whole),
        scratch_shapes=[
            pltpu.VMEM(concentration.shape, f32),
            pltpu.VMEM(FOURIER.shape, bf16),
            pltpu.VMEM(REAL.shape, bf16),
            pltpu.VMEM(Y_TWIST.shape, f32),
            pltpu.SemaphoreType.DMA((7,)),
        ],
        compiler_params=params,
    )(*[pltpu.with_memory_space_constraint(a, pltpu.HBM) for a in (concentration, FOURIER_T, REAL_T, Y_TWIST)])
    columns = exchange(outgoing)
    leaving, bulk = pl.pallas_call(
        middle_kernel,
        out_shape=(pltpu.VMEM((512, 128), f32), pltpu.VMEM((8, 128), f32)),
        in_specs=[whole] * 6,
        out_specs=(whole, whole),
        compiler_params=params,
    )(columns, rate, GATHER, LANES, SPREAD, X_TWIST)
    rows_back = exchange(leaving)
    new_field, energy = pl.pallas_call(
        inverse_kernel,
        out_shape=(jax.ShapeDtypeStruct(concentration.shape, f32), jax.ShapeDtypeStruct((1, 1), f32)),
        in_specs=[whole] * 5,
        out_specs=(whole, whole),
        compiler_params=params,
    )(rows_back, bulk, FOURIER, REAL, Y_TWIST)
    return new_field, energy.reshape(())


def solution(mesh):
    finer = Mesh(mesh.devices.reshape(2, 4, 2, 8, 2), ("section",) + SLAB)
    return jax.shard_map(
        per_device,
        mesh=finer,
        in_specs=(P("section", SLAB, None),),
        out_specs=(P("section", SLAB, None), P()),
        check_vma=False,
    )
```

```python
import math

import jax
import jax.numpy as jnp
import ml_dtypes
import numpy as np
from jax import lax
from jax.experimental import pallas as pl
from jax.experimental.pallas import tpu as pltpu
from jax.sharding import Mesh
from jax.sharding import PartitionSpec as P

SLAB = ("slab_y", "slab_x", "slab_z", "slab_core")
ALL = ("section", "slab_z", "slab_y", "slab_x", "slab_core")
NX = 2048
NY = 2048
NZ = 4
CELLS = NX * NY * NZ
time_step = 100.0
kappa_grad = 2.0
stabilizer = 8.0
f32 = jnp.float32
bf16 = jnp.bfloat16


def halves(matrix):
    high = matrix.astype(np.float32).astype(ml_dtypes.bfloat16)
    low = (matrix - high.astype(np.float64)).astype(np.float32).astype(ml_dtypes.bfloat16)
    return np.stack([high, low])


def fourier_table():
    index = np.arange(128)
    angle = 2.0 * np.pi * (np.outer(index, index) % 128) / 128
    return halves(np.block([[np.cos(angle), np.sin(angle)], [-np.sin(angle), np.cos(angle)]]))


def slab_order():
    return np.arange(128).reshape(4, 2, 8, 2).transpose(2, 0, 1, 3).reshape(128)


def real_table():
    angle = 2.0 * np.pi * (np.outer(np.arange(128), np.arange(256)) % 256) / 256
    lower = -np.sin(angle)
    lower[0] = 1.0 - 2.0 * (np.arange(256) % 2)
    return halves(np.concatenate([np.cos(angle), lower], 0))


def lane_table(parity):
    z_at, x_at = np.arange(2)[:, None, None, None], np.arange(16)[None, :, None, None]
    t_at, q_at = np.arange(2)[None, None, :, None], np.arange(16)[None, None, None, :]
    turn = (4 * parity * z_at + 8 * t_at * z_at + x_at * q_at) % 16
    value = np.exp(-2j * np.pi * turn / 16).reshape(32, 32)
    value = np.kron(np.eye(4), value)
    return halves(np.block([[value.real, value.imag], [-value.imag, value.real]]))


def y_twist_table():
    angle = 2.0 * np.pi * np.outer(np.arange(8), np.arange(128)) / 2048
    return np.concatenate([np.cos(angle), np.sin(angle)], 0).astype(np.float32)


def x_twist_table():
    angle = 2.0 * np.pi * np.outer(np.arange(128), np.arange(128) % 16) / 2048
    return np.stack([np.cos(angle), np.sin(angle)]).astype(np.float32)


FOURIER = fourier_table()
ORDER = slab_order()
GATHER = FOURIER[:, :, np.concatenate([ORDER, 128 + ORDER])]
SPREAD = np.concatenate([FOURIER[:, ORDER, :128], -FOURIER[:, ORDER, 128:]], 2)
REAL = real_table()
LANES = np.stack([lane_table(0), lane_table(1)])
FOURIER_T = FOURIER.transpose(0, 2, 1)
REAL_T = REAL.transpose(0, 2, 1)
Y_TWIST = y_twist_table()
X_TWIST = x_twist_table()
COS16 = [math.cos(2.0 * math.pi * m / 16) for m in range(16)]
SIN16 = [math.sin(2.0 * math.pi * m / 16) for m in range(16)]


def split(value):
    high = value.astype(bf16)
    return high, (value - high.astype(f32)).astype(bf16)


NN = (((1,), (0,)), ((), ()))
NT = (((1,), (1,)), ((), ()))


def product(left, right, pattern):
    total = left[0].shape[0]
    both = lax.dot_general(
        jnp.concatenate(left, 0), right[0], pattern, preferred_element_type=f32
    )
    rest = lax.dot_general(left[0], right[1], pattern, preferred_element_type=f32)
    return both[:total] + (both[total:] + rest)


def y_slots(at):
    add = [at[a] + at[a + 8] for a in range(8)]
    sub = [at[a] - at[a + 8] for a in range(8)]
    both = [add[a] + add[a + 4] for a in range(4)]
    diff = [add[a] - add[a + 4] for a in range(4)]
    zero = jnp.concatenate([both[0] + both[2], both[1] + both[3]], 1)
    near, far = (diff[1] - diff[3]) * COS16[2], (diff[1] + diff[3]) * COS16[2]
    minus = [None] + [sub[a] - sub[8 - a] for a in (1, 2, 3)]
    plus = [None] + [sub[a] + sub[8 - a] for a in (1, 2, 3)]
    middle_re = minus[2] * COS16[2]
    re_17, re_35 = sub[0] + middle_re, sub[0] - middle_re
    re_1, re_3 = minus[1] * COS16[1] + minus[3] * COS16[3], minus[1] * COS16[3] - minus[3] * COS16[1]
    im_1, im_3 = plus[1] * SIN16[1] + plus[3] * SIN16[3], plus[1] * SIN16[3] - plus[3] * SIN16[1]
    middle_im = plus[2] * SIN16[2]
    im_17, im_35 = middle_im + sub[4], middle_im - sub[4]
    return [
        zero,
        (re_17 + re_1, im_1 + im_17, -1),
        (diff[0] + near, diff[2] + far, -1),
        (re_35 + re_3, im_3 + im_35, -1),
        (both[0] - both[2], both[3] - both[1], 1),
        (re_35 - re_3, im_35 - im_3, 1),
        (diff[0] - near, diff[2] - far, 1),
        (re_17 - re_1, im_17 - im_1, 1),
    ]


def turned_slots(at, turns):
    slots = y_slots(at)
    for j in range(1, 8):
        re, n, sign = slots[j]
        cos, sin, negative = turns[j]
        if sign > 0:
            turned = [re * cos + n * sin, n * cos - re * sin]
        else:
            turned = [re * cos - n * sin, n * negative - re * sin]
        slots[j] = jnp.concatenate(turned, 1)
    return slots


def forward_y(read_rows, read_fourier, read_real, read_twist, put):
    twist = read_twist()
    turns = [(twist[j : j + 1], twist[8 + j : 9 + j], -twist[j : j + 1]) for j in range(8)]
    blocks, slots = [], []
    for group in range(4):
        rows = read_rows(group)
        blocks.append([rows[:, 128 * a : 128 * a + 128] for a in range(16)])
        slots.append(turned_slots(blocks[group], turns))
    real_rows = read_real()
    fourier = read_fourier()
    lanes = None
    for f in (0, 1):
        if f == 1:
            slots = []
            for block in blocks:
                cubic = []
                for value in block:
                    squared = value * value
                    bulk = squared * (0.25 * squared - 0.5)
                    lanes = bulk if lanes is None else lanes + bulk
                    cubic.append(squared * value - value)
                slots.append(turned_slots(cubic, turns))
        first = product(split(jnp.concatenate([slot[0] for slot in slots], 0)), real_rows, NN)
        others = [slot[j] for j in range(1, 8) for slot in slots]
        rest = product(split(jnp.concatenate(others, 0)), fourier, NN)
        for h, rows in ((0, jnp.concatenate([first, rest[:96]], 0)), (1, rest[96:])):
            put(h, 0, f, rows[:, :128].T)
            put(h, 1, f, rows[:, 128:].T)
    return lanes


def wave_square(index, length):
    signed = jnp.where(2 * index >= length, index - length, index)
    phase_angle = signed.astype(f32) * (2.0 * math.pi / length)
    return phase_angle * phase_angle


def rates(wave_sq):
    numerator = 1.0 + time_step * stabilizer * wave_sq
    inverse = 1.0 / (numerator + time_step * kappa_grad * wave_sq * wave_sq)
    return numerator * inverse, time_step * wave_sq * inverse


def all_rates(section_at, lane_at, put):
    lane = lax.broadcasted_iota(jnp.int32, (128, 128), 1)
    row = lax.broadcasted_iota(jnp.int32, (128, 128), 0)
    slot = 4 * section_at + lane // 32
    y_index = jnp.where(slot == 0, 8 * lane_at, slot + 16 * lane_at)
    x_index = row + 128 * (lane % 16)
    wave_x = wave_square(x_index, NX)
    wave_xy = wave_x + wave_square(y_index, NY)
    half_y = (2.0 * math.pi / NY * (NY // 2)) ** 2
    side_row = lax.broadcasted_iota(jnp.int32, (32, 128), 0)
    side_lane = lax.broadcasted_iota(jnp.int32, (32, 128), 1)
    side_x = wave_square(side_row + 32 * (side_lane // 32) + 128 * (side_lane % 16), NX)
    for sigma in (0, 1):
        for kind, value in enumerate(rates(wave_square(sigma + 2 * (lane // 16 % 2), NZ) + wave_xy)):
            put(sigma, 0, kind, value)
        side_z = wave_square(sigma + 2 * (side_lane // 16 % 2), NZ)
        for kind, value in enumerate(rates(side_z + (side_x + half_y))):
            put(sigma, 1, kind, value)


def pack(value, roll):
    lane = lax.broadcasted_iota(jnp.int32, (32, 128), 1)
    total = value[:32]
    for n in (1, 2, 3):
        total = jnp.where(lane // 32 == n, roll(value[32 * n : 32 * n + 32], 32 * n, 1), total)
    return total


def unpack(value, roll):
    return jnp.concatenate([value] + [roll(value, 128 - 32 * n, 1) for n in (1, 2, 3)], 0)


def middle(roll, get, get_rate, section_at, lane_at, gather, lanes, spread_table, twist, put):
    lane = lax.broadcasted_iota(jnp.int32, (128, 128), 1)
    packed = (lane < 32) & (section_at == 0) & (lane_at == 0)
    cos, sin = twist[0], twist[1]
    parts = []
    for s in (0, 1):
        c_re, c_im, g_re, g_im = get(s, 0, 0), get(s, 1, 0), get(s, 0, 1), get(s, 1, 1)
        c_im, g_re = jnp.where(packed, g_re, c_im), jnp.where(packed, c_im, g_re)
        parts.append((c_re, c_im, g_re, g_im))
    stacked = []
    for sigma in (0, 1):
        mixed = [a + b if sigma == 0 else a - b for a, b in zip(*parts)]
        stacked.append(
            jnp.concatenate(
                [jnp.concatenate([mixed[0], mixed[2]], 1), jnp.concatenate([mixed[1], mixed[3]], 1)], 0
            )
        )
    spreads = [product(gather, split(stacked[sigma]), NN) for sigma in (0, 1)]
    turned = []
    for spread in spreads:
        rows = []
        for f in (0, 1):
            re, im = spread[:128, 128 * f : 128 * f + 128], spread[128:, 128 * f : 128 * f + 128]
            rows.append(jnp.concatenate([re * cos + im * sin, im * cos - re * sin], 1))
        turned.append(split(jnp.concatenate(rows, 0)))
    tables = [(lanes[sigma, 0], lanes[sigma, 1]) for sigma in (0, 1)]
    specs = [product(turned[sigma], tables[sigma], NN) for sigma in (0, 1)]
    filtered = []
    for sigma, spec in enumerate(specs):
        c_re, c_im, g_re, g_im = spec[:128, :128], spec[:128, 128:], spec[128:, :128], spec[128:, 128:]
        keep, mix = get_rate(sigma, 0, 0), get_rate(sigma, 0, 1)
        keep_half, mix_half = get_rate(sigma, 1, 0), get_rate(sigma, 1, 1)
        main_re = keep * c_re - mix * jnp.where(packed, c_im, g_re)
        main_im = keep * c_im - mix * jnp.where(packed, -c_re, g_im)
        g_re, g_im = pack(g_re, roll), pack(g_im, roll)
        side_re = keep_half * g_re - mix_half * g_im
        side_im = keep_half * g_im + mix_half * g_re
        rows = jnp.concatenate(
            [jnp.concatenate([main_re, main_im], 1), jnp.concatenate([side_re, side_im], 1)], 0
        )
        filtered.append(split(rows))
    back = [product(filtered[sigma], tables[sigma], NT) for sigma in (0, 1)]
    for s in (0, 1):
        mixed = back[0] + back[1] if s == 0 else back[0] - back[1]
        re, im = mixed[:128, :128], mixed[:128, 128:]
        side_re, side_im = unpack(mixed[128:, :128], roll), unpack(mixed[128:, 128:], roll)
        other_re, other_im = jnp.where(packed, side_re, im), jnp.where(packed, side_im, -re)
        upper = jnp.concatenate([re * cos - im * sin, other_re * cos - other_im * sin], 1)
        lower = jnp.concatenate([im * cos + re * sin, other_im * cos + other_re * sin], 1)
        out = product(spread_table, split(jnp.concatenate([upper, lower], 0)), NN)
        put(s, 0, out[:, :128])
        put(s, 1, out[:, 128:])


def inverse_y(get, fourier, real_rows, twist, put):
    slots = []
    for h in (0, 1):
        re, im = get(h, 0), get(h, 1)
        if h == 0:
            row = lax.broadcasted_iota(jnp.int32, (128, 128), 0)
            lane = lax.broadcasted_iota(jnp.int32, (128, 128), 1)
            single = (row == 0) & (lane < 32)
            re, im = jnp.where(single, 0.5 * re, re), jnp.where(single, 0.5 * im, im)
        rows = split(jnp.concatenate([re.T, im.T], 1))
        if h == 0:
            first = product((rows[0][:32], rows[1][:32]), real_rows, NN)
            rows = (rows[0][32:], rows[1][32:])
        out = product(rows, fourier, NN)
        slots += [out[32 * m : 32 * m + 32] for m in range(out.shape[0] // 32)]
    scale = 2.0 / CELLS
    base = [first[:, :128] * scale, first[:, 128:] * scale]
    real, imag = {}, {}
    for j in range(1, 8):
        re, im = slots[j - 1][:, :128], slots[j - 1][:, 128:]
        cos, sin = twist[j : j + 1] * scale, twist[8 + j : 9 + j] * scale
        real[j], imag[j] = re * cos - im * sin, im * cos + re * sin
    ends, tips = real[2] + real[6], imag[6] - imag[2]
    near, far = (real[2] - real[6]) * COS16[2], (imag[2] + imag[6]) * COS16[2]
    part = [ends, near - far, tips, -(near + far)]
    four = [base[0] + real[4], base[1] - imag[4], base[0] - real[4], base[1] + imag[4]]
    even = [four[a] + part[a] for a in range(4)] + [four[a] - part[a] for a in range(4)]
    u, v, w, x = real[1] + real[7], real[3] + real[5], real[1] - real[7], real[3] - real[5]
    cosine = [u + v, w * COS16[1] + x * COS16[3], (u - v) * COS16[2], w * COS16[3] - x * COS16[1]]
    u, v, w, x = imag[1] + imag[7], imag[3] + imag[5], imag[1] - imag[7], imag[3] - imag[5]
    sine = [None, u * SIN16[1] + v * SIN16[3], (w + x) * SIN16[2], u * SIN16[3] - v * SIN16[1], w - x]
    put(0, even[0] + cosine[0])
    put(8, even[0] - cosine[0])
    for a in (1, 2, 3):
        odd, mirror = cosine[a] - sine[a], cosine[a] + sine[a]
        put(a, even[a] + odd)
        put(a + 8, even[a] - odd)
        put(8 - a, even[8 - a] - mirror)
        put(16 - a, even[8 - a] + mirror)
    put(4, even[4] - sine[4])
    put(12, even[4] + sine[4])


def lane_position():
    return (
        16 * lax.axis_index("slab_z")
        + 4 * lax.axis_index("slab_y")
        + 2 * lax.axis_index("slab_x")
        + lax.axis_index("slab_core")
    )


def forward_kernel(
    c_hbm,
    fourier_hbm,
    real_hbm,
    twist_hbm,
    out_ref,
    rate_ref,
    side_ref,
    c_ref,
    fourier_ref,
    real_ref,
    twist_ref,
    sems,
):
    def group_of(ref, n):
        return ref.at[n // 2, pl.ds(8 * (n % 2), 8), :]

    sources = [twist_hbm] + [group_of(c_hbm, n) for n in range(4)] + [real_hbm, fourier_hbm]
    targets = [twist_ref] + [group_of(c_ref, n) for n in range(4)] + [real_ref, fourier_ref]
    copies = [
        pltpu.make_async_copy(source, target, sems.at[n])
        for n, (source, target) in enumerate(zip(sources, targets))
    ]
    for copy in copies:
        copy.start()

    def put(h, part, f, value):
        out_ref[pl.ds(640 * h + 2 * part + f, 128, stride=5), :] = value

    def put_rate(sigma, side, kind, value):
        (rate_ref, side_ref)[side][2 * sigma + kind] = value

    def late(n, ref):
        def read():
            copies[n].wait()
            return ref[...]

        return read

    all_rates(lax.axis_index("section"), lane_position(), put_rate)
    def read_rows(n):
        copies[n + 1].wait()
        return c_ref[n // 2, 8 * (n % 2) : 8 * (n % 2) + 8, :]

    lanes = forward_y(read_rows, late(6, fourier_ref), late(5, real_ref), late(0, twist_ref), put)
    out_ref[pl.ds(4, 256, stride=5), :] = jnp.broadcast_to(jnp.sum(lanes, 0, keepdims=True), (256, 128))


def middle_kernel(
    in_ref, rate_ref, side_ref, gather_ref, lanes_ref, spread_ref, twist_ref, out_ref, bulk_ref
):
    def get(s, part, f):
        return in_ref[pl.ds(640 * s + 2 * part + f, 128, stride=5), :]

    def put(s, part, value):
        out_ref[pl.ds(256 * s + part, 128, stride=2), :] = value

    middle(
        pltpu.roll,
        get,
        lambda sigma, side, kind: (rate_ref, side_ref)[side][2 * sigma + kind],
        lax.axis_index("section"),
        lane_position(),
        (gather_ref[0], gather_ref[1]),
        lanes_ref,
        (spread_ref[0], spread_ref[1]),
        twist_ref,
        put,
    )
    bulk = jnp.sum(in_ref[pl.ds(4, 256, stride=5), :], 0, keepdims=True)
    bulk_ref[...] = jnp.broadcast_to(bulk, (8, 128))


def inverse_kernel(in_ref, bulk_ref, fourier_ref, real_ref, twist_ref, out_ref, energy_ref):
    def get(h, part):
        return in_ref[pl.ds(256 * h + part, 128, stride=2), :]

    def put(a, value):
        out_ref[0, :, 128 * a : 128 * a + 128] = value[:16]
        out_ref[1, :, 128 * a : 128 * a + 128] = value[16:]

    energy_ref[...] = jnp.sum(bulk_ref[0:1, :], keepdims=True) * (1.0 / CELLS)
    inverse_y(
        get, (fourier_ref[0], fourier_ref[1]), (real_ref[0], real_ref[1]), twist_ref[...], put
    )


def exchange(rows):
    width = rows.shape[0] // 256
    message = rows.reshape(256, 1, 128 * width)
    return lax.all_to_all(message, ALL, split_axis=0, concat_axis=0, tiled=True).reshape(rows.shape)


def per_device(concentration):
    whole = pl.BlockSpec(memory_space=pltpu.VMEM)
    params = pltpu.CompilerParams(vmem_limit_bytes=12 << 20)
    outgoing, rate, side = pl.pallas_call(
        forward_kernel,
        out_shape=(
            pltpu.VMEM((1280, 128), f32),
            pltpu.VMEM((4, 128, 128), f32),
            pltpu.VMEM((4, 32, 128), f32),
        ),
        in_specs=[pl.BlockSpec(memory_space=pltpu.HBM)] * 4,
        out_specs=(whole, whole, whole),
        scratch_shapes=[
            pltpu.VMEM(concentration.shape, f32),
            pltpu.VMEM(FOURIER.shape, bf16),
            pltpu.VMEM(REAL.shape, bf16),
            pltpu.VMEM(Y_TWIST.shape, f32),
            pltpu.SemaphoreType.DMA((7,)),
        ],
        compiler_params=params,
    )(*[pltpu.with_memory_space_constraint(a, pltpu.HBM) for a in (concentration, FOURIER_T, REAL_T, Y_TWIST)])
    columns = exchange(outgoing)
    leaving, bulk = pl.pallas_call(
        middle_kernel,
        out_shape=(pltpu.VMEM((512, 128), f32), pltpu.VMEM((8, 128), f32)),
        in_specs=[whole] * 7,
        out_specs=(whole, whole),
        compiler_params=params,
    )(columns, rate, side, GATHER, LANES, SPREAD, X_TWIST)
    rows_back = exchange(leaving)
    new_field, energy = pl.pallas_call(
        inverse_kernel,
        out_shape=(jax.ShapeDtypeStruct(concentration.shape, f32), jax.ShapeDtypeStruct((1, 1), f32)),
        in_specs=[whole] * 5,
        out_specs=(whole, whole),
        compiler_params=params,
    )(rows_back, bulk, FOURIER, REAL, Y_TWIST)
    return new_field, energy.reshape(())


def solution(mesh):
    finer = Mesh(mesh.devices.reshape(2, 4, 2, 8, 2), ("section",) + SLAB)
    return jax.shard_map(
        per_device,
        mesh=finer,
        in_specs=(P("section", SLAB, None),),
        out_specs=(P("section", SLAB, None), P()),
        check_vma=False,
    )
```

```python
import math

import jax
import jax.numpy as jnp
import ml_dtypes
import numpy as np
from jax import lax
from jax.experimental import pallas as pl
from jax.experimental.pallas import tpu as pltpu
from jax.sharding import Mesh
from jax.sharding import PartitionSpec as P

SLAB = ("slab_y", "slab_x", "slab_z", "slab_core")
ALL = ("section", "slab_z", "slab_y", "slab_x", "slab_core")
NX = 2048
NY = 2048
NZ = 4
CELLS = NX * NY * NZ
time_step = 100.0
kappa_grad = 2.0
stabilizer = 8.0
f32 = jnp.float32
bf16 = jnp.bfloat16


def halves(matrix):
    high = matrix.astype(np.float32).astype(ml_dtypes.bfloat16)
    low = (matrix - high.astype(np.float64)).astype(np.float32).astype(ml_dtypes.bfloat16)
    return np.stack([high, low])


def fourier_table():
    index = np.arange(128)
    angle = 2.0 * np.pi * (np.outer(index, index) % 128) / 128
    return halves(np.block([[np.cos(angle), np.sin(angle)], [-np.sin(angle), np.cos(angle)]]))


def slab_order():
    return np.arange(128).reshape(4, 2, 8, 2).transpose(2, 0, 1, 3).reshape(128)


def real_table():
    angle = 2.0 * np.pi * (np.outer(np.arange(128), np.arange(256)) % 256) / 256
    lower = -np.sin(angle)
    lower[0] = 1.0 - 2.0 * (np.arange(256) % 2)
    return halves(np.concatenate([np.cos(angle), lower], 0))


def lane_table(parity):
    z_at, x_at = np.arange(2)[:, None, None, None], np.arange(16)[None, :, None, None]
    t_at, q_at = np.arange(2)[None, None, :, None], np.arange(16)[None, None, None, :]
    turn = (4 * parity * z_at + 8 * t_at * z_at + x_at * q_at) % 16
    value = np.exp(-2j * np.pi * turn / 16).reshape(32, 32)
    value = np.kron(np.eye(4), value)
    return halves(np.block([[value.real, value.imag], [-value.imag, value.real]]))


def y_twist_table():
    angle = 2.0 * np.pi * np.outer(np.arange(8), np.arange(128)) / 2048
    return np.concatenate([np.cos(angle), np.sin(angle)], 0).astype(np.float32)


def x_twist_table():
    angle = 2.0 * np.pi * np.outer(np.arange(128), np.arange(128) % 16) / 2048
    return np.stack([np.cos(angle), np.sin(angle)]).astype(np.float32)


FOURIER = fourier_table()
ORDER = slab_order()
GATHER = FOURIER[:, :, np.concatenate([ORDER, 128 + ORDER])]
SPREAD = FOURIER[:, ORDER, :]
REAL = real_table()
LANES = np.stack([lane_table(0), lane_table(1)])
FOURIER_T = FOURIER.transpose(0, 2, 1)
REAL_T = REAL.transpose(0, 2, 1)
Y_TWIST = y_twist_table()
X_TWIST = x_twist_table()
COS16 = [math.cos(2.0 * math.pi * m / 16) for m in range(16)]
SIN16 = [math.sin(2.0 * math.pi * m / 16) for m in range(16)]


def split(value):
    high = value.astype(bf16)
    return high, (value - high.astype(f32)).astype(bf16)


NN = (((1,), (0,)), ((), ()))
NT = (((1,), (1,)), ((), ()))


def product(left, right, pattern):
    total = left[0].shape[0]
    both = lax.dot_general(
        jnp.concatenate(left, 0), right[0], pattern, preferred_element_type=f32
    )
    rest = lax.dot_general(left[0], right[1], pattern, preferred_element_type=f32)
    return both[:total] + (both[total:] + rest)


def y_slots(at):
    add = [at[a] + at[a + 8] for a in range(8)]
    sub = [at[a] - at[a + 8] for a in range(8)]
    both = [add[a] + add[a + 4] for a in range(4)]
    diff = [add[a] - add[a + 4] for a in range(4)]
    zero = jnp.concatenate([both[0] + both[2], both[1] + both[3]], 1)
    near, far = (diff[1] - diff[3]) * COS16[2], (diff[1] + diff[3]) * COS16[2]
    minus = [None] + [sub[a] - sub[8 - a] for a in (1, 2, 3)]
    plus = [None] + [sub[a] + sub[8 - a] for a in (1, 2, 3)]
    middle_re = minus[2] * COS16[2]
    re_17, re_35 = sub[0] + middle_re, sub[0] - middle_re
    re_1, re_3 = minus[1] * COS16[1] + minus[3] * COS16[3], minus[1] * COS16[3] - minus[3] * COS16[1]
    im_1, im_3 = plus[1] * SIN16[1] + plus[3] * SIN16[3], plus[1] * SIN16[3] - plus[3] * SIN16[1]
    middle_im = plus[2] * SIN16[2]
    im_17, im_35 = middle_im + sub[4], middle_im - sub[4]
    return [
        zero,
        (re_17 + re_1, im_1 + im_17, -1),
        (diff[0] + near, diff[2] + far, -1),
        (re_35 + re_3, im_3 + im_35, -1),
        (both[0] - both[2], both[3] - both[1], 1),
        (re_35 - re_3, im_35 - im_3, 1),
        (diff[0] - near, diff[2] - far, 1),
        (re_17 - re_1, im_17 - im_1, 1),
    ]


def turned_slots(at, turns):
    slots = y_slots(at)
    for j in range(1, 8):
        re, n, sign = slots[j]
        cos, sin, negative = turns[j]
        if sign > 0:
            turned = [re * cos + n * sin, n * cos - re * sin]
        else:
            turned = [re * cos - n * sin, n * negative - re * sin]
        slots[j] = jnp.concatenate(turned, 1)
    return slots


def forward_y(read_rows, read_fourier, read_real, read_twist, put):
    twist = read_twist()
    turns = [(twist[j : j + 1], twist[8 + j : 9 + j], -twist[j : j + 1]) for j in range(8)]
    blocks, slots = [], []
    for group in range(4):
        rows = read_rows(group)
        blocks.append([rows[:, 128 * a : 128 * a + 128] for a in range(16)])
        slots.append(turned_slots(blocks[group], turns))
    real_rows = read_real()
    fourier = read_fourier()
    lanes = None
    for f in (0, 1):
        if f == 1:
            slots = []
            for block in blocks:
                cubic = []
                for value in block:
                    squared = value * value
                    bulk = 0.25 * squared * squared - 0.5 * squared
                    lanes = bulk if lanes is None else lanes + bulk
                    cubic.append(squared * value - value)
                slots.append(turned_slots(cubic, turns))
        first = product(split(jnp.concatenate([slot[0] for slot in slots], 0)), real_rows, NN)
        others = [slot[j] for j in range(1, 8) for slot in slots]
        rest = product(split(jnp.concatenate(others, 0)), fourier, NN)
        for h, rows in ((0, jnp.concatenate([first, rest[:96]], 0)), (1, rest[96:])):
            put(h, 0, f, rows[:, :128].T)
            put(h, 1, f, rows[:, 128:].T)
    return lanes


def wave_square(index, length):
    signed = jnp.where(2 * index >= length, index - length, index)
    phase_angle = signed.astype(f32) * (2.0 * math.pi / length)
    return phase_angle * phase_angle


def rates(wave_sq):
    numerator = 1.0 + time_step * stabilizer * wave_sq
    inverse = 1.0 / (numerator + time_step * kappa_grad * wave_sq * wave_sq)
    return numerator * inverse, time_step * wave_sq * inverse


def all_rates(section_at, lane_at, put):
    lane = lax.broadcasted_iota(jnp.int32, (128, 128), 1)
    row = lax.broadcasted_iota(jnp.int32, (128, 128), 0)
    slot = 4 * section_at + lane // 32
    y_index = jnp.where(slot == 0, 8 * lane_at, slot + 16 * lane_at)
    x_index = row + 128 * (lane % 16)
    wave_x = wave_square(x_index, NX)
    wave_xy = wave_x + wave_square(y_index, NY)
    half_y = (2.0 * math.pi / NY * (NY // 2)) ** 2
    for sigma in (0, 1):
        wave_z = wave_square(sigma + 2 * (lane // 16 % 2), NZ)
        for side, wave_sq in ((0, wave_z + wave_xy), (1, wave_z + (wave_x + half_y))):
            keep, mix = rates(wave_sq)
            put(sigma, side, 0, keep)
            put(sigma, side, 1, mix)


def middle(get, get_rate, section_at, lane_at, gather, lanes, spread_table, twist, put):
    lane = lax.broadcasted_iota(jnp.int32, (128, 128), 1)
    packed = (lane < 32) & (section_at == 0) & (lane_at == 0)
    cos, sin = twist[0], twist[1]
    parts = []
    for s in (0, 1):
        c_re, c_im, g_re, g_im = get(s, 0, 0), get(s, 1, 0), get(s, 0, 1), get(s, 1, 1)
        c_im, g_re = jnp.where(packed, g_re, c_im), jnp.where(packed, c_im, g_re)
        parts.append((c_re, c_im, g_re, g_im))
    stacked = []
    for sigma in (0, 1):
        mixed = [a + b if sigma == 0 else a - b for a, b in zip(*parts)]
        stacked.append(
            jnp.concatenate(
                [jnp.concatenate([mixed[0], mixed[2]], 1), jnp.concatenate([mixed[1], mixed[3]], 1)], 0
            )
        )
    spreads = [product(gather, split(stacked[sigma]), NN) for sigma in (0, 1)]
    turned = []
    for spread in spreads:
        rows = []
        for f in (0, 1):
            re, im = spread[:128, 128 * f : 128 * f + 128], spread[128:, 128 * f : 128 * f + 128]
            rows.append(jnp.concatenate([re * cos + im * sin, im * cos - re * sin], 1))
        turned.append(split(jnp.concatenate(rows, 0)))
    tables = [(lanes[sigma, 0], lanes[sigma, 1]) for sigma in (0, 1)]
    specs = [product(turned[sigma], tables[sigma], NN) for sigma in (0, 1)]
    filtered = []
    for sigma, spec in enumerate(specs):
        c_re, c_im, g_re, g_im = spec[:128, :128], spec[:128, 128:], spec[128:, :128], spec[128:, 128:]
        keep, mix = get_rate(sigma, 0, 0), get_rate(sigma, 0, 1)
        keep_half, mix_half = get_rate(sigma, 1, 0), get_rate(sigma, 1, 1)
        main_re = keep * c_re - mix * jnp.where(packed, c_im, g_re)
        main_im = keep * c_im - mix * jnp.where(packed, -c_re, g_im)
        side_re = keep_half * g_re - mix_half * g_im
        side_im = keep_half * g_im + mix_half * g_re
        rows = jnp.concatenate(
            [jnp.concatenate([main_re, main_im], 1), jnp.concatenate([side_re, side_im], 1)], 0
        )
        filtered.append(split(rows))
    back = [product(filtered[sigma], tables[sigma], NT) for sigma in (0, 1)]
    for s in (0, 1):
        mixed = back[0] + back[1] if s == 0 else back[0] - back[1]
        both = []
        for f in (0, 1):
            re, im = mixed[128 * f : 128 * f + 128, :128], mixed[128 * f : 128 * f + 128, 128:]
            both.append((re * cos - im * sin, im * cos + re * sin))
        (m_re, m_im), (s_re, s_im) = both
        upper = jnp.concatenate([m_re, jnp.where(packed, s_re, m_im)], 1)
        lower = jnp.concatenate([-m_im, jnp.where(packed, -s_im, m_re)], 1)
        out = product(spread_table, split(jnp.concatenate([upper, lower], 0)), NN)
        put(s, 0, out[:, :128])
        put(s, 1, out[:, 128:])


def inverse_y(get, fourier, real_rows, twist, put):
    slots = []
    for h in (0, 1):
        re, im = get(h, 0), get(h, 1)
        if h == 0:
            row = lax.broadcasted_iota(jnp.int32, (128, 128), 0)
            lane = lax.broadcasted_iota(jnp.int32, (128, 128), 1)
            single = (row == 0) & (lane < 32)
            re, im = jnp.where(single, 0.5 * re, re), jnp.where(single, 0.5 * im, im)
        rows = split(jnp.concatenate([re.T, im.T], 1))
        if h == 0:
            first = product((rows[0][:32], rows[1][:32]), real_rows, NN)
            rows = (rows[0][32:], rows[1][32:])
        out = product(rows, fourier, NN)
        slots += [out[32 * m : 32 * m + 32] for m in range(out.shape[0] // 32)]
    scale = 2.0 / CELLS
    base = [first[:, :128] * scale, first[:, 128:] * scale]
    real, imag = {}, {}
    for j in range(1, 8):
        re, im = slots[j - 1][:, :128], slots[j - 1][:, 128:]
        cos, sin = twist[j : j + 1] * scale, twist[8 + j : 9 + j] * scale
        real[j], imag[j] = re * cos - im * sin, im * cos + re * sin
    ends, tips = real[2] + real[6], imag[6] - imag[2]
    near, far = (real[2] - real[6]) * COS16[2], (imag[2] + imag[6]) * COS16[2]
    part = [ends, near - far, tips, -(near + far)]
    four = [base[0] + real[4], base[1] - imag[4], base[0] - real[4], base[1] + imag[4]]
    even = [four[a] + part[a] for a in range(4)] + [four[a] - part[a] for a in range(4)]
    u, v, w, x = real[1] + real[7], real[3] + real[5], real[1] - real[7], real[3] - real[5]
    cosine = [u + v, w * COS16[1] + x * COS16[3], (u - v) * COS16[2], w * COS16[3] - x * COS16[1]]
    u, v, w, x = imag[1] + imag[7], imag[3] + imag[5], imag[1] - imag[7], imag[3] - imag[5]
    sine = [None, u * SIN16[1] + v * SIN16[3], (w + x) * SIN16[2], u * SIN16[3] - v * SIN16[1], w - x]
    put(0, even[0] + cosine[0])
    put(8, even[0] - cosine[0])
    for a in (1, 2, 3):
        odd, mirror = cosine[a] - sine[a], cosine[a] + sine[a]
        put(a, even[a] + odd)
        put(a + 8, even[a] - odd)
        put(8 - a, even[8 - a] - mirror)
        put(16 - a, even[8 - a] + mirror)
    put(4, even[4] - sine[4])
    put(12, even[4] + sine[4])


def lane_position():
    return (
        16 * lax.axis_index("slab_z")
        + 4 * lax.axis_index("slab_y")
        + 2 * lax.axis_index("slab_x")
        + lax.axis_index("slab_core")
    )


def forward_kernel(
    c_hbm,
    fourier_hbm,
    real_hbm,
    twist_hbm,
    out_ref,
    rate_ref,
    c_ref,
    fourier_ref,
    real_ref,
    twist_ref,
    sems,
):
    def group_of(ref, n):
        return ref.at[n // 2, pl.ds(8 * (n % 2), 8), :]

    sources = [twist_hbm] + [group_of(c_hbm, n) for n in range(4)] + [real_hbm, fourier_hbm]
    targets = [twist_ref] + [group_of(c_ref, n) for n in range(4)] + [real_ref, fourier_ref]
    copies = [
        pltpu.make_async_copy(source, target, sems.at[n])
        for n, (source, target) in enumerate(zip(sources, targets))
    ]
    for copy in copies:
        copy.start()

    def put(h, part, f, value):
        out_ref[pl.ds(640 * h + 2 * part + f, 128, stride=5), :] = value

    def put_rate(sigma, side, kind, value):
        rate_ref[4 * sigma + 2 * side + kind] = value

    def late(n, ref):
        def read():
            copies[n].wait()
            return ref[...]

        return read

    all_rates(lax.axis_index("section"), lane_position(), put_rate)
    def read_rows(n):
        copies[n + 1].wait()
        return c_ref[n // 2, 8 * (n % 2) : 8 * (n % 2) + 8, :]

    lanes = forward_y(read_rows, late(6, fourier_ref), late(5, real_ref), late(0, twist_ref), put)
    out_ref[pl.ds(4, 256, stride=5), :] = jnp.broadcast_to(jnp.sum(lanes, 0, keepdims=True), (256, 128))


def middle_kernel(
    in_ref, rate_ref, gather_ref, lanes_ref, spread_ref, twist_ref, out_ref, bulk_ref
):
    def get(s, part, f):
        return in_ref[pl.ds(640 * s + 2 * part + f, 128, stride=5), :]

    def put(s, part, value):
        out_ref[pl.ds(256 * s + part, 128, stride=2), :] = value

    middle(
        get,
        lambda sigma, side, kind: rate_ref[4 * sigma + 2 * side + kind],
        lax.axis_index("section"),
        lane_position(),
        (gather_ref[0], gather_ref[1]),
        lanes_ref,
        (spread_ref[0], spread_ref[1]),
        twist_ref,
        put,
    )
    bulk = jnp.sum(in_ref[pl.ds(4, 256, stride=5), :], 0, keepdims=True)
    bulk_ref[...] = jnp.broadcast_to(bulk, (8, 128))


def inverse_kernel(in_ref, bulk_ref, fourier_ref, real_ref, twist_ref, out_ref, energy_ref):
    def get(h, part):
        return in_ref[pl.ds(256 * h + part, 128, stride=2), :]

    def put(a, value):
        out_ref[0, :, 128 * a : 128 * a + 128] = value[:16]
        out_ref[1, :, 128 * a : 128 * a + 128] = value[16:]

    energy_ref[...] = jnp.sum(bulk_ref[0:1, :], keepdims=True) * (1.0 / CELLS)
    inverse_y(
        get, (fourier_ref[0], fourier_ref[1]), (real_ref[0], real_ref[1]), twist_ref[...], put
    )


def exchange(rows):
    width = rows.shape[0] // 256
    message = rows.reshape(256, 1, 128 * width)
    return lax.all_to_all(message, ALL, split_axis=0, concat_axis=0, tiled=True).reshape(rows.shape)


def per_device(concentration):
    whole = pl.BlockSpec(memory_space=pltpu.VMEM)
    params = pltpu.CompilerParams(vmem_limit_bytes=12 << 20)
    outgoing, rate = pl.pallas_call(
        forward_kernel,
        out_shape=(
            pltpu.VMEM((1280, 128), f32),
            pltpu.VMEM((8, 128, 128), f32),
        ),
        in_specs=[pl.BlockSpec(memory_space=pltpu.HBM)] * 4,
        out_specs=(whole, whole),
        scratch_shapes=[
            pltpu.VMEM(concentration.shape, f32),
            pltpu.VMEM(FOURIER.shape, bf16),
            pltpu.VMEM(REAL.shape, bf16),
            pltpu.VMEM(Y_TWIST.shape, f32),
            pltpu.SemaphoreType.DMA((7,)),
        ],
        compiler_params=params,
    )(*[pltpu.with_memory_space_constraint(a, pltpu.HBM) for a in (concentration, FOURIER_T, REAL_T, Y_TWIST)])
    columns = exchange(outgoing)
    leaving, bulk = pl.pallas_call(
        middle_kernel,
        out_shape=(pltpu.VMEM((512, 128), f32), pltpu.VMEM((8, 128), f32)),
        in_specs=[whole] * 6,
        out_specs=(whole, whole),
        compiler_params=params,
    )(columns, rate, GATHER, LANES, SPREAD, X_TWIST)
    rows_back = exchange(leaving)
    new_field, energy = pl.pallas_call(
        inverse_kernel,
        out_shape=(jax.ShapeDtypeStruct(concentration.shape, f32), jax.ShapeDtypeStruct((1, 1), f32)),
        in_specs=[whole] * 5,
        out_specs=(whole, whole),
        compiler_params=params,
    )(rows_back, bulk, FOURIER, REAL, Y_TWIST)
    return new_field, energy.reshape(())


def solution(mesh):
    finer = Mesh(mesh.devices.reshape(2, 4, 2, 8, 2), ("section",) + SLAB)
    return jax.shard_map(
        per_device,
        mesh=finer,
        in_specs=(P("section", SLAB, None),),
        out_specs=(P("section", SLAB, None), P()),
        check_vma=False,
    )
```

```python
import math

import jax
import jax.numpy as jnp
import ml_dtypes
import numpy as np
from jax import lax
from jax.experimental import pallas as pl
from jax.experimental.pallas import tpu as pltpu
from jax.sharding import Mesh
from jax.sharding import PartitionSpec as P

SLAB = ("slab_y", "slab_x", "slab_z", "slab_core")
ALL = ("section", "slab_z", "slab_y", "slab_x", "slab_core")
NX = 2048
NY = 2048
NZ = 4
CELLS = NX * NY * NZ
time_step = 100.0
kappa_grad = 2.0
stabilizer = 8.0
f32 = jnp.float32
bf16 = jnp.bfloat16


def halves(matrix):
    high = matrix.astype(np.float32).astype(ml_dtypes.bfloat16)
    low = (matrix - high.astype(np.float64)).astype(np.float32).astype(ml_dtypes.bfloat16)
    return np.stack([high, low])


def fourier_table():
    index = np.arange(128)
    angle = 2.0 * np.pi * (np.outer(index, index) % 128) / 128
    return halves(np.block([[np.cos(angle), np.sin(angle)], [-np.sin(angle), np.cos(angle)]]))


def slab_order():
    return np.arange(128).reshape(4, 2, 8, 2).transpose(2, 0, 1, 3).reshape(128)


def real_table():
    angle = 2.0 * np.pi * (np.outer(np.arange(128), np.arange(256)) % 256) / 256
    lower = -np.sin(angle)
    lower[0] = 1.0 - 2.0 * (np.arange(256) % 2)
    return halves(np.concatenate([np.cos(angle), lower], 0))


def lane_table(parity):
    z_at, x_at = np.arange(2)[:, None, None, None], np.arange(16)[None, :, None, None]
    t_at, q_at = np.arange(2)[None, None, :, None], np.arange(16)[None, None, None, :]
    turn = (4 * parity * z_at + 8 * t_at * z_at + x_at * q_at) % 16
    value = np.exp(-2j * np.pi * turn / 16).reshape(32, 32)
    value = np.kron(np.eye(4), value)
    return halves(np.block([[value.real, value.imag], [-value.imag, value.real]]))


def y_twist_table():
    angle = 2.0 * np.pi * np.outer(np.arange(8), np.arange(128)) / 2048
    return np.concatenate([np.cos(angle), np.sin(angle)], 0).astype(np.float32)


def x_twist_table():
    angle = 2.0 * np.pi * np.outer(np.arange(128), np.arange(128) % 16) / 2048
    return np.stack([np.cos(angle), np.sin(angle)]).astype(np.float32)


FOURIER = fourier_table()
ORDER = slab_order()
GATHER = FOURIER[:, :, np.concatenate([ORDER, 128 + ORDER])]
SPREAD = FOURIER[:, ORDER, :]
REAL = real_table()
LANES = np.stack([lane_table(0), lane_table(1)])
FOURIER_T = FOURIER.transpose(0, 2, 1)
REAL_T = REAL.transpose(0, 2, 1)
Y_TWIST = y_twist_table()
X_TWIST = x_twist_table()
COS16 = [math.cos(2.0 * math.pi * m / 16) for m in range(16)]
SIN16 = [math.sin(2.0 * math.pi * m / 16) for m in range(16)]


def split(value):
    high = value.astype(bf16)
    return high, (value - high.astype(f32)).astype(bf16)


NN = (((1,), (0,)), ((), ()))
NT = (((1,), (1,)), ((), ()))


def product(left, right, pattern):
    total = left[0].shape[0]
    both = lax.dot_general(
        jnp.concatenate(left, 0), right[0], pattern, preferred_element_type=f32
    )
    rest = lax.dot_general(left[0], right[1], pattern, preferred_element_type=f32)
    return both[:total] + (both[total:] + rest)


def y_slots(at):
    add = [at[a] + at[a + 8] for a in range(8)]
    sub = [at[a] - at[a + 8] for a in range(8)]
    both = [add[a] + add[a + 4] for a in range(4)]
    diff = [add[a] - add[a + 4] for a in range(4)]
    zero = jnp.concatenate([both[0] + both[2], both[1] + both[3]], 1)
    near, far = (diff[1] - diff[3]) * COS16[2], (diff[1] + diff[3]) * COS16[2]
    minus = [None] + [sub[a] - sub[8 - a] for a in (1, 2, 3)]
    plus = [None] + [sub[a] + sub[8 - a] for a in (1, 2, 3)]
    middle_re = minus[2] * COS16[2]
    re_17, re_35 = sub[0] + middle_re, sub[0] - middle_re
    re_1, re_3 = minus[1] * COS16[1] + minus[3] * COS16[3], minus[1] * COS16[3] - minus[3] * COS16[1]
    im_1, im_3 = plus[1] * SIN16[1] + plus[3] * SIN16[3], plus[1] * SIN16[3] - plus[3] * SIN16[1]
    middle_im = plus[2] * SIN16[2]
    im_17, im_35 = middle_im + sub[4], middle_im - sub[4]
    return [
        zero,
        (re_17 + re_1, im_1 + im_17, -1),
        (diff[0] + near, diff[2] + far, -1),
        (re_35 + re_3, im_3 + im_35, -1),
        (both[0] - both[2], both[3] - both[1], 1),
        (re_35 - re_3, im_35 - im_3, 1),
        (diff[0] - near, diff[2] - far, 1),
        (re_17 - re_1, im_17 - im_1, 1),
    ]


def turned_slots(at, turns):
    slots = y_slots(at)
    for j in range(1, 8):
        re, n, sign = slots[j]
        cos, sin, negative = turns[j]
        if sign > 0:
            turned = [re * cos + n * sin, n * cos - re * sin]
        else:
            turned = [re * cos - n * sin, n * negative - re * sin]
        slots[j] = jnp.concatenate(turned, 1)
    return slots


def forward_y(read_rows, read_fourier, read_real, read_twist, put):
    twist = read_twist()
    turns = [(twist[j : j + 1], twist[8 + j : 9 + j], -twist[j : j + 1]) for j in range(8)]
    blocks, slots = [], []
    for group in range(4):
        rows = read_rows(group)
        blocks.append([rows[:, 128 * a : 128 * a + 128] for a in range(16)])
        slots.append(turned_slots(blocks[group], turns))
    real_rows = read_real()
    fourier = read_fourier()
    lanes = None
    for f in (0, 1):
        if f == 1:
            slots = []
            for block in blocks:
                cubic = []
                for value in block:
                    squared = value * value
                    half = 0.5 * squared
                    bulk = half * half - half
                    lanes = bulk if lanes is None else lanes + bulk
                    cubic.append(squared * value - value)
                slots.append(turned_slots(cubic, turns))
        first = product(split(jnp.concatenate([slot[0] for slot in slots], 0)), real_rows, NN)
        others = [slot[j] for j in range(1, 8) for slot in slots]
        rest = product(split(jnp.concatenate(others, 0)), fourier, NN)
        for h, rows in ((0, jnp.concatenate([first, rest[:96]], 0)), (1, rest[96:])):
            put(h, 0, f, rows[:, :128].T)
            put(h, 1, f, rows[:, 128:].T)
    return lanes


def wave_square(index, length):
    signed = jnp.where(2 * index >= length, index - length, index)
    phase_angle = signed.astype(f32) * (2.0 * math.pi / length)
    return phase_angle * phase_angle


def rates(wave_sq):
    numerator = 1.0 + time_step * stabilizer * wave_sq
    inverse = 1.0 / (numerator + time_step * kappa_grad * wave_sq * wave_sq)
    return numerator * inverse, time_step * wave_sq * inverse


def all_rates(section_at, lane_at, put):
    lane = lax.broadcasted_iota(jnp.int32, (128, 128), 1)
    row = lax.broadcasted_iota(jnp.int32, (128, 128), 0)
    slot = 4 * section_at + lane // 32
    y_index = jnp.where(slot == 0, 8 * lane_at, slot + 16 * lane_at)
    x_index = row + 128 * (lane % 16)
    wave_x = wave_square(x_index, NX)
    wave_xy = wave_x + wave_square(y_index, NY)
    half_y = (2.0 * math.pi / NY * (NY // 2)) ** 2
    for sigma in (0, 1):
        wave_z = wave_square(sigma + 2 * (lane // 16 % 2), NZ)
        for side, wave_sq in ((0, wave_z + wave_xy), (1, wave_z + (wave_x + half_y))):
            keep, mix = rates(wave_sq)
            put(sigma, side, 0, keep)
            put(sigma, side, 1, mix)


def middle(get, get_rate, section_at, lane_at, gather, lanes, spread_table, twist, put):
    lane = lax.broadcasted_iota(jnp.int32, (128, 128), 1)
    packed = (lane < 32) & (section_at == 0) & (lane_at == 0)
    cos, sin = twist[0], twist[1]
    parts = []
    for s in (0, 1):
        c_re, c_im, g_re, g_im = get(s, 0, 0), get(s, 1, 0), get(s, 0, 1), get(s, 1, 1)
        c_im, g_re = jnp.where(packed, g_re, c_im), jnp.where(packed, c_im, g_re)
        parts.append((c_re, c_im, g_re, g_im))
    stacked = []
    for sigma in (0, 1):
        mixed = [a + b if sigma == 0 else a - b for a, b in zip(*parts)]
        stacked.append(
            jnp.concatenate(
                [jnp.concatenate([mixed[0], mixed[2]], 1), jnp.concatenate([mixed[1], mixed[3]], 1)], 0
            )
        )
    spreads = [product(gather, split(stacked[sigma]), NN) for sigma in (0, 1)]
    turned = []
    for spread in spreads:
        rows = []
        for f in (0, 1):
            re, im = spread[:128, 128 * f : 128 * f + 128], spread[128:, 128 * f : 128 * f + 128]
            rows.append(jnp.concatenate([re * cos + im * sin, im * cos - re * sin], 1))
        turned.append(split(jnp.concatenate(rows, 0)))
    tables = [(lanes[sigma, 0], lanes[sigma, 1]) for sigma in (0, 1)]
    specs = [product(turned[sigma], tables[sigma], NN) for sigma in (0, 1)]
    filtered = []
    for sigma, spec in enumerate(specs):
        c_re, c_im, g_re, g_im = spec[:128, :128], spec[:128, 128:], spec[128:, :128], spec[128:, 128:]
        keep, mix = get_rate(sigma, 0, 0), get_rate(sigma, 0, 1)
        keep_half, mix_half = get_rate(sigma, 1, 0), get_rate(sigma, 1, 1)
        main_re = keep * c_re - mix * jnp.where(packed, c_im, g_re)
        main_im = keep * c_im - mix * jnp.where(packed, -c_re, g_im)
        side_re = keep_half * g_re - mix_half * g_im
        side_im = keep_half * g_im + mix_half * g_re
        rows = jnp.concatenate(
            [jnp.concatenate([main_re, main_im], 1), jnp.concatenate([side_re, side_im], 1)], 0
        )
        filtered.append(split(rows))
    back = [product(filtered[sigma], tables[sigma], NT) for sigma in (0, 1)]
    for s in (0, 1):
        mixed = back[0] + back[1] if s == 0 else back[0] - back[1]
        both = []
        for f in (0, 1):
            re, im = mixed[128 * f : 128 * f + 128, :128], mixed[128 * f : 128 * f + 128, 128:]
            both.append((re * cos - im * sin, im * cos + re * sin))
        (m_re, m_im), (s_re, s_im) = both
        upper = jnp.concatenate([m_re, jnp.where(packed, s_re, m_im)], 1)
        lower = jnp.concatenate([-m_im, jnp.where(packed, -s_im, m_re)], 1)
        out = product(spread_table, split(jnp.concatenate([upper, lower], 0)), NN)
        put(s, 0, out[:, :128])
        put(s, 1, out[:, 128:])


def inverse_y(get, fourier, real_rows, twist, put):
    slots = []
    for h in (0, 1):
        re, im = get(h, 0), get(h, 1)
        if h == 0:
            row = lax.broadcasted_iota(jnp.int32, (128, 128), 0)
            lane = lax.broadcasted_iota(jnp.int32, (128, 128), 1)
            single = (row == 0) & (lane < 32)
            re, im = jnp.where(single, 0.5 * re, re), jnp.where(single, 0.5 * im, im)
        rows = split(jnp.concatenate([re.T, im.T], 1))
        if h == 0:
            first = product((rows[0][:32], rows[1][:32]), real_rows, NN)
            rows = (rows[0][32:], rows[1][32:])
        out = product(rows, fourier, NN)
        slots += [out[32 * m : 32 * m + 32] for m in range(out.shape[0] // 32)]
    scale = 2.0 / CELLS
    base = [first[:, :128] * scale, first[:, 128:] * scale]
    real, imag = {}, {}
    for j in range(1, 8):
        re, im = slots[j - 1][:, :128], slots[j - 1][:, 128:]
        cos, sin = twist[j : j + 1] * scale, twist[8 + j : 9 + j] * scale
        real[j], imag[j] = re * cos - im * sin, im * cos + re * sin
    ends, tips = real[2] + real[6], imag[6] - imag[2]
    near, far = (real[2] - real[6]) * COS16[2], (imag[2] + imag[6]) * COS16[2]
    part = [ends, near - far, tips, -(near + far)]
    four = [base[0] + real[4], base[1] - imag[4], base[0] - real[4], base[1] + imag[4]]
    even = [four[a] + part[a] for a in range(4)] + [four[a] - part[a] for a in range(4)]
    u, v, w, x = real[1] + real[7], real[3] + real[5], real[1] - real[7], real[3] - real[5]
    cosine = [u + v, w * COS16[1] + x * COS16[3], (u - v) * COS16[2], w * COS16[3] - x * COS16[1]]
    u, v, w, x = imag[1] + imag[7], imag[3] + imag[5], imag[1] - imag[7], imag[3] - imag[5]
    sine = [None, u * SIN16[1] + v * SIN16[3], (w + x) * SIN16[2], u * SIN16[3] - v * SIN16[1], w - x]
    put(0, even[0] + cosine[0])
    put(8, even[0] - cosine[0])
    for a in (1, 2, 3):
        odd, mirror = cosine[a] - sine[a], cosine[a] + sine[a]
        put(a, even[a] + odd)
        put(a + 8, even[a] - odd)
        put(8 - a, even[8 - a] - mirror)
        put(16 - a, even[8 - a] + mirror)
    put(4, even[4] - sine[4])
    put(12, even[4] + sine[4])


def lane_position():
    return (
        16 * lax.axis_index("slab_z")
        + 4 * lax.axis_index("slab_y")
        + 2 * lax.axis_index("slab_x")
        + lax.axis_index("slab_core")
    )


def forward_kernel(
    c_hbm,
    fourier_hbm,
    real_hbm,
    twist_hbm,
    out_ref,
    rate_ref,
    c_ref,
    fourier_ref,
    real_ref,
    twist_ref,
    sems,
):
    def group_of(ref, n):
        return ref.at[n // 2, pl.ds(8 * (n % 2), 8), :]

    sources = [twist_hbm] + [group_of(c_hbm, n) for n in range(4)] + [real_hbm, fourier_hbm]
    targets = [twist_ref] + [group_of(c_ref, n) for n in range(4)] + [real_ref, fourier_ref]
    copies = [
        pltpu.make_async_copy(source, target, sems.at[n])
        for n, (source, target) in enumerate(zip(sources, targets))
    ]
    for copy in copies:
        copy.start()

    def put(h, part, f, value):
        out_ref[pl.ds(640 * h + 2 * part + f, 128, stride=5), :] = value

    def put_rate(sigma, side, kind, value):
        rate_ref[4 * sigma + 2 * side + kind] = value

    def late(n, ref):
        def read():
            copies[n].wait()
            return ref[...]

        return read

    all_rates(lax.axis_index("section"), lane_position(), put_rate)
    def read_rows(n):
        copies[n + 1].wait()
        return c_ref[n // 2, 8 * (n % 2) : 8 * (n % 2) + 8, :]

    lanes = forward_y(read_rows, late(6, fourier_ref), late(5, real_ref), late(0, twist_ref), put)
    out_ref[pl.ds(4, 256, stride=5), :] = jnp.broadcast_to(jnp.sum(lanes, 0, keepdims=True), (256, 128))


def middle_kernel(
    in_ref, rate_ref, gather_ref, lanes_ref, spread_ref, twist_ref, out_ref, bulk_ref
):
    def get(s, part, f):
        return in_ref[pl.ds(640 * s + 2 * part + f, 128, stride=5), :]

    def put(s, part, value):
        out_ref[pl.ds(256 * s + part, 128, stride=2), :] = value

    middle(
        get,
        lambda sigma, side, kind: rate_ref[4 * sigma + 2 * side + kind],
        lax.axis_index("section"),
        lane_position(),
        (gather_ref[0], gather_ref[1]),
        lanes_ref,
        (spread_ref[0], spread_ref[1]),
        twist_ref,
        put,
    )
    bulk = jnp.sum(in_ref[pl.ds(4, 256, stride=5), :], 0, keepdims=True)
    bulk_ref[...] = jnp.broadcast_to(bulk, (8, 128))


def inverse_kernel(in_ref, bulk_ref, fourier_ref, real_ref, twist_ref, out_ref, energy_ref):
    def get(h, part):
        return in_ref[pl.ds(256 * h + part, 128, stride=2), :]

    def put(a, value):
        out_ref[0, :, 128 * a : 128 * a + 128] = value[:16]
        out_ref[1, :, 128 * a : 128 * a + 128] = value[16:]

    energy_ref[...] = jnp.sum(bulk_ref[0:1, :], keepdims=True) * (1.0 / CELLS)
    inverse_y(
        get, (fourier_ref[0], fourier_ref[1]), (real_ref[0], real_ref[1]), twist_ref[...], put
    )


def exchange(rows):
    width = rows.shape[0] // 256
    message = rows.reshape(256, 1, 128 * width)
    return lax.all_to_all(message, ALL, split_axis=0, concat_axis=0, tiled=True).reshape(rows.shape)


def per_device(concentration):
    whole = pl.BlockSpec(memory_space=pltpu.VMEM)
    params = pltpu.CompilerParams(vmem_limit_bytes=12 << 20)
    outgoing, rate = pl.pallas_call(
        forward_kernel,
        out_shape=(
            pltpu.VMEM((1280, 128), f32),
            pltpu.VMEM((8, 128, 128), f32),
        ),
        in_specs=[pl.BlockSpec(memory_space=pltpu.HBM)] * 4,
        out_specs=(whole, whole),
        scratch_shapes=[
            pltpu.VMEM(concentration.shape, f32),
            pltpu.VMEM(FOURIER.shape, bf16),
            pltpu.VMEM(REAL.shape, bf16),
            pltpu.VMEM(Y_TWIST.shape, f32),
            pltpu.SemaphoreType.DMA((7,)),
        ],
        compiler_params=params,
    )(*[pltpu.with_memory_space_constraint(a, pltpu.HBM) for a in (concentration, FOURIER_T, REAL_T, Y_TWIST)])
    columns = exchange(outgoing)
    leaving, bulk = pl.pallas_call(
        middle_kernel,
        out_shape=(pltpu.VMEM((512, 128), f32), pltpu.VMEM((8, 128), f32)),
        in_specs=[whole] * 6,
        out_specs=(whole, whole),
        compiler_params=params,
    )(columns, rate, GATHER, LANES, SPREAD, X_TWIST)
    rows_back = exchange(leaving)
    new_field, energy = pl.pallas_call(
        inverse_kernel,
        out_shape=(jax.ShapeDtypeStruct(concentration.shape, f32), jax.ShapeDtypeStruct((1, 1), f32)),
        in_specs=[whole] * 5,
        out_specs=(whole, whole),
        compiler_params=params,
    )(rows_back, bulk, FOURIER, REAL, Y_TWIST)
    return new_field, energy.reshape(())


def solution(mesh):
    finer = Mesh(mesh.devices.reshape(2, 4, 2, 8, 2), ("section",) + SLAB)
    return jax.shard_map(
        per_device,
        mesh=finer,
        in_specs=(P("section", SLAB, None),),
        out_specs=(P("section", SLAB, None), P()),
        check_vma=False,
    )
```

```python
import math

import jax
import jax.numpy as jnp
import ml_dtypes
import numpy as np
from jax import lax
from jax.experimental import pallas as pl
from jax.experimental.pallas import tpu as pltpu
from jax.sharding import Mesh
from jax.sharding import PartitionSpec as P

SLAB = ("slab_y", "slab_x", "slab_z", "slab_core")
ALL = ("slab_z", "slab_x", "slab_y", "slab_core", "section")
NX = 2048
NY = 2048
NZ = 4
CELLS = NX * NY * NZ
time_step = 100.0
kappa_grad = 2.0
stabilizer = 8.0
f32 = jnp.float32
bf16 = jnp.bfloat16


def halves(matrix):
    high = matrix.astype(np.float32).astype(ml_dtypes.bfloat16)
    low = (matrix - high.astype(np.float64)).astype(np.float32).astype(ml_dtypes.bfloat16)
    return np.stack([high, low])


def fourier_table():
    index = np.arange(128)
    angle = 2.0 * np.pi * (np.outer(index, index) % 128) / 128
    return halves(np.block([[np.cos(angle), np.sin(angle)], [-np.sin(angle), np.cos(angle)]]))


def slab_order():
    return np.arange(128).reshape(4, 2, 8, 2).transpose(2, 1, 0, 3).reshape(128)


def real_table():
    angle = 2.0 * np.pi * (np.outer(np.arange(128), np.arange(256)) % 256) / 256
    lower = -np.sin(angle)
    lower[0] = 1.0 - 2.0 * (np.arange(256) % 2)
    return halves(np.concatenate([np.cos(angle), lower], 0))


def lane_table(parity):
    z_at, x_at = np.arange(2)[:, None, None, None], np.arange(16)[None, :, None, None]
    t_at, q_at = np.arange(2)[None, None, :, None], np.arange(16)[None, None, None, :]
    turn = (4 * parity * z_at + 8 * t_at * z_at + x_at * q_at) % 16
    value = np.exp(-2j * np.pi * turn / 16).reshape(32, 32)
    value = np.kron(np.eye(4), value)
    return halves(np.block([[value.real, value.imag], [-value.imag, value.real]]))


def y_twist_table():
    angle = 2.0 * np.pi * np.outer(np.arange(8), np.arange(128)) / 2048
    return np.concatenate([np.cos(angle), np.sin(angle)], 0).astype(np.float32)


def x_twist_table():
    angle = 2.0 * np.pi * np.outer(np.arange(128), np.arange(128) % 16) / 2048
    return np.stack([np.cos(angle), np.sin(angle)]).astype(np.float32)


FOURIER = fourier_table()
ORDER = slab_order()
GATHER = FOURIER[:, :, np.concatenate([ORDER, 128 + ORDER])]
SPREAD = FOURIER[:, ORDER, :]
REAL = real_table()
LANES = np.stack([lane_table(0), lane_table(1)])
FOURIER_T = FOURIER.transpose(0, 2, 1)
REAL_T = REAL.transpose(0, 2, 1)
Y_TWIST = y_twist_table()
X_TWIST = x_twist_table()
COS16 = [math.cos(2.0 * math.pi * m / 16) for m in range(16)]
SIN16 = [math.sin(2.0 * math.pi * m / 16) for m in range(16)]


def split(value):
    high = value.astype(bf16)
    return high, (value - high.astype(f32)).astype(bf16)


NN = (((1,), (0,)), ((), ()))
NT = (((1,), (1,)), ((), ()))


def product(left, right, pattern):
    total = left[0].shape[0]
    both = lax.dot_general(
        jnp.concatenate(left, 0), right[0], pattern, preferred_element_type=f32
    )
    rest = lax.dot_general(left[0], right[1], pattern, preferred_element_type=f32)
    return both[:total] + (both[total:] + rest)


def y_slots(at):
    add = [at[a] + at[a + 8] for a in range(8)]
    sub = [at[a] - at[a + 8] for a in range(8)]
    both = [add[a] + add[a + 4] for a in range(4)]
    diff = [add[a] - add[a + 4] for a in range(4)]
    zero = jnp.concatenate([both[0] + both[2], both[1] + both[3]], 1)
    near, far = (diff[1] - diff[3]) * COS16[2], (diff[1] + diff[3]) * COS16[2]
    minus = [None] + [sub[a] - sub[8 - a] for a in (1, 2, 3)]
    plus = [None] + [sub[a] + sub[8 - a] for a in (1, 2, 3)]
    middle_re = minus[2] * COS16[2]
    re_17, re_35 = sub[0] + middle_re, sub[0] - middle_re
    re_1, re_3 = minus[1] * COS16[1] + minus[3] * COS16[3], minus[1] * COS16[3] - minus[3] * COS16[1]
    im_1, im_3 = plus[1] * SIN16[1] + plus[3] * SIN16[3], plus[1] * SIN16[3] - plus[3] * SIN16[1]
    middle_im = plus[2] * SIN16[2]
    im_17, im_35 = middle_im + sub[4], middle_im - sub[4]
    return [
        zero,
        (re_17 + re_1, im_1 + im_17, -1),
        (diff[0] + near, diff[2] + far, -1),
        (re_35 + re_3, im_3 + im_35, -1),
        (both[0] - both[2], both[3] - both[1], 1),
        (re_35 - re_3, im_35 - im_3, 1),
        (diff[0] - near, diff[2] - far, 1),
        (re_17 - re_1, im_17 - im_1, 1),
    ]


def turned_slots(at, turns):
    slots = y_slots(at)
    for j in range(1, 8):
        re, n, sign = slots[j]
        cos, sin, negative = turns[j]
        if sign > 0:
            turned = [re * cos + n * sin, n * cos - re * sin]
        else:
            turned = [re * cos - n * sin, n * negative - re * sin]
        slots[j] = jnp.concatenate(turned, 1)
    return slots


def forward_y(read_rows, read_fourier, read_real, read_twist, put):
    twist = read_twist()
    turns = [(twist[j : j + 1], twist[8 + j : 9 + j], -twist[j : j + 1]) for j in range(8)]
    blocks, slots = [], []
    for group in range(4):
        rows = read_rows(group)
        blocks.append([rows[:, 128 * a : 128 * a + 128] for a in range(16)])
        slots.append(turned_slots(blocks[group], turns))
    real_rows = read_real()
    fourier = read_fourier()
    lanes = None
    for f in (0, 1):
        if f == 1:
            slots = []
            for block in blocks:
                cubic = []
                for value in block:
                    squared = value * value
                    bulk = squared * (0.25 * squared - 0.5)
                    lanes = bulk if lanes is None else lanes + bulk
                    cubic.append(squared * value - value)
                slots.append(turned_slots(cubic, turns))
        first = product(split(jnp.concatenate([slot[0] for slot in slots], 0)), real_rows, NN)
        others = [slot[j] for j in range(1, 8) for slot in slots]
        rest = product(split(jnp.concatenate(others, 0)), fourier, NN)
        for h, rows in ((0, jnp.concatenate([first, rest[:96]], 0)), (1, rest[96:])):
            put(h, 0, f, rows[:, :128].T)
            put(h, 1, f, rows[:, 128:].T)
    return lanes


def wave_square(index, length):
    signed = jnp.where(2 * index >= length, index - length, index)
    phase_angle = signed.astype(f32) * (2.0 * math.pi / length)
    return phase_angle * phase_angle


def rates(wave_sq):
    numerator = 1.0 + time_step * stabilizer * wave_sq
    inverse = 1.0 / (numerator + time_step * kappa_grad * wave_sq * wave_sq)
    return numerator * inverse, time_step * wave_sq * inverse


def all_rates(section_at, lane_at, put):
    lane = lax.broadcasted_iota(jnp.int32, (128, 128), 1)
    row = lax.broadcasted_iota(jnp.int32, (128, 128), 0)
    slot = 4 * section_at + lane // 32
    y_index = jnp.where(slot == 0, 8 * lane_at, slot + 16 * lane_at)
    x_index = row + 128 * (lane % 16)
    wave_x = wave_square(x_index, NX)
    wave_xy = wave_x + wave_square(y_index, NY)
    half_y = (2.0 * math.pi / NY * (NY // 2)) ** 2
    for sigma in (0, 1):
        wave_z = wave_square(sigma + 2 * (lane // 16 % 2), NZ)
        for side, wave_sq in ((0, wave_z + wave_xy), (1, wave_z + (wave_x + half_y))):
            keep, mix = rates(wave_sq)
            put(sigma, side, 0, keep)
            put(sigma, side, 1, mix)


def middle(get, get_rate, section_at, lane_at, gather, lanes, spread_table, twist, put):
    lane = lax.broadcasted_iota(jnp.int32, (128, 128), 1)
    packed = (lane < 32) & (section_at == 0) & (lane_at == 0)
    cos, sin = twist[0], twist[1]
    parts = []
    for s in (0, 1):
        c_re, c_im, g_re, g_im = get(s, 0, 0), get(s, 1, 0), get(s, 0, 1), get(s, 1, 1)
        c_im, g_re = jnp.where(packed, g_re, c_im), jnp.where(packed, c_im, g_re)
        parts.append((c_re, c_im, g_re, g_im))
    stacked = []
    for sigma in (0, 1):
        mixed = [a + b if sigma == 0 else a - b for a, b in zip(*parts)]
        stacked.append(
            jnp.concatenate(
                [jnp.concatenate([mixed[0], mixed[2]], 1), jnp.concatenate([mixed[1], mixed[3]], 1)], 0
            )
        )
    spreads = [product(gather, split(stacked[sigma]), NN) for sigma in (0, 1)]
    turned = []
    for spread in spreads:
        rows = []
        for f in (0, 1):
            re, im = spread[:128, 128 * f : 128 * f + 128], spread[128:, 128 * f : 128 * f + 128]
            rows.append(jnp.concatenate([re * cos + im * sin, im * cos - re * sin], 1))
        turned.append(split(jnp.concatenate(rows, 0)))
    tables = [(lanes[sigma, 0], lanes[sigma, 1]) for sigma in (0, 1)]
    specs = [product(turned[sigma], tables[sigma], NN) for sigma in (0, 1)]
    filtered = []
    for sigma, spec in enumerate(specs):
        c_re, c_im, g_re, g_im = spec[:128, :128], spec[:128, 128:], spec[128:, :128], spec[128:, 128:]
        keep, mix = get_rate(sigma, 0, 0), get_rate(sigma, 0, 1)
        keep_half, mix_half = get_rate(sigma, 1, 0), get_rate(sigma, 1, 1)
        main_re = keep * c_re - mix * jnp.where(packed, c_im, g_re)
        main_im = keep * c_im - mix * jnp.where(packed, -c_re, g_im)
        side_re = keep_half * g_re - mix_half * g_im
        side_im = keep_half * g_im + mix_half * g_re
        rows = jnp.concatenate(
            [jnp.concatenate([main_re, main_im], 1), jnp.concatenate([side_re, side_im], 1)], 0
        )
        filtered.append(split(rows))
    back = [product(filtered[sigma], tables[sigma], NT) for sigma in (0, 1)]
    for s in (0, 1):
        mixed = back[0] + back[1] if s == 0 else back[0] - back[1]
        both = []
        for f in (0, 1):
            re, im = mixed[128 * f : 128 * f + 128, :128], mixed[128 * f : 128 * f + 128, 128:]
            both.append((re * cos - im * sin, im * cos + re * sin))
        (m_re, m_im), (s_re, s_im) = both
        upper = jnp.concatenate([m_re, jnp.where(packed, s_re, m_im)], 1)
        lower = jnp.concatenate([-m_im, jnp.where(packed, -s_im, m_re)], 1)
        out = product(spread_table, split(jnp.concatenate([upper, lower], 0)), NN)
        put(s, 0, out[:, :128])
        put(s, 1, out[:, 128:])


def inverse_y(get, fourier, real_rows, twist, put):
    slots = []
    for h in (0, 1):
        re, im = get(h, 0), get(h, 1)
        if h == 0:
            row = lax.broadcasted_iota(jnp.int32, (128, 128), 0)
            lane = lax.broadcasted_iota(jnp.int32, (128, 128), 1)
            single = (row == 0) & (lane < 32)
            re, im = jnp.where(single, 0.5 * re, re), jnp.where(single, 0.5 * im, im)
        rows = split(jnp.concatenate([re.T, im.T], 1))
        if h == 0:
            first = product((rows[0][:32], rows[1][:32]), real_rows, NN)
            rows = (rows[0][32:], rows[1][32:])
        out = product(rows, fourier, NN)
        slots += [out[32 * m : 32 * m + 32] for m in range(out.shape[0] // 32)]
    scale = 2.0 / CELLS
    base = [first[:, :128] * scale, first[:, 128:] * scale]
    real, imag = {}, {}
    for j in range(1, 8):
        re, im = slots[j - 1][:, :128], slots[j - 1][:, 128:]
        cos, sin = twist[j : j + 1] * scale, twist[8 + j : 9 + j] * scale
        real[j], imag[j] = re * cos - im * sin, im * cos + re * sin
    ends, tips = real[2] + real[6], imag[6] - imag[2]
    near, far = (real[2] - real[6]) * COS16[2], (imag[2] + imag[6]) * COS16[2]
    part = [ends, near - far, tips, -(near + far)]
    four = [base[0] + real[4], base[1] - imag[4], base[0] - real[4], base[1] + imag[4]]
    even = [four[a] + part[a] for a in range(4)] + [four[a] - part[a] for a in range(4)]
    u, v, w, x = real[1] + real[7], real[3] + real[5], real[1] - real[7], real[3] - real[5]
    cosine = [u + v, w * COS16[1] + x * COS16[3], (u - v) * COS16[2], w * COS16[3] - x * COS16[1]]
    u, v, w, x = imag[1] + imag[7], imag[3] + imag[5], imag[1] - imag[7], imag[3] - imag[5]
    sine = [None, u * SIN16[1] + v * SIN16[3], (w + x) * SIN16[2], u * SIN16[3] - v * SIN16[1], w - x]
    put(0, even[0] + cosine[0])
    put(8, even[0] - cosine[0])
    for a in (1, 2, 3):
        odd, mirror = cosine[a] - sine[a], cosine[a] + sine[a]
        put(a, even[a] + odd)
        put(a + 8, even[a] - odd)
        put(8 - a, even[8 - a] - mirror)
        put(16 - a, even[8 - a] + mirror)
    put(4, even[4] - sine[4])
    put(12, even[4] + sine[4])


def lane_position():
    return (
        16 * lax.axis_index("slab_z")
        + 8 * lax.axis_index("slab_x")
        + 2 * lax.axis_index("slab_y")
        + lax.axis_index("slab_core")
    )


def forward_kernel(
    c_hbm,
    fourier_hbm,
    real_hbm,
    twist_hbm,
    out_ref,
    rate_ref,
    c_ref,
    fourier_ref,
    real_ref,
    twist_ref,
    sems,
):
    def group_of(ref, n):
        return ref.at[n // 2, pl.ds(8 * (n % 2), 8), :]

    sources = [twist_hbm] + [group_of(c_hbm, n) for n in range(4)] + [real_hbm, fourier_hbm]
    targets = [twist_ref] + [group_of(c_ref, n) for n in range(4)] + [real_ref, fourier_ref]
    copies = [
        pltpu.make_async_copy(source, target, sems.at[n])
        for n, (source, target) in enumerate(zip(sources, targets))
    ]
    for copy in copies:
        copy.start()

    def put(h, part, f, value):
        out_ref[pl.ds(5 * h + 2 * part + f, 128, stride=10), :] = value

    def put_rate(sigma, side, kind, value):
        rate_ref[4 * sigma + 2 * side + kind] = value

    def late(n, ref):
        def read():
            copies[n].wait()
            return ref[...]

        return read

    all_rates(lax.axis_index("section"), lane_position(), put_rate)
    def read_rows(n):
        copies[n + 1].wait()
        return c_ref[n // 2, 8 * (n % 2) : 8 * (n % 2) + 8, :]

    lanes = forward_y(read_rows, late(6, fourier_ref), late(5, real_ref), late(0, twist_ref), put)
    out_ref[pl.ds(4, 256, stride=5), :] = jnp.broadcast_to(jnp.sum(lanes, 0, keepdims=True), (256, 128))


def middle_kernel(
    in_ref, rate_ref, gather_ref, lanes_ref, spread_ref, twist_ref, out_ref, bulk_ref
):
    def get(s, part, f):
        return in_ref[pl.ds(5 * s + 2 * part + f, 128, stride=10), :]

    def put(s, part, value):
        out_ref[pl.ds(2 * s + part, 128, stride=4), :] = value

    middle(
        get,
        lambda sigma, side, kind: rate_ref[4 * sigma + 2 * side + kind],
        lax.axis_index("section"),
        lane_position(),
        (gather_ref[0], gather_ref[1]),
        lanes_ref,
        (spread_ref[0], spread_ref[1]),
        twist_ref,
        put,
    )
    bulk = jnp.sum(in_ref[pl.ds(4, 256, stride=5), :], 0, keepdims=True)
    bulk_ref[...] = jnp.broadcast_to(bulk, (8, 128))


def inverse_kernel(in_ref, bulk_ref, fourier_ref, real_ref, twist_ref, out_ref, energy_ref):
    def get(h, part):
        return in_ref[pl.ds(2 * h + part, 128, stride=4), :]

    def put(a, value):
        out_ref[0, :, 128 * a : 128 * a + 128] = value[:16]
        out_ref[1, :, 128 * a : 128 * a + 128] = value[16:]

    energy_ref[...] = jnp.sum(bulk_ref[0:1, :], keepdims=True) * (1.0 / CELLS)
    inverse_y(
        get, (fourier_ref[0], fourier_ref[1]), (real_ref[0], real_ref[1]), twist_ref[...], put
    )


def exchange(rows):
    width = rows.shape[0] // 256
    message = rows.reshape(256, 1, 128 * width)
    return lax.all_to_all(message, ALL, split_axis=0, concat_axis=0, tiled=True).reshape(rows.shape)


def per_device(concentration):
    whole = pl.BlockSpec(memory_space=pltpu.VMEM)
    params = pltpu.CompilerParams(vmem_limit_bytes=12 << 20)
    outgoing, rate = pl.pallas_call(
        forward_kernel,
        out_shape=(
            pltpu.VMEM((1280, 128), f32),
            pltpu.VMEM((8, 128, 128), f32),
        ),
        in_specs=[pl.BlockSpec(memory_space=pltpu.HBM)] * 4,
        out_specs=(whole, whole),
        scratch_shapes=[
            pltpu.VMEM(concentration.shape, f32),
            pltpu.VMEM(FOURIER.shape, bf16),
            pltpu.VMEM(REAL.shape, bf16),
            pltpu.VMEM(Y_TWIST.shape, f32),
            pltpu.SemaphoreType.DMA((7,)),
        ],
        compiler_params=params,
    )(*[pltpu.with_memory_space_constraint(a, pltpu.HBM) for a in (concentration, FOURIER_T, REAL_T, Y_TWIST)])
    columns = exchange(outgoing)
    leaving, bulk = pl.pallas_call(
        middle_kernel,
        out_shape=(pltpu.VMEM((512, 128), f32), pltpu.VMEM((8, 128), f32)),
        in_specs=[whole] * 6,
        out_specs=(whole, whole),
        compiler_params=params,
    )(columns, rate, GATHER, LANES, SPREAD, X_TWIST)
    rows_back = exchange(leaving)
    new_field, energy = pl.pallas_call(
        inverse_kernel,
        out_shape=(jax.ShapeDtypeStruct(concentration.shape, f32), jax.ShapeDtypeStruct((1, 1), f32)),
        in_specs=[whole] * 5,
        out_specs=(whole, whole),
        compiler_params=params,
    )(rows_back, bulk, FOURIER, REAL, Y_TWIST)
    return new_field, energy.reshape(())


def solution(mesh):
    finer = Mesh(mesh.devices.reshape(2, 4, 2, 8, 2), ("section",) + SLAB)
    return jax.shard_map(
        per_device,
        mesh=finer,
        in_specs=(P("section", SLAB, None),),
        out_specs=(P("section", SLAB, None), P()),
        check_vma=False,
    )
```

```python
import math

import jax
import jax.numpy as jnp
import ml_dtypes
import numpy as np
from jax import lax
from jax.experimental import pallas as pl
from jax.experimental.pallas import tpu as pltpu
from jax.sharding import Mesh
from jax.sharding import PartitionSpec as P

SLAB = ("slab_y", "slab_x", "slab_z", "slab_core")
ALL = ("slab_z", "slab_x", "slab_y", "slab_core", "section")
NX = 2048
NY = 2048
NZ = 4
CELLS = NX * NY * NZ
time_step = 100.0
kappa_grad = 2.0
stabilizer = 8.0
f32 = jnp.float32
bf16 = jnp.bfloat16


def halves(matrix):
    high = matrix.astype(np.float32).astype(ml_dtypes.bfloat16)
    low = (matrix - high.astype(np.float64)).astype(np.float32).astype(ml_dtypes.bfloat16)
    return np.stack([high, low])


def fourier_table():
    index = np.arange(128)
    angle = 2.0 * np.pi * (np.outer(index, index) % 128) / 128
    return halves(np.block([[np.cos(angle), np.sin(angle)], [-np.sin(angle), np.cos(angle)]]))


def slab_order():
    return np.arange(128).reshape(4, 2, 8, 2).transpose(2, 1, 0, 3).reshape(128)


def real_table():
    angle = 2.0 * np.pi * (np.outer(np.arange(128), np.arange(256)) % 256) / 256
    lower = -np.sin(angle)
    lower[0] = 1.0 - 2.0 * (np.arange(256) % 2)
    return halves(np.concatenate([np.cos(angle), lower], 0))


def lane_table(parity):
    z_at, x_at = np.arange(2)[:, None, None, None], np.arange(16)[None, :, None, None]
    t_at, q_at = np.arange(2)[None, None, :, None], np.arange(16)[None, None, None, :]
    turn = (4 * parity * z_at + 8 * t_at * z_at + x_at * q_at) % 16
    value = np.exp(-2j * np.pi * turn / 16).reshape(32, 32)
    value = np.kron(np.eye(4), value)
    return halves(np.block([[value.real, value.imag], [-value.imag, value.real]]))


def y_twist_table():
    angle = 2.0 * np.pi * np.outer(np.arange(8), np.arange(128)) / 2048
    return np.concatenate([np.cos(angle), np.sin(angle)], 0).astype(np.float32)


def x_twist_table():
    angle = 2.0 * np.pi * np.outer(np.arange(128), np.arange(128) % 16) / 2048
    return np.stack([np.cos(angle), np.sin(angle)]).astype(np.float32)


FOURIER = fourier_table()
ORDER = slab_order()
GATHER = FOURIER[:, :, np.concatenate([ORDER, 128 + ORDER])]
SPREAD = np.concatenate([FOURIER[:, ORDER, :128], -FOURIER[:, ORDER, 128:]], 2)
REAL = real_table()
LANES = np.stack([lane_table(0), lane_table(1)])
FOURIER_T = FOURIER.transpose(0, 2, 1)
REAL_T = REAL.transpose(0, 2, 1)
Y_TWIST = y_twist_table()
X_TWIST = x_twist_table()
COS16 = [math.cos(2.0 * math.pi * m / 16) for m in range(16)]
SIN16 = [math.sin(2.0 * math.pi * m / 16) for m in range(16)]


def split(value):
    high = value.astype(bf16)
    return high, (value - high.astype(f32)).astype(bf16)


NN = (((1,), (0,)), ((), ()))
NT = (((1,), (1,)), ((), ()))


def product(left, right, pattern):
    total = left[0].shape[0]
    both = lax.dot_general(
        jnp.concatenate(left, 0), right[0], pattern, preferred_element_type=f32
    )
    rest = lax.dot_general(left[0], right[1], pattern, preferred_element_type=f32)
    return both[:total] + (both[total:] + rest)


def y_slots(at):
    add = [at[a] + at[a + 8] for a in range(8)]
    sub = [at[a] - at[a + 8] for a in range(8)]
    both = [add[a] + add[a + 4] for a in range(4)]
    diff = [add[a] - add[a + 4] for a in range(4)]
    zero = jnp.concatenate([both[0] + both[2], both[1] + both[3]], 1)
    near, far = (diff[1] - diff[3]) * COS16[2], (diff[1] + diff[3]) * COS16[2]
    minus = [None] + [sub[a] - sub[8 - a] for a in (1, 2, 3)]
    plus = [None] + [sub[a] + sub[8 - a] for a in (1, 2, 3)]
    middle_re = minus[2] * COS16[2]
    re_17, re_35 = sub[0] + middle_re, sub[0] - middle_re
    re_1, re_3 = minus[1] * COS16[1] + minus[3] * COS16[3], minus[1] * COS16[3] - minus[3] * COS16[1]
    im_1, im_3 = plus[1] * SIN16[1] + plus[3] * SIN16[3], plus[1] * SIN16[3] - plus[3] * SIN16[1]
    middle_im = plus[2] * SIN16[2]
    im_17, im_35 = middle_im + sub[4], middle_im - sub[4]
    return [
        zero,
        (re_17 + re_1, im_1 + im_17, -1),
        (diff[0] + near, diff[2] + far, -1),
        (re_35 + re_3, im_3 + im_35, -1),
        (both[0] - both[2], both[3] - both[1], 1),
        (re_35 - re_3, im_35 - im_3, 1),
        (diff[0] - near, diff[2] - far, 1),
        (re_17 - re_1, im_17 - im_1, 1),
    ]


def turned_slots(at, turns):
    slots = y_slots(at)
    for j in range(1, 8):
        re, n, sign = slots[j]
        cos, sin, negative = turns[j]
        if sign > 0:
            turned = [re * cos + n * sin, n * cos - re * sin]
        else:
            turned = [re * cos - n * sin, n * negative - re * sin]
        slots[j] = jnp.concatenate(turned, 1)
    return slots


def forward_y(read_rows, read_fourier, read_real, read_twist, put):
    twist = read_twist()
    turns = [(twist[j : j + 1], twist[8 + j : 9 + j], -twist[j : j + 1]) for j in range(8)]
    blocks, slots = [], []
    for group in range(4):
        rows = read_rows(group)
        blocks.append([rows[:, 128 * a : 128 * a + 128] for a in range(16)])
        slots.append(turned_slots(blocks[group], turns))
    real_rows = read_real()
    fourier = read_fourier()
    lanes = None
    for f in (0, 1):
        if f == 1:
            slots = []
            for block in blocks:
                cubic = []
                for value in block:
                    squared = value * value
                    bulk = squared * (0.25 * squared - 0.5)
                    lanes = bulk if lanes is None else lanes + bulk
                    cubic.append(squared * value - value)
                slots.append(turned_slots(cubic, turns))
        first = product(split(jnp.concatenate([slot[0] for slot in slots], 0)), real_rows, NN)
        others = [slot[j] for j in range(1, 8) for slot in slots]
        rest = product(split(jnp.concatenate(others, 0)), fourier, NN)
        for h, rows in ((0, jnp.concatenate([first, rest[:96]], 0)), (1, rest[96:])):
            put(h, 0, f, rows[:, :128].T)
            put(h, 1, f, rows[:, 128:].T)
    return lanes


def wave_square(index, length):
    signed = jnp.where(2 * index >= length, index - length, index)
    phase_angle = signed.astype(f32) * (2.0 * math.pi / length)
    return phase_angle * phase_angle


def rates(wave_sq):
    numerator = 1.0 + time_step * stabilizer * wave_sq
    inverse = 1.0 / (numerator + time_step * kappa_grad * wave_sq * wave_sq)
    return numerator * inverse, time_step * wave_sq * inverse


def all_rates(section_at, lane_at, put):
    lane = lax.broadcasted_iota(jnp.int32, (128, 128), 1)
    row = lax.broadcasted_iota(jnp.int32, (128, 128), 0)
    slot = 4 * section_at + lane // 32
    y_index = jnp.where(slot == 0, 8 * lane_at, slot + 16 * lane_at)
    x_index = row + 128 * (lane % 16)
    wave_x = wave_square(x_index, NX)
    wave_xy = wave_x + wave_square(y_index, NY)
    half_y = (2.0 * math.pi / NY * (NY // 2)) ** 2
    for sigma in (0, 1):
        wave_z = wave_square(sigma + 2 * (lane // 16 % 2), NZ)
        for side, wave_sq in ((0, wave_z + wave_xy), (1, wave_z + (wave_x + half_y))):
            keep, mix = rates(wave_sq)
            put(sigma, side, 0, keep)
            put(sigma, side, 1, mix)


def middle(get, get_rate, section_at, lane_at, gather, lanes, spread_table, twist, put):
    lane = lax.broadcasted_iota(jnp.int32, (128, 128), 1)
    packed = (lane < 32) & (section_at == 0) & (lane_at == 0)
    cos, sin = twist[0], twist[1]
    parts = []
    for s in (0, 1):
        c_re, c_im, g_re, g_im = get(s, 0, 0), get(s, 1, 0), get(s, 0, 1), get(s, 1, 1)
        c_im, g_re = jnp.where(packed, g_re, c_im), jnp.where(packed, c_im, g_re)
        parts.append((c_re, c_im, g_re, g_im))
    stacked = []
    for sigma in (0, 1):
        mixed = [a + b if sigma == 0 else a - b for a, b in zip(*parts)]
        stacked.append(
            jnp.concatenate(
                [jnp.concatenate([mixed[0], mixed[2]], 1), jnp.concatenate([mixed[1], mixed[3]], 1)], 0
            )
        )
    spreads = [product(gather, split(stacked[sigma]), NN) for sigma in (0, 1)]
    turned = []
    for spread in spreads:
        rows = []
        for f in (0, 1):
            re, im = spread[:128, 128 * f : 128 * f + 128], spread[128:, 128 * f : 128 * f + 128]
            rows.append(jnp.concatenate([re * cos + im * sin, im * cos - re * sin], 1))
        turned.append(split(jnp.concatenate(rows, 0)))
    tables = [(lanes[sigma, 0], lanes[sigma, 1]) for sigma in (0, 1)]
    specs = [product(turned[sigma], tables[sigma], NN) for sigma in (0, 1)]
    filtered = []
    for sigma, spec in enumerate(specs):
        c_re, c_im, g_re, g_im = spec[:128, :128], spec[:128, 128:], spec[128:, :128], spec[128:, 128:]
        keep, mix = get_rate(sigma, 0, 0), get_rate(sigma, 0, 1)
        keep_half, mix_half = get_rate(sigma, 1, 0), get_rate(sigma, 1, 1)
        main_re = keep * c_re - mix * jnp.where(packed, c_im, g_re)
        main_im = keep * c_im - mix * jnp.where(packed, -c_re, g_im)
        side_re = keep_half * g_re - mix_half * g_im
        side_im = keep_half * g_im + mix_half * g_re
        rows = jnp.concatenate(
            [jnp.concatenate([main_re, main_im], 1), jnp.concatenate([side_re, side_im], 1)], 0
        )
        filtered.append(split(rows))
    back = [product(filtered[sigma], tables[sigma], NT) for sigma in (0, 1)]
    for s in (0, 1):
        mixed = back[0] + back[1] if s == 0 else back[0] - back[1]
        both = []
        for f in (0, 1):
            re, im = mixed[128 * f : 128 * f + 128, :128], mixed[128 * f : 128 * f + 128, 128:]
            both.append((re * cos - im * sin, im * cos + re * sin))
        (m_re, m_im), (s_re, s_im) = both
        upper = jnp.concatenate([m_re, jnp.where(packed, s_re, m_im)], 1)
        lower = jnp.concatenate([m_im, jnp.where(packed, s_im, -m_re)], 1)
        out = product(spread_table, split(jnp.concatenate([upper, lower], 0)), NN)
        put(s, 0, out[:, :128])
        put(s, 1, out[:, 128:])


def inverse_y(get, fourier, real_rows, twist, put):
    slots = []
    for h in (0, 1):
        re, im = get(h, 0), get(h, 1)
        if h == 0:
            row = lax.broadcasted_iota(jnp.int32, (128, 128), 0)
            lane = lax.broadcasted_iota(jnp.int32, (128, 128), 1)
            single = (row == 0) & (lane < 32)
            re, im = jnp.where(single, 0.5 * re, re), jnp.where(single, 0.5 * im, im)
        rows = split(jnp.concatenate([re.T, im.T], 1))
        if h == 0:
            first = product((rows[0][:32], rows[1][:32]), real_rows, NN)
            rows = (rows[0][32:], rows[1][32:])
        out = product(rows, fourier, NN)
        slots += [out[32 * m : 32 * m + 32] for m in range(out.shape[0] // 32)]
    scale = 2.0 / CELLS
    base = [first[:, :128] * scale, first[:, 128:] * scale]
    real, imag = {}, {}
    for j in range(1, 8):
        re, im = slots[j - 1][:, :128], slots[j - 1][:, 128:]
        cos, sin = twist[j : j + 1] * scale, twist[8 + j : 9 + j] * scale
        real[j], imag[j] = re * cos - im * sin, im * cos + re * sin
    ends, tips = real[2] + real[6], imag[6] - imag[2]
    near, far = (real[2] - real[6]) * COS16[2], (imag[2] + imag[6]) * COS16[2]
    part = [ends, near - far, tips, -(near + far)]
    four = [base[0] + real[4], base[1] - imag[4], base[0] - real[4], base[1] + imag[4]]
    even = [four[a] + part[a] for a in range(4)] + [four[a] - part[a] for a in range(4)]
    u, v, w, x = real[1] + real[7], real[3] + real[5], real[1] - real[7], real[3] - real[5]
    cosine = [u + v, w * COS16[1] + x * COS16[3], (u - v) * COS16[2], w * COS16[3] - x * COS16[1]]
    u, v, w, x = imag[1] + imag[7], imag[3] + imag[5], imag[1] - imag[7], imag[3] - imag[5]
    sine = [None, u * SIN16[1] + v * SIN16[3], (w + x) * SIN16[2], u * SIN16[3] - v * SIN16[1], w - x]
    put(0, even[0] + cosine[0])
    put(8, even[0] - cosine[0])
    for a in (1, 2, 3):
        odd, mirror = cosine[a] - sine[a], cosine[a] + sine[a]
        put(a, even[a] + odd)
        put(a + 8, even[a] - odd)
        put(8 - a, even[8 - a] - mirror)
        put(16 - a, even[8 - a] + mirror)
    put(4, even[4] - sine[4])
    put(12, even[4] + sine[4])


def lane_position():
    return (
        16 * lax.axis_index("slab_z")
        + 8 * lax.axis_index("slab_x")
        + 2 * lax.axis_index("slab_y")
        + lax.axis_index("slab_core")
    )


def forward_kernel(
    c_hbm,
    fourier_hbm,
    real_hbm,
    twist_hbm,
    out_ref,
    rate_ref,
    c_ref,
    fourier_ref,
    real_ref,
    twist_ref,
    sems,
):
    def group_of(ref, n):
        return ref.at[n // 2, pl.ds(8 * (n % 2), 8), :]

    sources = [twist_hbm] + [group_of(c_hbm, n) for n in range(4)] + [real_hbm, fourier_hbm]
    targets = [twist_ref] + [group_of(c_ref, n) for n in range(4)] + [real_ref, fourier_ref]
    copies = [
        pltpu.make_async_copy(source, target, sems.at[n])
        for n, (source, target) in enumerate(zip(sources, targets))
    ]
    for copy in copies:
        copy.start()

    def put(h, part, f, value):
        out_ref[pl.ds(5 * h + 2 * part + f, 128, stride=10), :] = value

    def put_rate(sigma, side, kind, value):
        rate_ref[4 * sigma + 2 * side + kind] = value

    def late(n, ref):
        def read():
            copies[n].wait()
            return ref[...]

        return read

    all_rates(lax.axis_index("section"), lane_position(), put_rate)
    def read_rows(n):
        copies[n + 1].wait()
        return c_ref[n // 2, 8 * (n % 2) : 8 * (n % 2) + 8, :]

    lanes = forward_y(read_rows, late(6, fourier_ref), late(5, real_ref), late(0, twist_ref), put)
    out_ref[pl.ds(4, 256, stride=5), :] = jnp.broadcast_to(jnp.sum(lanes, 0, keepdims=True), (256, 128))


def middle_kernel(
    in_ref, rate_ref, gather_ref, lanes_ref, spread_ref, twist_ref, out_ref, bulk_ref
):
    def get(s, part, f):
        return in_ref[pl.ds(5 * s + 2 * part + f, 128, stride=10), :]

    def put(s, part, value):
        out_ref[pl.ds(2 * s + part, 128, stride=4), :] = value

    middle(
        get,
        lambda sigma, side, kind: rate_ref[4 * sigma + 2 * side + kind],
        lax.axis_index("section"),
        lane_position(),
        (gather_ref[0], gather_ref[1]),
        lanes_ref,
        (spread_ref[0], spread_ref[1]),
        twist_ref,
        put,
    )
    bulk = jnp.sum(in_ref[pl.ds(4, 256, stride=5), :], 0, keepdims=True)
    bulk_ref[...] = jnp.broadcast_to(bulk, (8, 128))


def inverse_kernel(in_ref, bulk_ref, fourier_ref, real_ref, twist_ref, out_ref, energy_ref):
    def get(h, part):
        return in_ref[pl.ds(2 * h + part, 128, stride=4), :]

    def put(a, value):
        out_ref[0, :, 128 * a : 128 * a + 128] = value[:16]
        out_ref[1, :, 128 * a : 128 * a + 128] = value[16:]

    energy_ref[...] = jnp.sum(bulk_ref[0:1, :], keepdims=True) * (1.0 / CELLS)
    inverse_y(
        get, (fourier_ref[0], fourier_ref[1]), (real_ref[0], real_ref[1]), twist_ref[...], put
    )


def exchange(rows):
    width = rows.shape[0] // 256
    message = rows.reshape(256, 1, 128 * width)
    return lax.all_to_all(message, ALL, split_axis=0, concat_axis=0, tiled=True).reshape(rows.shape)


def per_device(concentration):
    whole = pl.BlockSpec(memory_space=pltpu.VMEM)
    params = pltpu.CompilerParams(vmem_limit_bytes=12 << 20)
    outgoing, rate = pl.pallas_call(
        forward_kernel,
        out_shape=(
            pltpu.VMEM((1280, 128), f32),
            pltpu.VMEM((8, 128, 128), f32),
        ),
        in_specs=[pl.BlockSpec(memory_space=pltpu.HBM)] * 4,
        out_specs=(whole, whole),
        scratch_shapes=[
            pltpu.VMEM(concentration.shape, f32),
            pltpu.VMEM(FOURIER.shape, bf16),
            pltpu.VMEM(REAL.shape, bf16),
            pltpu.VMEM(Y_TWIST.shape, f32),
            pltpu.SemaphoreType.DMA((7,)),
        ],
        compiler_params=params,
    )(*[pltpu.with_memory_space_constraint(a, pltpu.HBM) for a in (concentration, FOURIER_T, REAL_T, Y_TWIST)])
    columns = exchange(outgoing)
    leaving, bulk = pl.pallas_call(
        middle_kernel,
        out_shape=(pltpu.VMEM((512, 128), f32), pltpu.VMEM((8, 128), f32)),
        in_specs=[whole] * 6,
        out_specs=(whole, whole),
        compiler_params=params,
    )(columns, rate, GATHER, LANES, SPREAD, X_TWIST)
    rows_back = exchange(leaving)
    new_field, energy = pl.pallas_call(
        inverse_kernel,
        out_shape=(jax.ShapeDtypeStruct(concentration.shape, f32), jax.ShapeDtypeStruct((1, 1), f32)),
        in_specs=[whole] * 5,
        out_specs=(whole, whole),
        compiler_params=params,
    )(rows_back, bulk, FOURIER, REAL, Y_TWIST)
    return new_field, energy.reshape(())


def solution(mesh):
    finer = Mesh(mesh.devices.reshape(2, 4, 2, 8, 2), ("section",) + SLAB)
    return jax.shard_map(
        per_device,
        mesh=finer,
        in_specs=(P("section", SLAB, None),),
        out_specs=(P("section", SLAB, None), P()),
        check_vma=False,
    )
```

```python
import math

import jax
import jax.numpy as jnp
import ml_dtypes
import numpy as np
from jax import lax
from jax.experimental import pallas as pl
from jax.experimental.pallas import tpu as pltpu
from jax.sharding import Mesh
from jax.sharding import PartitionSpec as P

SLAB = ("slab_y", "slab_x", "slab_z", "slab_core")
ALL = ("slab_x", "slab_z", "slab_y", "slab_core", "section")
NX = 2048
NY = 2048
NZ = 4
CELLS = NX * NY * NZ
time_step = 100.0
kappa_grad = 2.0
stabilizer = 8.0
f32 = jnp.float32
bf16 = jnp.bfloat16


def halves(matrix):
    high = matrix.astype(np.float32).astype(ml_dtypes.bfloat16)
    low = (matrix - high.astype(np.float64)).astype(np.float32).astype(ml_dtypes.bfloat16)
    return np.stack([high, low])


def fourier_table():
    index = np.arange(128)
    angle = 2.0 * np.pi * (np.outer(index, index) % 128) / 128
    return halves(np.block([[np.cos(angle), np.sin(angle)], [-np.sin(angle), np.cos(angle)]]))


def slab_order():
    return np.arange(128).reshape(4, 2, 8, 2).transpose(1, 2, 0, 3).reshape(128)


def real_table():
    angle = 2.0 * np.pi * (np.outer(np.arange(128), np.arange(256)) % 256) / 256
    lower = -np.sin(angle)
    lower[0] = 1.0 - 2.0 * (np.arange(256) % 2)
    return halves(np.concatenate([np.cos(angle), lower], 0))


def lane_table(parity):
    z_at, x_at = np.arange(2)[:, None, None, None], np.arange(16)[None, :, None, None]
    t_at, q_at = np.arange(2)[None, None, :, None], np.arange(16)[None, None, None, :]
    turn = (4 * parity * z_at + 8 * t_at * z_at + x_at * q_at) % 16
    value = np.exp(-2j * np.pi * turn / 16).reshape(32, 32)
    value = np.kron(np.eye(4), value)
    return halves(np.block([[value.real, value.imag], [-value.imag, value.real]]))


def y_twist_table():
    angle = 2.0 * np.pi * np.outer(np.arange(8), np.arange(128)) / 2048
    return np.concatenate([np.cos(angle), np.sin(angle)], 0).astype(np.float32)


def x_twist_table():
    angle = 2.0 * np.pi * np.outer(np.arange(128), np.arange(128) % 16) / 2048
    return np.stack([np.cos(angle), np.sin(angle)]).astype(np.float32)


FOURIER = fourier_table()
ORDER = slab_order()
GATHER = FOURIER[:, :, np.concatenate([ORDER, 128 + ORDER])]
SPREAD = FOURIER[:, ORDER, :]
REAL = real_table()
LANES = np.stack([lane_table(0), lane_table(1)])
FOURIER_T = FOURIER.transpose(0, 2, 1)
REAL_T = REAL.transpose(0, 2, 1)
Y_TWIST = y_twist_table()
X_TWIST = x_twist_table()
COS16 = [math.cos(2.0 * math.pi * m / 16) for m in range(16)]
SIN16 = [math.sin(2.0 * math.pi * m / 16) for m in range(16)]


def split(value):
    high = value.astype(bf16)
    return high, (value - high.astype(f32)).astype(bf16)


NN = (((1,), (0,)), ((), ()))
NT = (((1,), (1,)), ((), ()))


def product(left, right, pattern):
    total = left[0].shape[0]
    both = lax.dot_general(
        jnp.concatenate(left, 0), right[0], pattern, preferred_element_type=f32
    )
    rest = lax.dot_general(left[0], right[1], pattern, preferred_element_type=f32)
    return both[:total] + (both[total:] + rest)


def y_slots(at):
    add = [at[a] + at[a + 8] for a in range(8)]
    sub = [at[a] - at[a + 8] for a in range(8)]
    both = [add[a] + add[a + 4] for a in range(4)]
    diff = [add[a] - add[a + 4] for a in range(4)]
    zero = jnp.concatenate([both[0] + both[2], both[1] + both[3]], 1)
    near, far = (diff[1] - diff[3]) * COS16[2], (diff[1] + diff[3]) * COS16[2]
    minus = [None] + [sub[a] - sub[8 - a] for a in (1, 2, 3)]
    plus = [None] + [sub[a] + sub[8 - a] for a in (1, 2, 3)]
    middle_re = minus[2] * COS16[2]
    re_17, re_35 = sub[0] + middle_re, sub[0] - middle_re
    re_1, re_3 = minus[1] * COS16[1] + minus[3] * COS16[3], minus[1] * COS16[3] - minus[3] * COS16[1]
    im_1, im_3 = plus[1] * SIN16[1] + plus[3] * SIN16[3], plus[1] * SIN16[3] - plus[3] * SIN16[1]
    middle_im = plus[2] * SIN16[2]
    im_17, im_35 = middle_im + sub[4], middle_im - sub[4]
    return [
        zero,
        (re_17 + re_1, im_1 + im_17, -1),
        (diff[0] + near, diff[2] + far, -1),
        (re_35 + re_3, im_3 + im_35, -1),
        (both[0] - both[2], both[3] - both[1], 1),
        (re_35 - re_3, im_35 - im_3, 1),
        (diff[0] - near, diff[2] - far, 1),
        (re_17 - re_1, im_17 - im_1, 1),
    ]


def turned_slots(at, turns):
    slots = y_slots(at)
    for j in range(1, 8):
        re, n, sign = slots[j]
        cos, sin, negative = turns[j]
        if sign > 0:
            turned = [re * cos + n * sin, n * cos - re * sin]
        else:
            turned = [re * cos - n * sin, n * negative - re * sin]
        slots[j] = jnp.concatenate(turned, 1)
    return slots


def forward_y(read_rows, read_fourier, read_real, read_twist, put):
    twist = read_twist()
    turns = [(twist[j : j + 1], twist[8 + j : 9 + j], -twist[j : j + 1]) for j in range(8)]
    blocks, slots = [], []
    for group in range(4):
        rows = read_rows(group)
        blocks.append([rows[:, 128 * a : 128 * a + 128] for a in range(16)])
        slots.append(turned_slots(blocks[group], turns))
    real_rows = read_real()
    fourier = read_fourier()
    lanes = None
    for f in (0, 1):
        if f == 1:
            slots = []
            for block in blocks:
                cubic = []
                for value in block:
                    squared = value * value
                    bulk = squared * (0.25 * squared - 0.5)
                    lanes = bulk if lanes is None else lanes + bulk
                    cubic.append(squared * value - value)
                slots.append(turned_slots(cubic, turns))
        first = product(split(jnp.concatenate([slot[0] for slot in slots], 0)), real_rows, NN)
        others = [slot[j] for j in range(1, 8) for slot in slots]
        rest = product(split(jnp.concatenate(others, 0)), fourier, NN)
        for h, rows in ((0, jnp.concatenate([first, rest[:96]], 0)), (1, rest[96:])):
            put(h, 0, f, rows[:, :128].T)
            put(h, 1, f, rows[:, 128:].T)
    return lanes


def wave_square(index, length):
    signed = jnp.where(2 * index >= length, index - length, index)
    phase_angle = signed.astype(f32) * (2.0 * math.pi / length)
    return phase_angle * phase_angle


def rates(wave_sq):
    numerator = 1.0 + time_step * stabilizer * wave_sq
    inverse = 1.0 / (numerator + time_step * kappa_grad * wave_sq * wave_sq)
    return numerator * inverse, time_step * wave_sq * inverse


def all_rates(section_at, lane_at, put):
    lane = lax.broadcasted_iota(jnp.int32, (128, 128), 1)
    row = lax.broadcasted_iota(jnp.int32, (128, 128), 0)
    slot = 4 * section_at + lane // 32
    y_index = jnp.where(slot == 0, 8 * lane_at, slot + 16 * lane_at)
    x_index = row + 128 * (lane % 16)
    wave_x = wave_square(x_index, NX)
    wave_xy = wave_x + wave_square(y_index, NY)
    half_y = (2.0 * math.pi / NY * (NY // 2)) ** 2
    for sigma in (0, 1):
        wave_z = wave_square(sigma + 2 * (lane // 16 % 2), NZ)
        for side, wave_sq in ((0, wave_z + wave_xy), (1, wave_z + (wave_x + half_y))):
            keep, mix = rates(wave_sq)
            put(sigma, side, 0, keep)
            put(sigma, side, 1, mix)


def middle(get, get_rate, section_at, lane_at, gather, lanes, spread_table, twist, put):
    lane = lax.broadcasted_iota(jnp.int32, (128, 128), 1)
    packed = (lane < 32) & (section_at == 0) & (lane_at == 0)
    cos, sin = twist[0], twist[1]
    parts = []
    for s in (0, 1):
        c_re, c_im, g_re, g_im = get(s, 0, 0), get(s, 1, 0), get(s, 0, 1), get(s, 1, 1)
        c_im, g_re = jnp.where(packed, g_re, c_im), jnp.where(packed, c_im, g_re)
        parts.append((c_re, c_im, g_re, g_im))
    stacked = []
    for sigma in (0, 1):
        mixed = [a + b if sigma == 0 else a - b for a, b in zip(*parts)]
        stacked.append(
            jnp.concatenate(
                [jnp.concatenate([mixed[0], mixed[2]], 1), jnp.concatenate([mixed[1], mixed[3]], 1)], 0
            )
        )
    spreads = [product(gather, split(stacked[sigma]), NN) for sigma in (0, 1)]
    turned = []
    for spread in spreads:
        rows = []
        for f in (0, 1):
            re, im = spread[:128, 128 * f : 128 * f + 128], spread[128:, 128 * f : 128 * f + 128]
            rows.append(jnp.concatenate([re * cos + im * sin, im * cos - re * sin], 1))
        turned.append(split(jnp.concatenate(rows, 0)))
    tables = [(lanes[sigma, 0], lanes[sigma, 1]) for sigma in (0, 1)]
    specs = [product(turned[sigma], tables[sigma], NN) for sigma in (0, 1)]
    filtered = []
    for sigma, spec in enumerate(specs):
        c_re, c_im, g_re, g_im = spec[:128, :128], spec[:128, 128:], spec[128:, :128], spec[128:, 128:]
        keep, mix = get_rate(sigma, 0, 0), get_rate(sigma, 0, 1)
        keep_half, mix_half = get_rate(sigma, 1, 0), get_rate(sigma, 1, 1)
        main_re = keep * c_re - mix * jnp.where(packed, c_im, g_re)
        main_im = keep * c_im - mix * jnp.where(packed, -c_re, g_im)
        side_re = keep_half * g_re - mix_half * g_im
        side_im = keep_half * g_im + mix_half * g_re
        rows = jnp.concatenate(
            [jnp.concatenate([main_re, main_im], 1), jnp.concatenate([side_re, side_im], 1)], 0
        )
        filtered.append(split(rows))
    back = [product(filtered[sigma], tables[sigma], NT) for sigma in (0, 1)]
    for s in (0, 1):
        mixed = back[0] + back[1] if s == 0 else back[0] - back[1]
        both = []
        for f in (0, 1):
            re, im = mixed[128 * f : 128 * f + 128, :128], mixed[128 * f : 128 * f + 128, 128:]
            both.append((re * cos - im * sin, im * cos + re * sin))
        (m_re, m_im), (s_re, s_im) = both
        upper = jnp.concatenate([m_re, jnp.where(packed, s_re, m_im)], 1)
        lower = jnp.concatenate([-m_im, jnp.where(packed, -s_im, m_re)], 1)
        out = product(spread_table, split(jnp.concatenate([upper, lower], 0)), NN)
        put(s, 0, out[:, :128])
        put(s, 1, out[:, 128:])


def inverse_y(get, fourier, real_rows, twist, put):
    slots = []
    for h in (0, 1):
        re, im = get(h, 0), get(h, 1)
        if h == 0:
            row = lax.broadcasted_iota(jnp.int32, (128, 128), 0)
            lane = lax.broadcasted_iota(jnp.int32, (128, 128), 1)
            single = (row == 0) & (lane < 32)
            re, im = jnp.where(single, 0.5 * re, re), jnp.where(single, 0.5 * im, im)
        rows = split(jnp.concatenate([re.T, im.T], 1))
        if h == 0:
            first = product((rows[0][:32], rows[1][:32]), real_rows, NN)
            rows = (rows[0][32:], rows[1][32:])
        out = product(rows, fourier, NN)
        slots += [out[32 * m : 32 * m + 32] for m in range(out.shape[0] // 32)]
    scale = 2.0 / CELLS
    base = [first[:, :128] * scale, first[:, 128:] * scale]
    real, imag = {}, {}
    for j in range(1, 8):
        re, im = slots[j - 1][:, :128], slots[j - 1][:, 128:]
        cos, sin = twist[j : j + 1] * scale, twist[8 + j : 9 + j] * scale
        real[j], imag[j] = re * cos - im * sin, im * cos + re * sin
    ends, tips = real[2] + real[6], imag[6] - imag[2]
    near, far = (real[2] - real[6]) * COS16[2], (imag[2] + imag[6]) * COS16[2]
    part = [ends, near - far, tips, -(near + far)]
    four = [base[0] + real[4], base[1] - imag[4], base[0] - real[4], base[1] + imag[4]]
    even = [four[a] + part[a] for a in range(4)] + [four[a] - part[a] for a in range(4)]
    u, v, w, x = real[1] + real[7], real[3] + real[5], real[1] - real[7], real[3] - real[5]
    cosine = [u + v, w * COS16[1] + x * COS16[3], (u - v) * COS16[2], w * COS16[3] - x * COS16[1]]
    u, v, w, x = imag[1] + imag[7], imag[3] + imag[5], imag[1] - imag[7], imag[3] - imag[5]
    sine = [None, u * SIN16[1] + v * SIN16[3], (w + x) * SIN16[2], u * SIN16[3] - v * SIN16[1], w - x]
    put(0, even[0] + cosine[0])
    put(8, even[0] - cosine[0])
    for a in (1, 2, 3):
        odd, mirror = cosine[a] - sine[a], cosine[a] + sine[a]
        put(a, even[a] + odd)
        put(a + 8, even[a] - odd)
        put(8 - a, even[8 - a] - mirror)
        put(16 - a, even[8 - a] + mirror)
    put(4, even[4] - sine[4])
    put(12, even[4] + sine[4])


def lane_position():
    return (
        8 * lax.axis_index("slab_z")
        + 64 * lax.axis_index("slab_x")
        + 2 * lax.axis_index("slab_y")
        + lax.axis_index("slab_core")
    )


def forward_kernel(
    c_hbm,
    fourier_hbm,
    real_hbm,
    twist_hbm,
    out_ref,
    rate_ref,
    c_ref,
    fourier_ref,
    real_ref,
    twist_ref,
    sems,
):
    def group_of(ref, n):
        return ref.at[n // 2, pl.ds(8 * (n % 2), 8), :]

    sources = [twist_hbm] + [group_of(c_hbm, n) for n in range(4)] + [real_hbm, fourier_hbm]
    targets = [twist_ref] + [group_of(c_ref, n) for n in range(4)] + [real_ref, fourier_ref]
    copies = [
        pltpu.make_async_copy(source, target, sems.at[n])
        for n, (source, target) in enumerate(zip(sources, targets))
    ]
    for copy in copies:
        copy.start()

    def put(h, part, f, value):
        out_ref[pl.ds(5 * h + 2 * part + f, 128, stride=10), :] = value

    def put_rate(sigma, side, kind, value):
        rate_ref[4 * sigma + 2 * side + kind] = value

    def late(n, ref):
        def read():
            copies[n].wait()
            return ref[...]

        return read

    all_rates(lax.axis_index("section"), lane_position(), put_rate)
    def read_rows(n):
        copies[n + 1].wait()
        return c_ref[n // 2, 8 * (n % 2) : 8 * (n % 2) + 8, :]

    lanes = forward_y(read_rows, late(6, fourier_ref), late(5, real_ref), late(0, twist_ref), put)
    out_ref[pl.ds(4, 256, stride=5), :] = jnp.broadcast_to(jnp.sum(lanes, 0, keepdims=True), (256, 128))


def middle_kernel(
    in_ref, rate_ref, gather_ref, lanes_ref, spread_ref, twist_ref, out_ref, bulk_ref
):
    def get(s, part, f):
        return in_ref[pl.ds(5 * s + 2 * part + f, 128, stride=10), :]

    def put(s, part, value):
        out_ref[pl.ds(2 * s + part, 128, stride=4), :] = value

    middle(
        get,
        lambda sigma, side, kind: rate_ref[4 * sigma + 2 * side + kind],
        lax.axis_index("section"),
        lane_position(),
        (gather_ref[0], gather_ref[1]),
        lanes_ref,
        (spread_ref[0], spread_ref[1]),
        twist_ref,
        put,
    )
    bulk = jnp.sum(in_ref[pl.ds(4, 256, stride=5), :], 0, keepdims=True)
    bulk_ref[...] = jnp.broadcast_to(bulk, (8, 128))


def inverse_kernel(in_ref, bulk_ref, fourier_ref, real_ref, twist_ref, out_ref, energy_ref):
    def get(h, part):
        return in_ref[pl.ds(2 * h + part, 128, stride=4), :]

    def put(a, value):
        out_ref[0, :, 128 * a : 128 * a + 128] = value[:16]
        out_ref[1, :, 128 * a : 128 * a + 128] = value[16:]

    energy_ref[...] = jnp.sum(bulk_ref[0:1, :], keepdims=True) * (1.0 / CELLS)
    inverse_y(
        get, (fourier_ref[0], fourier_ref[1]), (real_ref[0], real_ref[1]), twist_ref[...], put
    )


def exchange(rows):
    width = rows.shape[0] // 256
    message = rows.reshape(256, 1, 128 * width)
    return lax.all_to_all(message, ALL, split_axis=0, concat_axis=0, tiled=True).reshape(rows.shape)


def per_device(concentration):
    whole = pl.BlockSpec(memory_space=pltpu.VMEM)
    params = pltpu.CompilerParams(vmem_limit_bytes=12 << 20)
    outgoing, rate = pl.pallas_call(
        forward_kernel,
        out_shape=(
            pltpu.VMEM((1280, 128), f32),
            pltpu.VMEM((8, 128, 128), f32),
        ),
        in_specs=[pl.BlockSpec(memory_space=pltpu.HBM)] * 4,
        out_specs=(whole, whole),
        scratch_shapes=[
            pltpu.VMEM(concentration.shape, f32),
            pltpu.VMEM(FOURIER.shape, bf16),
            pltpu.VMEM(REAL.shape, bf16),
            pltpu.VMEM(Y_TWIST.shape, f32),
            pltpu.SemaphoreType.DMA((7,)),
        ],
        compiler_params=params,
    )(*[pltpu.with_memory_space_constraint(a, pltpu.HBM) for a in (concentration, FOURIER_T, REAL_T, Y_TWIST)])
    columns = exchange(outgoing)
    leaving, bulk = pl.pallas_call(
        middle_kernel,
        out_shape=(pltpu.VMEM((512, 128), f32), pltpu.VMEM((8, 128), f32)),
        in_specs=[whole] * 6,
        out_specs=(whole, whole),
        compiler_params=params,
    )(columns, rate, GATHER, LANES, SPREAD, X_TWIST)
    rows_back = exchange(leaving)
    new_field, energy = pl.pallas_call(
        inverse_kernel,
        out_shape=(jax.ShapeDtypeStruct(concentration.shape, f32), jax.ShapeDtypeStruct((1, 1), f32)),
        in_specs=[whole] * 5,
        out_specs=(whole, whole),
        compiler_params=params,
    )(rows_back, bulk, FOURIER, REAL, Y_TWIST)
    return new_field, energy.reshape(())


def solution(mesh):
    finer = Mesh(mesh.devices.reshape(2, 4, 2, 8, 2), ("section",) + SLAB)
    return jax.shard_map(
        per_device,
        mesh=finer,
        in_specs=(P("section", SLAB, None),),
        out_specs=(P("section", SLAB, None), P()),
        check_vma=False,
    )
```
